256 devices in a mesh: rep: 4 (over z_hi), px: 8 (over x, core), py: 8 (over z_lo, y).
Axes of the slice: x: 4, y: 4, z: 8 (z_hi: 4, z_lo: 2; z = z_hi * 2 + z_lo), core: 2. Of those that a mesh axis runs over, the one named last changes fastest.
Arguments:
- state: float32 [12, 2, 192, 96, 256], P('rep', None, 'px', 'py'), parts along dimension 0, may hold values from -6 to 6
- cotangent: float32 [12, 2, 192, 96, 256], P('rep', None, 'px', 'py'), parts along dimension 0, may hold values from -6 to 6
- w_in: bfloat16 [512, 192], replicated, may hold values from -0.4375 to 0.4375
- b_in: float32 [512], replicated, may hold values from -5 to 5
- w_out: bfloat16 [192, 512], replicated, may hold values from -0.25 to 0.25
Outputs:
- state_grad: float32 [12, 2, 192, 96, 256], P('rep', None, 'px', 'py'), parts along dimension 0
- grad_in: float32 [512, 768], P(('px', 'py'), 'rep'), parts along dimension 1
- grad_out: float32 [768, 512], P('rep', ('px', 'py')), parts along dimension 0
- grad_bias: float32 [4, 512], P('rep', ('px', 'py')), parts along dimension 0
The draws below stay inside these ranges and needn't reach their ends.
There are 4 independent parts, one for each index of `rep`. The reference program is written for one: setup_inputs(seed, part) draws one part's arguments, and reference() takes and returns one part's arrays. A program takes and returns all parts, laid end to end along the dimension named above; an argument that names none is the same for every part. Nothing has to cross between parts.
All inputs are finite; a program needn't handle non-finite values.
Results may differ from the reference program's by a relative error of at most 0.0065.
The reference program's roundings to bfloat16 on the way count: a program that leaves them out, or rounds other values in their place, can miss the bound.
Values may be sent and summed in bfloat16 or wider, within the bound.
A program may use at most 128 MiB of HBM per device.

```python
import math
import jax
import jax.numpy as jnp
from jax import lax

NG = 256
KY = 192
KZ = 96
PATCH = 4
FEAT = 192
HID = 512


def steps_of(rng, shape, cuts, smallest, largest):
    def one(position, blocks):
        heights = jax.random.uniform(jax.random.fold_in(jax.random.fold_in(rng, 6), position), (blocks,), jnp.float32, smallest / len(cuts), largest / len(cuts))
        return jnp.repeat(jnp.exp(heights), shape[position] // blocks).reshape((-1,) + (1,) * (len(shape) - position - 1))

    level = one(*cuts[0])
    for cut in cuts[1:]:
        level = level * one(*cut)
    return level


def centred(rng, dims, deviation, reach, pieces=(), held_as=jnp.bfloat16):
    drawn = jax.random.normal(rng, dims, jnp.float32) * deviation
    if len(pieces) > 0:
        drawn = steps_of(rng, dims, pieces, -0.22, 0.18) * drawn
    return jnp.clip(drawn, min=-reach, max=reach).astype(held_as)


def setup_inputs(seed: int = 0, part: int = 0) -> dict:
    seeds = jax.random.split(jax.random.key(seed), 6)
    own_keys = jax.random.split(jax.random.fold_in(seeds[5], part), 6)
    state = centred(own_keys[0], (3, 2, KY, KZ, NG), 1.3, 6.0, ((2, 8), (3, 8)), jnp.float32)
    cotangent = centred(own_keys[1], (3, 2, KY, KZ, NG), 1.0, 6.0, ((2, 8), (3, 8)), jnp.float32)
    w_in = centred(seeds[2], (HID, FEAT), FEAT ** -0.5, 0.4375)
    b_in = centred(seeds[3], (HID,), 1.0, 5.0, (), jnp.float32)
    w_out = centred(seeds[4], (FEAT, HID), HID ** -0.5, 0.25)
    return dict(state=state, cotangent=cotangent, w_in=w_in, b_in=b_in, w_out=w_out)


NU_DT = 5e-05
TIME_STEP = 0.01
FORCING = 20.0

def angles(leading, trailing, length):
    product = leading[:, None] * trailing[None, :] % length
    phases = product.astype(jnp.float32) * (2.0 * math.pi / length)
    factor = 1.0 / math.sqrt(length)
    return (jnp.cos(phases) * factor, jnp.sin(phases) * factor)

def mode_ids(count, length):
    counter = jnp.arange(count, dtype=jnp.int32)
    return jnp.where(counter < count // 2, counter, counter + length - count).astype(jnp.int32)

def mode_table(modes, length, direction):
    cosine, sine_part = angles(modes, jnp.arange(length, dtype=jnp.int32), length)
    top_rows = jnp.stack([cosine, direction * sine_part], axis=1)
    low_rows = jnp.stack([-direction * sine_part, cosine], axis=1)
    return jnp.stack([top_rows, low_rows], axis=0).astype(jnp.bfloat16)

def complex_table(length, direction):
    return mode_table(jnp.arange(length, dtype=jnp.int32), length, direction)

def real_table(length, mode_count):
    cosine, sine_part = angles(jnp.arange(mode_count, dtype=jnp.int32), jnp.arange(length, dtype=jnp.int32), length)
    return jnp.stack([cosine, -sine_part], axis=0).astype(jnp.bfloat16)

def rounded(values):
    return lax.optimization_barrier(values.astype(jnp.bfloat16)).astype(jnp.float32)

def signed(counter, length):
    return jnp.where(counter < length // 2, counter, counter - length).astype(jnp.float32)

def factors(ky_ids, kz_ids, length, ky_count):
    cutoff = length // 3
    wave_y = signed(ky_ids, ky_count)[:, None, None]
    wave_z = kz_ids.astype(jnp.float32)[None, :, None]
    wave_x = signed(jnp.arange(length, dtype=jnp.int32), length)[None, None, :]
    retained = ((jnp.abs(wave_x) <= cutoff) & (jnp.abs(wave_y) <= cutoff) & (wave_z <= cutoff)).astype(jnp.float32)
    square = wave_x * wave_x + wave_y * wave_y + wave_z * wave_z
    damping = jnp.exp(-NU_DT * square)
    weight = jnp.where(kz_ids[None, :, None] == 0, 1.0, 2.0).astype(jnp.float32)
    return ((wave_x, wave_y, wave_z), retained, damping, weight, square)

def cross(former, latter):
    return [former[1] * latter[2] - former[2] * latter[1], former[2] * latter[0] - former[0] * latter[2], former[0] * latter[1] - former[1] * latter[0]]

def curl_modes(waves, spectra):
    real_part = cross(waves, [spectra[slot, 0] for slot in range(3)])
    imag_part = cross(waves, [spectra[slot, 1] for slot in range(3)])
    return jnp.stack([jnp.stack([-imag_part[slot], real_part[slot]]) for slot in range(3)])

def project(waves, square, spectra):
    dotted = waves[0] * spectra[0] + waves[1] * spectra[1] + waves[2] * spectra[2]
    along_k = dotted / jnp.maximum(square, 1.0)
    return jnp.stack([spectra[slot] - waves[slot] * along_k for slot in range(3)])

def to_physical(spectra):
    length = spectra.shape[4]
    inverse = complex_table(length, 1.0).astype(jnp.float32)
    y_inverse = mode_table(mode_ids(spectra.shape[2], length), length, 1.0).astype(jnp.float32)
    z_table = real_table(length, spectra.shape[3]).astype(jnp.float32)
    sectioned = rounded(spectra)
    sectioned = rounded(jnp.einsum('cramn,rnsx->csamx', sectioned, inverse, precision=lax.Precision.HIGHEST))
    sectioned = rounded(jnp.einsum('csamx,saty->ctmxy', sectioned, y_inverse, precision=lax.Precision.HIGHEST))
    return jnp.einsum('ctmxy,tmz->cxyz', sectioned, z_table, precision=lax.Precision.HIGHEST).astype(jnp.bfloat16)

def to_spectral(field):
    length = field.shape[3]
    forward = complex_table(length, -1.0).astype(jnp.float32)
    y_forward = mode_table(mode_ids(KY, length), length, -1.0).astype(jnp.float32).transpose(0, 3, 2, 1)
    z_table = real_table(length, KZ).astype(jnp.float32)
    sectioned = field.astype(jnp.float32)
    sectioned = rounded(jnp.einsum('cxyz,rmz->crmxy', sectioned, z_table, precision=lax.Precision.HIGHEST))
    sectioned = rounded(jnp.einsum('crmxy,rysa->csamx', sectioned, y_forward, precision=lax.Precision.HIGHEST))
    return jnp.einsum('csamx,sxtn->ctamn', sectioned, forward, precision=lax.Precision.HIGHEST)

def to_boxes(field):
    channels, span_x, span_y, span_z = field.shape
    tiles = field.reshape(channels, span_x // PATCH, PATCH, span_y // PATCH, PATCH, span_z // PATCH, PATCH)
    return tiles.transpose(0, 2, 4, 6, 1, 3, 5).reshape(channels * PATCH ** 3, -1)

def from_boxes(box_values, layout):
    channels, span_x, span_y, span_z = layout
    tiles = box_values.reshape(channels, PATCH, PATCH, PATCH, span_x // PATCH, span_y // PATCH, span_z // PATCH)
    return tiles.transpose(0, 4, 1, 5, 2, 6, 3).reshape(layout)

def closure_terms(velocity, force_adj, w_in, b_in, w_out):
    features = to_boxes(velocity)
    adjoints = to_boxes(force_adj)
    pre_act = jnp.dot(w_in, features, preferred_element_type=jnp.float32) + b_in[:, None]
    hidden = jax.nn.silu(pre_act).astype(jnp.bfloat16)
    sigmoid = jax.nn.sigmoid(pre_act)
    hidden_adj = FORCING * jnp.dot(w_out.T, adjoints, preferred_element_type=jnp.float32)
    pre_adj = (hidden_adj * sigmoid * (1.0 + pre_act * (1.0 - sigmoid))).astype(jnp.bfloat16)
    grad_in = jnp.dot(pre_adj, features.T, preferred_element_type=jnp.float32)
    grad_out = FORCING * jnp.dot(adjoints, hidden.T, preferred_element_type=jnp.float32)
    grad_bias = lax.optimization_barrier(jnp.sum(pre_adj.astype(jnp.float32), axis=1))[None, :]
    feat_adj = jnp.dot(w_in.T, pre_adj, preferred_element_type=jnp.float32)
    return (from_boxes(feat_adj, velocity.shape), grad_in, grad_out, grad_bias)

def pointwise(feat_adj, velocity, vorticity, force_adj):
    vel_list = [velocity[slot].astype(jnp.float32) for slot in range(3)]
    vort_list = [vorticity[slot].astype(jnp.float32) for slot in range(3)]
    force_list = [force_adj[slot].astype(jnp.float32) for slot in range(3)]
    turned = cross(vort_list, force_list)
    vel_adj = jnp.stack([feat_adj[slot] + turned[slot] for slot in range(3)]).astype(jnp.bfloat16)
    vort_adj = jnp.stack(cross(force_list, vel_list)).astype(jnp.bfloat16)
    return (vel_adj, vort_adj)

def reference(state, cotangent, w_in, b_in, w_out):
    waves, retained, damping, weight, square = factors(jnp.arange(KY, dtype=jnp.int32), jnp.arange(KZ, dtype=jnp.int32), NG, KY)
    kept = retained * state
    spectra = weight * jnp.concatenate([kept, curl_modes(waves, kept)], axis=0)
    fields = to_physical(spectra)
    velocity, vorticity = (fields[:3], fields[3:])
    force_spec = TIME_STEP * retained * project(waves, square, damping * cotangent)
    force_adj = to_physical(force_spec)
    feat_adj, grad_in, grad_out, grad_bias = closure_terms(velocity, force_adj, w_in, b_in, w_out)
    vel_adj, vort_adj = pointwise(feat_adj, velocity, vorticity, force_adj)
    spectral = to_spectral(jnp.concatenate([vel_adj, vort_adj], axis=0))
    state_grad = damping * cotangent + weight * retained * (spectral[:3] + curl_modes(waves, spectral[3:]))
    return (state_grad, grad_in, grad_out, grad_bias)
```

```python
import numpy as np

import jax
import jax.numpy as jnp
from jax import lax
from jax.experimental import pallas as pl
from jax.experimental.pallas import tpu as pltpu
from jax.sharding import PartitionSpec as P

F32 = jnp.float32
BF16 = jnp.bfloat16
MESH = pl.DeviceIdType.MESH
NN = (((1,), (0,)), ((), ()))
NT = (((1,), (1,)), ((), ()))
TN = (((0,), (0,)), ((), ()))

NG, KY, KZ, HID, FEAT = 256, 192, 96, 512, 192
CUT = NG // 3
NU_DT = 5e-05
TIME_STEP = 0.01
FORCING = 20.0
NDEV = 64
WY, WZ = 24, 12
SLOT = 48
INV = 8
INV_W = INV * 3 * SLOT
FWD_W = 16 * SLOT
SEND_W = FWD_W + 256
PITCH = 72


def dot(a, b, dims=NN, **kw):
    return lax.dot_general(a, b, dims, preferred_element_type=F32, **kw)


def make_tables():
    bf = jnp.bfloat16

    def angle(k, x):
        theta = 2 * np.pi * ((np.asarray(k)[:, None] % NG) * np.asarray(x)[None, :] % NG) / NG
        return np.cos(theta) / np.sqrt(NG), np.sin(theta) / np.sqrt(NG)

    order_x = np.arange(NG).reshape(64, 4).T.reshape(-1)
    c, s = angle(order_x, np.arange(NG))
    tx = np.concatenate([c, -s], axis=1)
    order = np.arange(NG).reshape(64, 4).T.reshape(-1)
    ids = np.arange(KY)
    ky = np.where(ids < KY // 2, ids, ids - KY)
    c, s = angle(ky, order)
    top = np.concatenate([c, s], axis=1).reshape(8, 1, WY, 2 * NG)
    low = np.concatenate([-s, c], axis=1).reshape(8, 1, WY, 2 * NG)
    kcol = ky.reshape(8, 1, WY, 1)
    ty = np.concatenate([top, low], axis=1).reshape(2 * KY, 2 * NG)
    tyk = np.concatenate([-kcol * low, kcol * top], axis=1).reshape(2 * KY, 2 * NG)
    kz = (np.arange(8)[None, :, None] * WZ + np.arange(3)[:, None, None] * 4 + np.arange(4)[None, None, :]).reshape(-1)
    c, s = angle(order, kz)
    tz = np.concatenate([c, -s], axis=1)
    kk = np.concatenate([kz, kz])[None, :]
    tzk = np.concatenate([s, c], axis=1) * kk
    perm = np.zeros((FEAT, FEAT), np.float32)
    src = np.arange(FEAT).reshape(3, 4, 4, 4).transpose(2, 0, 1, 3).reshape(-1)
    perm[src, np.arange(FEAT)] = 1.0
    back = np.zeros((256, 256), np.float32)
    back[:FEAT, :FEAT] = perm.T
    back[FEAT, FEAT] = 1.0
    two = lambda t: np.concatenate([t, t], axis=0)
    arrays = dict(tx=tx, ty=two(ty), tyk=two(tyk), tz=tz, tzk=tzk, tzt=tz.T, tzkt=tzk.T, perm=perm)
    out = {k: np.asarray(v, np.float32).astype(bf) for k, v in arrays.items()}
    out["back"] = back
    return out


def waves_of(m, j, l):
    kz_id = l * WZ + m
    kz = kz_id.astype(F32)
    a = lax.broadcasted_iota(jnp.int32, (WY, NG), 0) + j * WY
    n = lax.broadcasted_iota(jnp.int32, (WY, NG), 1)
    ky = jnp.where(a < KY // 2, a, a - KY).astype(F32)
    kx = jnp.where(n < NG // 2, n, n - NG).astype(F32)
    keep = (jnp.abs(kx) <= CUT) & (jnp.abs(ky) <= CUT) & (kz <= float(CUT))
    retained = keep.astype(F32)
    square = kx * kx + ky * ky + kz * kz
    damping = jnp.exp(-NU_DT * square)
    weight = jnp.where(kz_id == 0, 1.0, 2.0).astype(F32)
    return kx, ky, kz, retained, square, damping, weight


def spectral_out(state_ref, cot_ref, tx_ref, a_ref, s_ref, a32):
    j, l = lax.axis_index("px"), lax.axis_index("py")

    def one(mp, carry):
        for mh in range(3):
            m = mh * 4 + mp
            kx, ky, kz, retained, square, damping, weight = waves_of(m, j, l)
            scale = weight * retained
            v = [[scale * state_ref[c, r, m] for r in range(2)] for c in range(3)]
            wy = [-(kz * v[0][1] - kx * v[2][1]), kz * v[0][0] - kx * v[2][0]]
            wz = [-(kx * v[1][1] - ky * v[0][1]), kx * v[1][0] - ky * v[0][0]]
            inverse = 1.0 / jnp.maximum(square, 1.0)
            fscale = TIME_STEP * retained
            force = [[None, None], [None, None], [None, None]]
            for r in range(2):
                g = [damping * cot_ref[c, r, m] for c in range(3)]
                along = (kx * g[0] + ky * g[1] + kz * g[2]) * inverse
                for c, k in enumerate((kx, ky, kz)):
                    force[c][r] = fscale * (g[c] - k * along)
            for f, (re, im) in enumerate([v[0], v[1], v[2], wy, wz, *force]):
                g, pp = divmod(f * 3 + mh, 8)
                top = jnp.concatenate([re, im], axis=1)
                low = jnp.concatenate([im, -re], axis=1)
                block = jnp.concatenate([top, low], axis=0).astype(BF16)
                row = pl.multiple_of(g * 384 + lax.rem(pp + j, 8) * SLOT, 16)
                s_ref[pl.ds(row, SLOT), :] = block
        for first in range(0, INV_W, 256):
            width = min(256, INV_W - first)
            out = dot(tx_ref[...], s_ref[first : first + width, :], NT)
            for c in range(width // 128):
                for xx in range(4):
                    a32[first // 128 + c, pl.ds(mp * 4 + xx, 64, stride=24), :] = out[
                        xx * 64 : (xx + 1) * 64, c * 128 : (c + 1) * 128
                    ]
        return carry

    lax.fori_loop(0, 4, one, 0)

    def pack(d, carry):
        row = pl.multiple_of(d * 24, 8)
        for c in range(INV_W // 128):
            a_ref[d, :, c * 128 : (c + 1) * 128] = a32[c, pl.ds(row, 16), :].astype(BF16)
        return carry

    lax.fori_loop(0, 64, pack, 0)


def exchange(x_ref, o_ref, send_sem, recv_sem, own_sem):
    px, py = lax.axis_index("px"), lax.axis_index("py")
    me = px * 8 + py

    def peer(k):
        t = lax.rem(me + k, NDEV)
        return t, {"px": t // 8, "py": lax.rem(t, 8)}

    barrier = pltpu.get_barrier_semaphore()

    def greet(k, carry):
        pl.semaphore_signal(barrier, inc=1, device_id=peer(k)[1], device_id_type=MESH)
        return carry

    lax.fori_loop(1, NDEV, greet, 0)
    own = pltpu.make_async_copy(x_ref.at[me], o_ref.at[me], own_sem)
    own.start()
    pl.semaphore_wait(barrier, NDEV - 1)

    def send(k, carry):
        t, where = peer(k)
        pltpu.make_async_remote_copy(
            src_ref=x_ref.at[t],
            dst_ref=o_ref.at[me],
            send_sem=send_sem,
            recv_sem=recv_sem,
            device_id=where,
            device_id_type=MESH,
        ).start()
        return carry

    lax.fori_loop(1, NDEV, send, 0)
    own.wait()
    rest = pl.ds(0, NDEV - 1)
    whole = pltpu.make_async_remote_copy(
        src_ref=x_ref.at[rest],
        dst_ref=o_ref.at[rest],
        send_sem=send_sem,
        recv_sem=recv_sem,
        device_id=peer(1)[1],
        device_id_type=MESH,
    )
    whole.wait_send()
    whole.wait_recv()


def lane_select(lane, v, pick):
    slots = [q for q in range(8) if q * SLOT < (v + 1) * 128 and (q + 1) * SLOT > v * 128]
    value = pick(slots[0])
    for q in slots[1:]:
        value = jnp.where(lane >= float(q * SLOT - v * 128), pick(q), value)
    return value


def cross(a, b):
    return [a[1] * b[2] - a[2] * b[1], a[2] * b[0] - a[0] * b[2], a[0] * b[1] - a[1] * b[0]]


def slab(
    r_ref, ty_ref, tyk_ref, tz_ref, tzk_ref, tzt_ref, tzkt_ref, perm_ref, w_in_t, b_ref, w_out,
    o_ref,
    lhs, y32, v32, va32, l32, o16, win, wint, woutt, gin, gout,
):
    lane = lax.broadcasted_iota(jnp.int32, (1, 128), 1).astype(BF16)
    lane = jnp.broadcast_to(lane, (128, 128))

    perm = perm_ref[...]
    win[...] = dot(w_in_t[...], perm, TN).astype(BF16)
    wint[...] = dot(perm, w_in_t[...], TN).astype(BF16)
    woutt[...] = dot(w_out[...], perm, TN).astype(BF16)

    for pp in range(8):
        first = (8 - pp) * SLOT
        for g in range(3):
            for v in range(3):
                at = g * 384 + v * 128
                lhs[g * 128 : (g + 1) * 128, v * 128 : (v + 1) * 128] = lane_select(
                    lane, v, lambda q: r_ref[(q - pp) % 8, :, at : at + 128]
                )
        out = dot(lhs[...], ty_ref[first : first + 384, :])
        for c in range(4):
            y32[c, pp * 384 : (pp + 1) * 384, :] = out[:, c * 128 : (c + 1) * 128]
        for mh in range(3):
            g, own = divmod(2 * 3 + mh, 8)
            if own == pp:
                out = -dot(lhs[g * 128 : (g + 1) * 128, :], tyk_ref[first : first + 384, :])
                row = 3072 + mh * 128
                for c in range(4):
                    y32[c, row : row + 128, :] = out[:, c * 128 : (c + 1) * 128]

    def block_of(f, mh):
        if f == INV:
            return 24 + mh
        g, pp = divmod(f * 3 + mh, 8)
        return pp * 3 + g

    def columns(f, xx):
        parts = []
        for t in range(2):
            for mh in range(3):
                rows = pl.ds(block_of(f, mh) * 128 + xx, 32, stride=4)
                parts.append(jnp.concatenate([y32[2 * t, rows, :], y32[2 * t + 1, rows, :]], axis=1))
        return jnp.concatenate(parts, axis=0).astype(BF16)

    def along_z(xx, carry):
        for slot, f in enumerate((0, 1, 2, INV, 3, 4, 5, 6, 7)):
            out = dot(tz_ref[...], columns(f, xx))
            if f == INV:
                out = out + dot(tzk_ref[...], columns(1, xx))
            out = out.astype(BF16).astype(F32)
            for dz in range(4):
                row = pl.multiple_of((slot * 16 + xx * 4 + dz) * PITCH, 8)
                for h in range(2):
                    v32[h, pl.ds(row, 64), :] = out[dz * 64 : (dz + 1) * 64, h * 128 : (h + 1) * 128]
        return carry

    lax.fori_loop(0, 4, along_z, 0)

    gin[...] = jnp.zeros_like(gin)
    gout[...] = jnp.zeros_like(gout)
    ones = jnp.ones((64, 256), BF16)

    def rows_of(field, bz):
        rows = pl.ds(field * 16 * PITCH + bz, 48, stride=PITCH)
        return [v32[h, rows, :] for h in range(2)]

    def boxes(planes):
        parts = []
        for dy in range(4):
            h, at = dy // 2, dy % 2 * 64
            parts.append(jnp.concatenate([p[h][:, at : at + 64] for p in planes], axis=1))
        return jnp.concatenate(parts, axis=0).astype(BF16)

    def closure(group, carry):
        bzs = [group * 4 + b for b in range(4)]
        velocity = [rows_of(0, bz) for bz in bzs]
        force = [rows_of(6, bz) for bz in bzs]
        features = boxes(velocity)
        adjoints = boxes(force)
        pre = dot(win[...], features) + b_ref[...]
        sigmoid = 1.0 / (1.0 + jnp.exp(-pre))
        hidden = (pre * sigmoid).astype(BF16)
        hidden_adj = FORCING * dot(woutt[...], adjoints)
        pre_adj = (hidden_adj * sigmoid * (1.0 + pre * (1.0 - sigmoid))).astype(BF16)
        gin[...] += dot(pre_adj, jnp.concatenate([features, ones], axis=0), NT)
        gout[:, 0:FEAT] += dot(hidden, adjoints, NT)
        feat_adj = dot(wint[...], pre_adj)
        for b, bz in enumerate(bzs):
            spin = rows_of(3, bz)
            for h in range(2):
                back = jnp.concatenate(
                    [feat_adj[dy * 48 : (dy + 1) * 48, b * 64 : (b + 1) * 64] for dy in (2 * h, 2 * h + 1)], axis=1
                )
                pick = lambda a: [a[c * 16 : (c + 1) * 16, :] for c in range(3)]
                vel, vor, frc = pick(velocity[b][h]), pick(spin[h]), pick(force[b][h])
                first = jnp.concatenate(cross(vor, frc), axis=0) + back
                second = jnp.concatenate(cross(frc, vel), axis=0)
                va32[h, pl.ds(bz, 48, stride=PITCH), :] = first
                va32[h, pl.ds(48 * PITCH + bz, 48, stride=PITCH), :] = second
        return carry

    lax.fori_loop(0, 16, closure, 0)

    def field_of(c, xx):
        parts = []
        for dz in range(4):
            row = pl.multiple_of((c * 16 + xx * 4 + dz) * PITCH, 8)
            parts.append(jnp.concatenate([va32[0, pl.ds(row, 64), :], va32[1, pl.ds(row, 64), :]], axis=1))
        return jnp.concatenate(parts, axis=0).astype(BF16)

    def put(block, value, xx):
        for r in range(2):
            for mh in range(3):
                for h in range(2):
                    l32[2 * r + h, pl.ds(block(mh) * 128 + xx, 32, stride=4), :] = value[
                        r * 96 + mh * 32 : r * 96 + (mh + 1) * 32, h * 128 : (h + 1) * 128
                    ]

    def main(f):
        def block(mh):
            g, pp = divmod(f * 3 + mh, 8)
            return pp * 2 + g
        return block

    def extra(f):
        return lambda mh: 16 + f * 3 + mh

    def forward_z(xx, carry):
        vort = field_of(4, xx)
        tzt = tzt_ref[...]
        tzkt = tzkt_ref[...]
        put(main(0), dot(tzt, field_of(0, xx)) - dot(tzkt, vort), xx)
        put(main(3), dot(tzt, vort), xx)
        vort = field_of(3, xx)
        put(main(2), dot(tzt, field_of(1, xx)) + dot(tzkt, vort), xx)
        put(extra(1), -dot(tzt, vort), xx)
        put(main(1), dot(tzt, field_of(2, xx)), xx)
        value = dot(tzt, field_of(5, xx))
        put(main(4), value, xx)
        put(extra(0), value, xx)
        return carry

    for c in range(4):
        l32[c, 15 * 128 : 16 * 128, :] = jnp.zeros((128, 128), F32)
    lax.fori_loop(0, 4, forward_z, 0)

    for pp in range(8):
        first = (8 - pp) * SLOT
        rows = slice(pp * 256, (pp + 1) * 256)
        left = jnp.concatenate([l32[c, rows, :] for c in range(4)], axis=1).astype(BF16)
        out = dot(left, ty_ref[first : first + 384, :], NT)
        if pp < 6:
            rows = slice((16 + pp) * 128, (17 + pp) * 128)
            left = jnp.concatenate([l32[c, rows, :] for c in range(4)], axis=1).astype(BF16)
            more = dot(left, tyk_ref[first : first + 384, :], NT)
            o16[pp, 0:128, :] = (out[0:128] + more).astype(BF16)
            o16[pp, 128:256, :] = out[128:256].astype(BF16)
        else:
            o16[pp] = out.astype(BF16)
    for j in range(8):
        for g in range(2):
            for v in range(3):
                at = g * 384 + v * 128
                o_ref[j, :, at : at + 128] = lane_select(
                    lane, v, lambda q: o16[(q - j) % 8, g * 128 : (g + 1) * 128, v * 128 : (v + 1) * 128]
                )
    for j in range(8):
        rows = slice(j * 64, (j + 1) * 64)
        both = jnp.concatenate([gin[rows, :].reshape(8, 8, 256), (FORCING * gout[rows, :]).reshape(8, 8, 256)], axis=1)
        o_ref[j, :, FWD_W:SEND_W] = both.reshape(128, 256).astype(BF16)


def spectral_in(q_ref, cot_ref, tx_ref, back_ref, out_ref, grad_ref, q32, o32):
    j, l = lax.axis_index("px"), lax.axis_index("py")

    def unpack(d, total):
        row = pl.multiple_of(d * 24, 8)
        for c in range(FWD_W // 128):
            q32[c, pl.ds(row, 16), :] = q_ref[d, :, c * 128 : (c + 1) * 128].astype(F32)
        return total + q_ref[d, :, FWD_W:SEND_W].astype(F32)

    total = lax.fori_loop(0, 64, unpack, jnp.zeros((16, 256), F32))
    grad_ref[...] = dot(total, back_ref[...], precision=lax.Precision.HIGHEST)

    def one(mp, carry):
        for c in range(FWD_W // 128):
            left = jnp.concatenate([q32[c, pl.ds(mp * 4 + xx, 64, stride=24), :] for xx in range(4)], axis=0)
            o32[c * 128 : (c + 1) * 128, :] = dot(left.astype(BF16), tx_ref[...], TN)
        for mh in range(3):
            m = mh * 4 + mp
            kx, ky, kz, retained, square, damping, weight = waves_of(m, j, l)
            scale = weight * retained
            parts = []
            for f in range(5):
                g, pp = divmod(f * 3 + mh, 8)
                row = pl.multiple_of(g * 384 + lax.rem(pp + j, 8) * SLOT, 8)
                re = o32[pl.ds(row, WY), :]
                im = o32[pl.ds(row + WY, WY), :]
                parts.append((re[:, :NG] - im[:, NG:], im[:, :NG] + re[:, NG:]))
            ax, az, ay, wy, wz = parts
            spec = [
                ax,
                (ay[0] + kx * wz[1], ay[1] - kx * wz[0]),
                (az[0] - kx * wy[1], az[1] + kx * wy[0]),
            ]
            for c in range(3):
                for r in range(2):
                    out_ref[c, r, m] = damping * cot_ref[c, r, m] + scale * spec[c][r]
        return carry

    lax.fori_loop(0, 4, one, 0)


VMEM = pl.BlockSpec(memory_space=pltpu.VMEM)
ANY = pl.BlockSpec(memory_space=pl.ANY)
LIMIT = 60 * 1024 * 1024


def call(body, outs, ins, scratch, **params):
    return pl.pallas_call(
        body,
        out_shape=outs,
        in_specs=[VMEM] * ins,
        out_specs=jax.tree.map(lambda _: VMEM, outs),
        scratch_shapes=scratch,
        compiler_params=pltpu.CompilerParams(vmem_limit_bytes=LIMIT, **params),
    )


def all_to_all(x, number):
    return pl.pallas_call(
        exchange,
        out_shape=jax.ShapeDtypeStruct(x.shape, x.dtype),
        in_specs=[ANY],
        out_specs=ANY,
        scratch_shapes=[pltpu.SemaphoreType.DMA] * 3,
        compiler_params=pltpu.CompilerParams(collective_id=number, has_side_effects=True),
    )(x)


def shards(state, cotangent, w_in, b_in, w_out):
    t = {k: jnp.asarray(v) for k, v in make_tables().items()}
    state = state.transpose(0, 1, 3, 2, 4)
    cotangent = cotangent.transpose(0, 1, 3, 2, 4)
    sds = jax.ShapeDtypeStruct
    sent = call(
        spectral_out,
        sds((NDEV, 16, INV_W), BF16),
        3,
        [pltpu.VMEM((INV_W, 2 * NG), BF16), pltpu.VMEM((INV_W // 128, 64 * 24, 128), F32)],
    )(state, cotangent, t["tx"])
    got = all_to_all(sent, 0).reshape(8, 128, INV_W)
    back = call(
        slab,
        sds((8, 128, SEND_W), BF16),
        11,
        [
            pltpu.VMEM((384, 384), BF16),
            pltpu.VMEM((4, 27 * 128, 128), F32),
            pltpu.VMEM((2, 144 * PITCH, 128), F32),
            pltpu.VMEM((2, 96 * PITCH, 128), F32),
            pltpu.VMEM((4, 22 * 128, 128), F32),
            pltpu.VMEM((8, 256, 384), BF16),
            pltpu.VMEM((HID, FEAT), BF16),
            pltpu.VMEM((FEAT, HID), BF16),
            pltpu.VMEM((HID, FEAT), BF16),
            pltpu.VMEM((HID, 256), F32),
            pltpu.VMEM((HID, 256), F32),
        ],
    )(
        got, t["ty"], t["tyk"], t["tz"], t["tzk"], t["tzt"], t["tzkt"], t["perm"],
        w_in.T, b_in[:, None], w_out,
    )
    mine = all_to_all(back.reshape(NDEV, 16, SEND_W), 1)
    grad, sums = call(
        spectral_in,
        (sds((3, 2, WZ, WY, NG), F32), sds((16, 256), F32)),
        4,
        [pltpu.VMEM((FWD_W // 128, 64 * 24, 128), F32), pltpu.VMEM((FWD_W, 2 * NG), F32)],
    )(mine, cotangent, t["tx"], t["back"])
    return (
        grad.transpose(0, 1, 3, 2, 4),
        sums[0:8, 0:FEAT],
        sums[8:16, 0:FEAT].T,
        sums[0:8, FEAT][None, :],
    )


def solution(mesh):
    split = P("rep", None, "px", "py", None)
    both = ("px", "py")
    return jax.shard_map(
        shards,
        mesh=mesh,
        in_specs=(split, split, P(), P(), P()),
        out_specs=(split, P(both, "rep"), P("rep", both), P("rep", both)),
        check_vma=False,
    )
```

```python
import numpy as np

import jax
import jax.numpy as jnp
from jax import lax
from jax.experimental import pallas as pl
from jax.experimental.pallas import tpu as pltpu
from jax.sharding import PartitionSpec as P

F32 = jnp.float32
BF16 = jnp.bfloat16
MESH = pl.DeviceIdType.MESH
NN = (((1,), (0,)), ((), ()))
NT = (((1,), (1,)), ((), ()))
TN = (((0,), (0,)), ((), ()))

NG, KY, KZ, HID, FEAT = 256, 192, 96, 512, 192
CUT = NG // 3
NU_DT = 5e-05
TIME_STEP = 0.01
FORCING = 20.0
NDEV = 64
WY, WZ = 24, 12
SLOT = 48
ROW = 8 * SLOT
INV = 8
FWD = 2
PITCH = 72


def dot(a, b, dims=NN, **kw):
    return lax.dot_general(a, b, dims, preferred_element_type=F32, **kw)


def make_tables():
    bf = jnp.bfloat16

    def angle(k, x):
        theta = 2 * np.pi * ((np.asarray(k)[:, None] % NG) * np.asarray(x)[None, :] % NG) / NG
        return np.cos(theta) / np.sqrt(NG), np.sin(theta) / np.sqrt(NG)

    order_x = np.arange(NG).reshape(64, 4).T.reshape(-1)
    c, s = angle(order_x, np.arange(NG))
    tx = np.concatenate([c, -s], axis=1)
    order = np.arange(NG).reshape(64, 4).T.reshape(-1)
    ids = np.arange(KY)
    ky = np.where(ids < KY // 2, ids, ids - KY)
    c, s = angle(ky, order)
    top = np.concatenate([c, s], axis=1).reshape(8, 1, WY, 2 * NG)
    low = np.concatenate([-s, c], axis=1).reshape(8, 1, WY, 2 * NG)
    kcol = ky.reshape(8, 1, WY, 1)
    ty = np.concatenate([top, low], axis=1).reshape(2 * KY, 2 * NG)
    tyk = np.concatenate([-kcol * low, kcol * top], axis=1).reshape(2 * KY, 2 * NG)
    kz = (np.arange(8)[None, :, None] * WZ + np.arange(3)[:, None, None] * 4 + np.arange(4)[None, None, :]).reshape(-1)
    c, s = angle(order, kz)
    tz = np.concatenate([c, -s], axis=1)
    kk = np.concatenate([kz, kz])[None, :]
    tzk = np.concatenate([s, c], axis=1) * kk
    perm = np.zeros((FEAT, FEAT), np.float32)
    src = np.arange(FEAT).reshape(3, 4, 4, 4).transpose(2, 0, 1, 3).reshape(-1)
    perm[src, np.arange(FEAT)] = 1.0
    back = np.zeros((256, 256), np.float32)
    back[:FEAT, :FEAT] = perm.T
    back[FEAT, FEAT] = 1.0
    arrays = dict(tx=tx, ty=ty, tyk=tyk, tz=tz, tzk=tzk, tzt=tz.T, tzkt=tzk.T, perm=perm)
    out = {k: np.asarray(v, np.float32).astype(bf) for k, v in arrays.items()}
    out["back"] = back
    return out


def waves_of(m, j, l):
    kz_id = l * WZ + m
    kz = kz_id.astype(F32)
    a = lax.broadcasted_iota(jnp.int32, (WY, NG), 0) + j * WY
    n = lax.broadcasted_iota(jnp.int32, (WY, NG), 1)
    ky = jnp.where(a < KY // 2, a, a - KY).astype(F32)
    kx = jnp.where(n < NG // 2, n, n - NG).astype(F32)
    keep = (jnp.abs(kx) <= CUT) & (jnp.abs(ky) <= CUT) & (kz <= float(CUT))
    retained = keep.astype(F32)
    square = kx * kx + ky * ky + kz * kz
    damping = jnp.exp(-NU_DT * square)
    weight = jnp.where(kz_id == 0, 1.0, 2.0).astype(F32)
    return kx, ky, kz, retained, square, damping, weight


PART = 24
GRADS = INV * 3 // 8


def lane_select(lane, v, pick):
    slots = [q for q in range(8) if q * SLOT < (v + 1) * 128 and (q + 1) * SLOT > v * 128]
    value = pick(slots[0])
    for q in slots[1:]:
        value = jnp.where(lane >= float(q * SLOT - v * 128), pick(q), value)
    return value


def cross(a, b):
    return [a[1] * b[2] - a[2] * b[1], a[2] * b[0] - a[0] * b[2], a[0] * b[1] - a[1] * b[0]]


def main_kernel(
    state_ref, cot_ref, tx_ref, tz_ref, tzk_ref, tzt_ref, tzkt_ref, perm_ref, back_ref, w_in_t, b_ref, w_out,
    ty_hbm, tyk_hbm,
    out_ref, grad_ref,
    s_ref, flat, sent, got, v32, va32, l32, o16, back, mine, gsent, ggot, o32, ty_ref, tyk_ref,
    win, wint, woutt, gin, gout, table_sem, send_sem, recv_sem,
):
    j, l = lax.axis_index("px"), lax.axis_index("py")
    me = j * 8 + l
    x, core, z, y = j // 2, lax.rem(j, 2), l // 4, lax.rem(l, 4)

    def peer(k):
        k = k + jnp.where(k >= 11, 1, 0)
        i = lax.rem(k, 4)
        dx = jnp.where(i == 0, 1, jnp.where(i == 1, 3, jnp.where(i == 2, 2, 0)))
        dy = jnp.where(i == 0, 1, jnp.where(i == 1, 3, jnp.where(i == 2, 0, 2))) + lax.rem(k // 4, 4)
        tx = lax.rem(x + dx, 4)
        ty = lax.rem(y + dy, 4)
        tc = lax.rem(core + k // 16, 2)
        tz = lax.rem(z + k // 32, 2)
        px, py = tx * 2 + tc, tz * 4 + ty
        return px * 8 + py, {"px": px, "py": py}

    barrier = pltpu.get_barrier_semaphore()

    def greet(k, carry):
        pl.semaphore_signal(barrier, inc=1, device_id=peer(k)[1], device_id_type=MESH)
        return carry

    lax.fori_loop(0, NDEV - 1, greet, 0)
    half = 2 * KY
    loads = [
        pltpu.make_async_copy(src, dst.at[pl.ds(n * half, half)], table_sem.at[k * 2 + n])
        for k, (src, dst) in enumerate([(ty_hbm, ty_ref), (tyk_hbm, tyk_ref)])
        for n in range(2)
    ]
    for load in loads:
        load.start()

    def copy(src, dst, number, where):
        return pltpu.make_async_remote_copy(
            src_ref=src,
            dst_ref=dst,
            send_sem=send_sem.at[number],
            recv_sem=recv_sem.at[number],
            device_id=where,
            device_id_type=MESH,
        )

    def send_all(src, dst, number):
        def send(k, carry):
            t, where = peer(k)
            copy(src.at[t], dst.at[me], number, where).start()
            return carry

        dst[pl.ds(me, 1)] = src[pl.ds(me, 1)]
        lax.fori_loop(0, NDEV - 1, send, 0)

    def whole(src, dst, number):
        rest = pl.ds(0, NDEV - 1)
        return copy(src.at[rest], dst.at[rest], number, peer(0)[1])

    for group in range(3):

        def one(mp, carry):
            for mh in range(3):
                fields = [f for f in range(INV) if (f * 3 + mh) // 8 == group]
                m = mh * 4 + mp
                kx, ky, kz, retained, square, damping, weight = waves_of(m, j, l)
                value = {}
                if any(f >= 3 for f in fields):
                    scale = weight * retained
                    v = [[scale * state_ref[c, r, m] for r in range(2)] for c in range(3)]
                    value.update({3 + c: v[c] for c in range(3)})
                    value[6] = [-(kz * v[0][1] - kx * v[2][1]), kz * v[0][0] - kx * v[2][0]]
                    value[7] = [-(kx * v[1][1] - ky * v[0][1]), kx * v[1][0] - ky * v[0][0]]
                if any(f < 3 for f in fields):
                    inverse = 1.0 / jnp.maximum(square, 1.0)
                    scale = TIME_STEP * retained
                    force = [[], [], []]
                    for r in range(2):
                        w = [damping * cot_ref[c, r, m] for c in range(3)]
                        along = (kx * w[0] + ky * w[1] + kz * w[2]) * inverse
                        for c, k in enumerate((kx, ky, kz)):
                            force[c].append(scale * (w[c] - k * along))
                    value.update({c: force[c] for c in range(3)})
                for f in fields:
                    re, im = value[f]
                    top = jnp.concatenate([re, im], axis=1)
                    low = jnp.concatenate([im, -re], axis=1)
                    row = pl.multiple_of(lax.rem((f * 3 + mh) % 8 + j, 8) * SLOT, 16)
                    s_ref[pl.ds(row, SLOT), :] = jnp.concatenate([top, low], axis=0).astype(BF16)
            for first in range(0, ROW, 256):
                width = min(256, ROW - first)
                out = dot(tx_ref[...], s_ref[first : first + width, :], NT)
                for c in range(width // 128):
                    for xx in range(4):
                        base = (first // 128 + c) * NDEV * PART
                        flat[pl.ds(base + mp * 4 + xx, NDEV, stride=PART), :] = out[
                            xx * 64 : (xx + 1) * 64, c * 128 : (c + 1) * 128
                        ]
            return carry

        lax.fori_loop(0, 4, one, 0)

        def pack(d, carry):
            for c in range(3):
                row = pl.multiple_of(c * NDEV * PART + d * PART, 8)
                sent[group, d, :, c * 128 : (c + 1) * 128] = flat[pl.ds(row, 16), :].astype(BF16)
            return carry

        lax.fori_loop(0, NDEV, pack, 0, unroll=4)
        if group == 0:
            pl.semaphore_wait(barrier, NDEV - 1)
        send_all(sent.at[group], got.at[group], group)

    lane = lax.broadcasted_iota(jnp.int32, (1, 128), 1).astype(BF16)
    lane = jnp.broadcast_to(lane, (128, 128))

    perm = perm_ref[...]
    win[...] = dot(w_in_t[...], perm, TN).astype(BF16)
    wint[...] = dot(perm, w_in_t[...], TN).astype(BF16)
    woutt[...] = dot(w_out[...], perm, TN).astype(BF16)
    gin[...] = jnp.zeros_like(gin)
    gout[...] = jnp.zeros_like(gout)
    for c in range(4):
        l32[(c * 22 + 15) * 128 : (c * 22 + 16) * 128, :] = jnp.zeros((128, 128), F32)
    for load in loads:
        load.wait()

    BLOCKS = 27

    def along_y(group):
        for pp in range(8):
            first = (8 - pp) * SLOT
            parts = []
            for v in range(3):
                pick = lambda q: got[group, (q - pp) % 8 * 8 : (q - pp) % 8 * 8 + 8, :, v * 128 : (v + 1) * 128].reshape(128, 128)
                parts.append(lane_select(lane, v, pick))
            left = jnp.concatenate(parts, axis=1)
            todo = [(pp * 3 + group, dot(left, ty_ref[first : first + 2 * KY, :]))]
            f, mh = divmod(group * 8 + pp, 3)
            if f == 5:
                todo.append((24 + mh, -dot(left, tyk_ref[first : first + 2 * KY, :])))
            for block, out in todo:
                for c in range(4):
                    row = (c * BLOCKS + block) * 128
                    flat[row : row + 128, :] = out[:, c * 128 : (c + 1) * 128]

    def columns(f, xx):
        parts = []
        for t in range(2):
            for mh in range(3):
                g, pp = divmod(f * 3 + mh, 8)
                block = 24 + mh if f == INV else pp * 3 + g
                lanes = [
                    flat[pl.ds(((2 * t + h) * BLOCKS + block) * 128 + xx, 32, stride=4), :] for h in range(2)
                ]
                parts.append(jnp.concatenate(lanes, axis=1))
        return jnp.concatenate(parts, axis=0).astype(BF16)

    def along_z(fields):
        def one(xx, carry):
            for slot, f in fields:
                out = dot(tz_ref[...], columns(f, xx))
                if f == INV:
                    out = out + dot(tzk_ref[...], columns(4, xx))
                out = out.astype(BF16).astype(F32)
                for dz in range(4):
                    row = pl.multiple_of((slot * 16 + xx * 4 + dz) * PITCH, 8)
                    for h in range(2):
                        v32[h, pl.ds(row, 64), :] = out[dz * 64 : (dz + 1) * 64, h * 128 : (h + 1) * 128]
            return carry

        lax.fori_loop(0, 4, one, 0)

    for group, fields in enumerate([[(6, 0), (7, 1)], [(8, 2), (0, 3), (1, 4)], [(2, 5), (3, INV), (4, 6), (5, 7)]]):
        whole(sent.at[group], got.at[group], group).wait_recv()
        along_y(group)
        along_z(fields)

    ones = jnp.ones((64, 256), BF16)

    def rows_of(field, bz):
        rows = pl.ds(field * 16 * PITCH + bz, 48, stride=PITCH)
        return [v32[h, rows, :] for h in range(2)]

    def boxes(planes):
        parts = []
        for dy in range(4):
            h, at = dy // 2, dy % 2 * 64
            parts.append(jnp.concatenate([p[h][:, at : at + 64] for p in planes], axis=1))
        return jnp.concatenate(parts, axis=0).astype(BF16)

    def closure(group, carry):
        bzs = [group * 4 + b for b in range(4)]
        velocity = [rows_of(0, bz) for bz in bzs]
        force = [rows_of(6, bz) for bz in bzs]
        features = boxes(velocity)
        adjoints = boxes(force)
        pre = dot(win[...], features) + b_ref[...]
        sigmoid = 1.0 / (1.0 + jnp.exp(-pre))
        hidden = (pre * sigmoid).astype(BF16)
        hidden_adj = FORCING * dot(woutt[...], adjoints)
        pre_adj = (hidden_adj * sigmoid * (1.0 + pre * (1.0 - sigmoid))).astype(BF16)
        gin[...] += dot(pre_adj, jnp.concatenate([features, ones], axis=0), NT)
        gout[:, 0:FEAT] += dot(hidden, adjoints, NT)
        feat_adj = dot(wint[...], pre_adj)
        for b, bz in enumerate(bzs):
            spin = rows_of(3, bz)
            for h in range(2):
                lanes = [feat_adj[dy * 48 : (dy + 1) * 48, b * 64 : (b + 1) * 64] for dy in (2 * h, 2 * h + 1)]
                pick = lambda a: [a[c * 16 : (c + 1) * 16, :] for c in range(3)]
                vel, vor, frc = pick(velocity[b][h]), pick(spin[h]), pick(force[b][h])
                first = jnp.concatenate(cross(vor, frc), axis=0) + jnp.concatenate(lanes, axis=1)
                second = jnp.concatenate(cross(frc, vel), axis=0)
                va32[h, pl.ds(bz, 48, stride=PITCH), :] = first
                va32[h, pl.ds(48 * PITCH + bz, 48, stride=PITCH), :] = second
        return carry

    lax.fori_loop(0, 16, closure, 0)

    def slices(d, carry):
        rows = pl.ds(pl.multiple_of(d * 8, 8), 8)
        gsent[d] = jnp.concatenate([gin[rows, :], FORCING * gout[rows, :]], axis=0).astype(BF16)
        return carry

    lax.fori_loop(0, NDEV, slices, 0, unroll=4)
    send_all(gsent, ggot, GRADS)

    def field_of(c, xx):
        parts = []
        for dz in range(4):
            row = pl.multiple_of((c * 16 + xx * 4 + dz) * PITCH, 8)
            parts.append(jnp.concatenate([va32[0, pl.ds(row, 64), :], va32[1, pl.ds(row, 64), :]], axis=1))
        return jnp.concatenate(parts, axis=0).astype(BF16)

    def put(block, value, xx):
        for r in range(2):
            for mh in range(3):
                for h in range(2):
                    row = ((2 * r + h) * 22 + block(mh)) * 128 + xx
                    l32[pl.ds(row, 32, stride=4), :] = value[
                        r * 96 + mh * 32 : r * 96 + (mh + 1) * 32, h * 128 : (h + 1) * 128
                    ]

    def direct(f):
        def block(mh):
            g, pp = divmod(f * 3 + mh, 8)
            return pp * 2 + g

        return block

    def extra(f):
        return lambda mh: 16 + f * 3 + mh

    def forward_z(xx, carry):
        vort = field_of(4, xx)
        tzt = tzt_ref[...]
        tzkt = tzkt_ref[...]
        put(direct(0), dot(tzt, field_of(0, xx)) - dot(tzkt, vort), xx)
        put(direct(3), dot(tzt, vort), xx)
        vort = field_of(3, xx)
        put(direct(2), dot(tzt, field_of(1, xx)) + dot(tzkt, vort), xx)
        put(extra(1), -dot(tzt, vort), xx)
        put(direct(1), dot(tzt, field_of(2, xx)), xx)
        value = dot(tzt, field_of(5, xx))
        put(direct(4), value, xx)
        put(extra(0), value, xx)
        return carry

    lax.fori_loop(0, 4, forward_z, 0)

    def left_of(block, count):
        parts = [l32[(c * 22 + block) * 128 : (c * 22 + block + count) * 128, :] for c in range(4)]
        return jnp.concatenate(parts, axis=1).astype(BF16)

    for pp in range(8):
        first = (8 - pp) * SLOT
        out = dot(left_of(pp * 2, 2), ty_ref[first : first + 2 * KY, :], NT)
        if pp < 6:
            more = dot(left_of(16 + pp, 1), tyk_ref[first : first + 2 * KY, :], NT)
            o16[pp, 0:128, :] = (out[0:128] + more).astype(BF16)
            o16[pp, 128:256, :] = out[128:256].astype(BF16)
        else:
            o16[pp] = out.astype(BF16)
    for g in range(FWD):
        for to in range(8):
            for v in range(3):
                pick = lambda q: o16[(q - to) % 8, g * 128 : (g + 1) * 128, v * 128 : (v + 1) * 128]
                back[g, to * 8 : to * 8 + 8, :, v * 128 : (v + 1) * 128] = lane_select(lane, v, pick).reshape(8, 16, 128)
        send_all(back.at[g], mine.at[g], GRADS + 1 + g)

    whole(gsent, ggot, GRADS).wait_recv()
    total = lax.fori_loop(0, NDEV, lambda d, t: t + ggot[d].astype(F32), jnp.zeros((16, 256), F32), unroll=4)
    grad_ref[...] = dot(total, back_ref[...], precision=lax.Precision.HIGHEST)

    for g in range(FWD):
        whole(back.at[g], mine.at[g], GRADS + 1 + g).wait_recv()

        def unpack(d, carry):
            for c in range(3):
                row = pl.multiple_of(((g * 3 + c) * NDEV + d) * PART, 8)
                flat[pl.ds(row, 16), :] = mine[g, d, :, c * 128 : (c + 1) * 128].astype(F32)
            return carry

        lax.fori_loop(0, NDEV, unpack, 0, unroll=4)

        def along_x(mp, carry):
            for c in range(3):
                rows = [
                    flat[pl.ds((g * 3 + c) * NDEV * PART + mp * 4 + xx, NDEV, stride=PART), :] for xx in range(4)
                ]
                left = jnp.concatenate(rows, axis=0).astype(BF16)
                o32[mp, (g * 3 + c) * 128 : (g * 3 + c + 1) * 128, :] = dot(left, tx_ref[...], TN)
            return carry

        lax.fori_loop(0, 4, along_x, 0)

    def finish(mp, carry):
        for mh in range(3):
            m = mh * 4 + mp
            kx, ky, kz, retained, square, damping, weight = waves_of(m, j, l)
            scale = weight * retained
            parts = []
            for f in range(5):
                g, pp = divmod(f * 3 + mh, 8)
                row = pl.multiple_of(g * ROW + lax.rem(pp + j, 8) * SLOT, 8)
                re = o32[mp, pl.ds(row, WY), :]
                im = o32[mp, pl.ds(row + WY, WY), :]
                parts.append((re[:, :NG] - im[:, NG:], im[:, :NG] + re[:, NG:]))
            ax, az, ay, wy, wz = parts
            spec = [
                ax,
                (ay[0] + kx * wz[1], ay[1] - kx * wz[0]),
                (az[0] - kx * wy[1], az[1] + kx * wy[0]),
            ]
            for c in range(3):
                for r in range(2):
                    out_ref[c, r, m] = damping * cot_ref[c, r, m] + scale * spec[c][r]
        return carry

    lax.fori_loop(0, 4, finish, 0)
    for group in range(3):
        whole(sent.at[group], got.at[group], group).wait_send()
    whole(gsent, ggot, GRADS).wait_send()
    for g in range(FWD):
        whole(back.at[g], mine.at[g], GRADS + 1 + g).wait_send()


VMEM = pl.BlockSpec(memory_space=pltpu.VMEM)
ANY = pl.BlockSpec(memory_space=pl.ANY)


def shards(state, cotangent, w_in, b_in, w_out):
    t = {k: jnp.asarray(v) for k, v in make_tables().items()}
    state = state.transpose(0, 1, 3, 2, 4)
    cotangent = cotangent.transpose(0, 1, 3, 2, 4)
    sds = jax.ShapeDtypeStruct
    grad, sums = pl.pallas_call(
        main_kernel,
        out_shape=(sds((3, 2, WZ, WY, NG), F32), sds((16, 256), F32)),
        in_specs=[VMEM] * 12 + [ANY] * 2,
        out_specs=(VMEM, VMEM),
        scratch_shapes=[
            pltpu.VMEM((ROW, 2 * NG), BF16),
            pltpu.VMEM((4 * 27 * 128, 128), F32),
            pltpu.VMEM((3, NDEV, 16, ROW), BF16),
            pltpu.VMEM((3, NDEV, 16, ROW), BF16),
            pltpu.VMEM((2, 144 * PITCH, 128), F32),
            pltpu.VMEM((2, 96 * PITCH, 128), F32),
            pltpu.VMEM((4 * 22 * 128, 128), F32),
            pltpu.VMEM((8, 256, ROW), BF16),
            pltpu.VMEM((FWD, NDEV, 16, ROW), BF16),
            pltpu.VMEM((FWD, NDEV, 16, ROW), BF16),
            pltpu.VMEM((NDEV, 16, 256), BF16),
            pltpu.VMEM((NDEV, 16, 256), BF16),
            pltpu.VMEM((4, FWD * ROW, 2 * NG), F32),
            pltpu.VMEM((4 * KY, 2 * NG), BF16),
            pltpu.VMEM((4 * KY, 2 * NG), BF16),
            pltpu.VMEM((HID, FEAT), BF16),
            pltpu.VMEM((FEAT, HID), BF16),
            pltpu.VMEM((HID, FEAT), BF16),
            pltpu.VMEM((HID, 256), F32),
            pltpu.VMEM((HID, 256), F32),
            pltpu.SemaphoreType.DMA((4,)),
            pltpu.SemaphoreType.DMA((6,)),
            pltpu.SemaphoreType.DMA((6,)),
        ],
        compiler_params=pltpu.CompilerParams(
            collective_id=0, has_side_effects=True, vmem_limit_bytes=64000 * 1024
        ),
    )(
        state, cotangent, t["tx"], t["tz"], t["tzk"], t["tzt"], t["tzkt"], t["perm"], t["back"],
        w_in.T, b_in[:, None], w_out, t["ty"], t["tyk"],
    )
    return (
        grad.transpose(0, 1, 3, 2, 4),
        sums[0:8, 0:FEAT],
        sums[8:16, 0:FEAT].T,
        sums[0:8, FEAT][None, :],
    )


def solution(mesh):
    split = P("rep", None, "px", "py", None)
    both = ("px", "py")
    return jax.shard_map(
        shards,
        mesh=mesh,
        in_specs=(split, split, P(), P(), P()),
        out_specs=(split, P(both, "rep"), P("rep", both), P("rep", both)),
        check_vma=False,
    )
```

```python
import numpy as np

import jax
import jax.numpy as jnp
from jax import lax
from jax.experimental import pallas as pl
from jax.experimental.pallas import tpu as pltpu
from jax.sharding import PartitionSpec as P

F32 = jnp.float32
BF16 = jnp.bfloat16
MESH = pl.DeviceIdType.MESH
NN = (((1,), (0,)), ((), ()))
NT = (((1,), (1,)), ((), ()))
TN = (((0,), (0,)), ((), ()))

NG, KY, KZ, HID, FEAT = 256, 192, 96, 512, 192
CUT = NG // 3
NU_DT = 5e-05
TIME_STEP = 0.01
FORCING = 20.0
NDEV = 64
WY, WZ = 24, 12
SLOT = 48
ROW = 8 * SLOT
INV = 8
FWD = 2
PITCH = 72


def dot(a, b, dims=NN, **kw):
    return lax.dot_general(a, b, dims, preferred_element_type=F32, **kw)


def make_tables():
    bf = jnp.bfloat16

    def angle(k, x):
        theta = 2 * np.pi * ((np.asarray(k)[:, None] % NG) * np.asarray(x)[None, :] % NG) / NG
        return np.cos(theta) / np.sqrt(NG), np.sin(theta) / np.sqrt(NG)

    order_x = np.arange(NG).reshape(64, 4).T.reshape(-1)
    c, s = angle(order_x, np.arange(NG))
    tx = np.concatenate([c, -s], axis=1)
    order = np.arange(NG).reshape(64, 4).T.reshape(-1)
    ids = np.arange(KY)
    ky = np.where(ids < KY // 2, ids, ids - KY)
    c, s = angle(ky, order)
    top = np.concatenate([c, s], axis=1).reshape(8, 1, WY, 2 * NG)
    low = np.concatenate([-s, c], axis=1).reshape(8, 1, WY, 2 * NG)
    kcol = ky.reshape(8, 1, WY, 1)
    ty = np.concatenate([top, low], axis=1).reshape(2 * KY, 2 * NG)
    tyk = np.concatenate([-kcol * low, kcol * top], axis=1).reshape(2 * KY, 2 * NG)
    kz = (np.arange(8)[None, :, None] * WZ + np.arange(3)[:, None, None] * 4 + np.arange(4)[None, None, :]).reshape(-1)
    c, s = angle(order, kz)
    tz = np.concatenate([c, -s], axis=1)
    kk = np.concatenate([kz, kz])[None, :]
    tzk = np.concatenate([s, c], axis=1) * kk
    perm = np.zeros((FEAT, FEAT), np.float32)
    src = np.arange(FEAT).reshape(3, 4, 4, 4).transpose(2, 0, 1, 3).reshape(-1)
    perm[src, np.arange(FEAT)] = 1.0
    back = np.zeros((256, 256), np.float32)
    back[:FEAT, :FEAT] = perm.T
    back[FEAT, FEAT] = 1.0
    arrays = dict(tx=tx, ty=ty, tyk=tyk, tz=tz, tzk=tzk, tzt=tz.T, tzkt=tzk.T, perm=perm)
    out = {k: np.asarray(v, np.float32).astype(bf) for k, v in arrays.items()}
    out["back"] = back
    return out


def waves_of(m, j, l):
    kz_id = l * WZ + m
    kz = kz_id.astype(F32)
    a = lax.broadcasted_iota(jnp.int32, (WY, NG), 0) + j * WY
    n = lax.broadcasted_iota(jnp.int32, (WY, NG), 1)
    ky = jnp.where(a < KY // 2, a, a - KY).astype(F32)
    kx = jnp.where(n < NG // 2, n, n - NG).astype(F32)
    keep = (jnp.abs(kx) <= CUT) & (jnp.abs(ky) <= CUT) & (kz <= float(CUT))
    retained = keep.astype(F32)
    square = kx * kx + ky * ky + kz * kz
    damping = jnp.exp(-NU_DT * square)
    weight = jnp.where(kz_id == 0, 1.0, 2.0).astype(F32)
    return kx, ky, kz, retained, square, damping, weight


LIMIT = 46 * 1024 * 1024
PART = 24
GRADS = INV * 3 // 8


def lane_select(lane, v, pick):
    slots = [q for q in range(8) if q * SLOT < (v + 1) * 128 and (q + 1) * SLOT > v * 128]
    value = pick(slots[0])
    for q in slots[1:]:
        value = jnp.where(lane >= float(q * SLOT - v * 128), pick(q), value)
    return value


def cross(a, b):
    return [a[1] * b[2] - a[2] * b[1], a[2] * b[0] - a[0] * b[2], a[0] * b[1] - a[1] * b[0]]


def main_kernel(
    state_hbm, cot_hbm, tx_hbm, tz_hbm, tzk_hbm, tzt_hbm, tzkt_hbm, perm_hbm, back_hbm, w_in_hbm, b_hbm, w_out_hbm,
    ty_hbm, tyk_hbm,
    out_ref, grad_in_ref, grad_out_ref, grad_bias_ref,
    state_ref, cot_ref, tx_ref, tz_ref, tzk_ref, tzt_ref, tzkt_ref, perm_ref, back_ref, w_in_t, b_row, w_out,
    s_ref, flat, sent, got, v32, va32, o16, back, mine, gsent, ggot, ty_ref, tyk_ref,
    win, wint, woutt, bias, gin, gout, load_sem, send_sem, recv_sem,
):
    j, l = lax.axis_index("px"), lax.axis_index("py")
    me = j * 8 + l
    x, core, z, y = j >> 1, j & 1, l >> 2, l & 3
    l32, o32 = v32, va32

    def peer(k):
        k = k + jnp.where(k >= 3, 1, 0)
        dx = (k & 3) + 1
        dy = dx + ((k >> 2) & 3)
        px = (((x + dx) & 3) << 1) + ((core + (k >> 4)) & 1)
        py = (((z + (k >> 5)) & 1) << 2) + ((y + dy) & 3)
        return (px << 3) + py, {"px": px, "py": py}

    barrier = pltpu.get_barrier_semaphore()

    def greet(k, carry):
        pl.semaphore_signal(barrier, inc=1, device_id=peer(k)[1], device_id_type=MESH)
        return carry

    half = 2 * KY
    pairs = [(cot_hbm, cot_ref), (tx_hbm, tx_ref), (state_hbm, state_ref)]
    for src, dst in [(ty_hbm, ty_ref), (tyk_hbm, tyk_ref)]:
        pairs += [(src, dst.at[pl.ds(0, half)]), (src, dst.at[pl.ds(half, half)])]
    pairs += [(tz_hbm, tz_ref), (tzk_hbm, tzk_ref), (tzt_hbm, tzt_ref), (tzkt_hbm, tzkt_ref), (perm_hbm, perm_ref)]
    pairs += [(back_hbm, back_ref), (w_in_hbm, w_in_t), (b_hbm, b_row), (w_out_hbm, w_out)]
    loads = [pltpu.make_async_copy(src, dst, load_sem.at[n]) for n, (src, dst) in enumerate(pairs)]
    for load in loads:
        load.start()
    lax.fori_loop(0, NDEV - 1, greet, 0, unroll=3)

    def copy(src, dst, number, where):
        return pltpu.make_async_remote_copy(
            src_ref=src,
            dst_ref=dst,
            send_sem=send_sem.at[number],
            recv_sem=recv_sem.at[number],
            device_id=where,
            device_id_type=MESH,
        )

    def send_all(src, dst, number):
        def send(k, carry):
            t, where = peer(k)
            copy(src.at[t], dst.at[me], number, where).start()
            return carry

        dst[pl.ds(me, 1)] = src[pl.ds(me, 1)]
        lax.fori_loop(0, NDEV - 1, send, 0, unroll=3)

    def whole(src, dst, number):
        rest = pl.ds(0, NDEV - 1)
        return copy(src.at[rest], dst.at[rest], number, peer(0)[1])

    for group in range(3):
        for load in [loads[0:2], loads[2:3], []][group]:
            load.wait()

        def one(mp, carry):
            for mh in range(3):
                fields = [f for f in range(INV) if (f * 3 + mh) // 8 == group]
                m = mh * 4 + mp
                kx, ky, kz, retained, square, damping, weight = waves_of(m, j, l)
                value = {}
                if any(f >= 3 for f in fields):
                    scale = weight * retained
                    v = [[scale * state_ref[c, r, m] for r in range(2)] for c in range(3)]
                    value.update({3 + c: v[c] for c in range(3)})
                    value[6] = [-(kz * v[0][1] - kx * v[2][1]), kz * v[0][0] - kx * v[2][0]]
                    value[7] = [-(kx * v[1][1] - ky * v[0][1]), kx * v[1][0] - ky * v[0][0]]
                if any(f < 3 for f in fields):
                    inverse = 1.0 / jnp.maximum(square, 1.0)
                    scale = TIME_STEP * retained
                    force = [[], [], []]
                    for r in range(2):
                        w = [damping * cot_ref[c, r, m] for c in range(3)]
                        along = (kx * w[0] + ky * w[1] + kz * w[2]) * inverse
                        for c, k in enumerate((kx, ky, kz)):
                            force[c].append(scale * (w[c] - k * along))
                    value.update({c: force[c] for c in range(3)})
                for f in fields:
                    re, im = value[f]
                    top = jnp.concatenate([re, im], axis=1)
                    low = jnp.concatenate([im, -re], axis=1)
                    row = pl.multiple_of((((f * 3 + mh) % 8 + j) & 7) * SLOT, 16)
                    s_ref[pl.ds(row, SLOT), :] = jnp.concatenate([top, low], axis=0).astype(BF16)
            for first in range(0, ROW, 256):
                width = min(256, ROW - first)
                out = dot(tx_ref[...], s_ref[first : first + width, :], NT)
                for c in range(width // 128):
                    for xx in range(4):
                        base = (first // 128 + c) * NDEV * PART
                        flat[pl.ds(base + mp * 4 + xx, NDEV, stride=PART), :] = out[
                            xx * 64 : (xx + 1) * 64, c * 128 : (c + 1) * 128
                        ]
            return carry

        lax.fori_loop(0, 4, one, 0)

        def pack(d, carry):
            for c in range(3):
                row = pl.multiple_of(c * NDEV * PART + d * PART, 8)
                sent[group, d, :, c * 128 : (c + 1) * 128] = flat[pl.ds(row, 16), :].astype(BF16)
            return carry

        lax.fori_loop(0, NDEV, pack, 0, unroll=4)
        if group == 0:
            pl.semaphore_wait(barrier, NDEV - 1)
        send_all(sent.at[group], got.at[group], group)

    lane = lax.broadcasted_iota(jnp.int32, (1, 128), 1).astype(BF16)
    lane = jnp.broadcast_to(lane, (128, 128))

    for load in loads[3:]:
        load.wait()
    perm = perm_ref[...]
    win[...] = dot(w_in_t[...], perm, TN).astype(BF16)
    wint[...] = dot(perm, w_in_t[...], TN).astype(BF16)
    woutt[...] = dot(w_out[...], perm, TN).astype(BF16)
    gin[...] = jnp.zeros_like(gin)
    gout[...] = jnp.zeros_like(gout)
    bias[...] = jnp.broadcast_to(b_row[...], (128, HID)).T

    BLOCKS = 27

    def along_y(group):
        for pp in range(8):
            first = (8 - pp) * SLOT
            parts = []
            for v in range(3):
                pick = lambda q: got[group, (q - pp) % 8 * 8 : (q - pp) % 8 * 8 + 8, :, v * 128 : (v + 1) * 128].reshape(128, 128)
                parts.append(lane_select(lane, v, pick))
            left = jnp.concatenate(parts, axis=1)
            todo = [(pp * 3 + group, dot(left, ty_ref[first : first + 2 * KY, :]))]
            f, mh = divmod(group * 8 + pp, 3)
            if f == 5:
                todo.append((24 + mh, -dot(left, tyk_ref[first : first + 2 * KY, :])))
            for block, out in todo:
                for c in range(4):
                    row = (c * BLOCKS + block) * 128
                    flat[row : row + 128, :] = out[:, c * 128 : (c + 1) * 128]

    def columns(f, xx):
        parts = []
        for t in range(2):
            for mh in range(3):
                g, pp = divmod(f * 3 + mh, 8)
                block = 24 + mh if f == INV else pp * 3 + g
                lanes = [
                    flat[pl.ds(((2 * t + h) * BLOCKS + block) * 128 + xx, 32, stride=4), :] for h in range(2)
                ]
                parts.append(jnp.concatenate(lanes, axis=1))
        return jnp.concatenate(parts, axis=0).astype(BF16)

    def along_z(fields):
        def one(xx, carry):
            for slot, f in fields:
                out = dot(tz_ref[...], columns(f, xx))
                if f == INV:
                    out = out + dot(tzk_ref[...], columns(4, xx))
                out = out.astype(BF16).astype(F32)
                for dz in range(4):
                    row = pl.multiple_of((slot * 16 + xx * 4 + dz) * PITCH, 8)
                    for h in range(2):
                        v32[h, pl.ds(row, 64), :] = out[dz * 64 : (dz + 1) * 64, h * 128 : (h + 1) * 128]
            return carry

        lax.fori_loop(0, 4, one, 0)

    for group, fields in enumerate([[(6, 0), (7, 1)], [(8, 2), (0, 3), (1, 4)], [(2, 5), (3, INV), (4, 6), (5, 7)]]):
        whole(sent.at[group], got.at[group], group).wait_recv()
        along_y(group)
        along_z(fields)

    ones = jnp.ones((64, 256), BF16)

    def rows_of(field, bz):
        rows = pl.ds(field * 16 * PITCH + bz, 48, stride=PITCH)
        return [v32[h, rows, :] for h in range(2)]

    def boxes(planes):
        parts = []
        for dy in range(4):
            h, at = dy // 2, dy % 2 * 64
            parts.append(jnp.concatenate([p[h][:, at : at + 64] for p in planes], axis=1))
        return jnp.concatenate(parts, axis=0).astype(BF16)

    def closure(group, carry):
        bzs = [group * 4 + b for b in range(4)]
        velocity = [rows_of(0, bz) for bz in bzs]
        force = [rows_of(6, bz) for bz in bzs]
        features = boxes(velocity)
        adjoints = boxes(force)
        shift = bias[...]
        pre = dot(win[...], features) + jnp.concatenate([shift, shift], axis=1)
        sigmoid = 0.5 + 0.5 * jnp.tanh(0.5 * pre)
        hidden = (pre * sigmoid).astype(BF16)
        hidden_adj = FORCING * dot(woutt[...], adjoints)
        pre_adj = (hidden_adj * sigmoid * (1.0 + pre * (1.0 - sigmoid))).astype(BF16)
        gin[...] += dot(pre_adj, jnp.concatenate([features, ones], axis=0), NT)
        gout[:, 0:FEAT] += dot(hidden, adjoints, NT)
        feat_adj = dot(wint[...], pre_adj)
        for b, bz in enumerate(bzs):
            spin = rows_of(3, bz)
            for h in range(2):
                lanes = [feat_adj[dy * 48 : (dy + 1) * 48, b * 64 : (b + 1) * 64] for dy in (2 * h, 2 * h + 1)]
                pick = lambda a: [a[c * 16 : (c + 1) * 16, :] for c in range(3)]
                vel, vor, frc = pick(velocity[b][h]), pick(spin[h]), pick(force[b][h])
                first = jnp.concatenate(cross(vor, frc), axis=0) + jnp.concatenate(lanes, axis=1)
                second = jnp.concatenate(cross(frc, vel), axis=0)
                va32[h, pl.ds(bz, 48, stride=PITCH), :] = first
                va32[h, pl.ds(48 * PITCH + bz, 48, stride=PITCH), :] = second
        return carry

    lax.fori_loop(0, 16, closure, 0)

    def slices(d, carry):
        rows = pl.ds(pl.multiple_of(d * 8, 8), 8)
        gsent[d] = jnp.concatenate([gin[rows, :], FORCING * gout[rows, :]], axis=0).astype(BF16)
        return carry

    lax.fori_loop(0, NDEV, slices, 0, unroll=4)
    send_all(gsent, ggot, GRADS)

    def field_of(c, xx):
        parts = []
        for dz in range(4):
            row = pl.multiple_of((c * 16 + xx * 4 + dz) * PITCH, 8)
            parts.append(jnp.concatenate([va32[0, pl.ds(row, 64), :], va32[1, pl.ds(row, 64), :]], axis=1))
        return jnp.concatenate(parts, axis=0).astype(BF16)

    def l32_row(r, block):
        return (r * 22 + block) * 128

    def put(block, value, xx):
        for r in range(2):
            for mh in range(3):
                for h in range(2):
                    l32[h, pl.ds(l32_row(r, block(mh)) + xx, 32, stride=4), :] = value[
                        r * 96 + mh * 32 : r * 96 + (mh + 1) * 32, h * 128 : (h + 1) * 128
                    ]

    def direct(f):
        def block(mh):
            g, pp = divmod(f * 3 + mh, 8)
            return pp * 2 + g

        return block

    def extra(f):
        return lambda mh: 16 + f * 3 + mh

    def forward_z(xx, carry):
        vort = field_of(4, xx)
        tzt = tzt_ref[...]
        tzkt = tzkt_ref[...]
        put(direct(0), dot(tzt, field_of(0, xx)) - dot(tzkt, vort), xx)
        put(direct(3), dot(tzt, vort), xx)
        vort = field_of(3, xx)
        put(direct(2), dot(tzt, field_of(1, xx)) + dot(tzkt, vort), xx)
        put(extra(1), -dot(tzt, vort), xx)
        put(direct(1), dot(tzt, field_of(2, xx)), xx)
        value = dot(tzt, field_of(5, xx))
        put(direct(4), value, xx)
        put(extra(0), value, xx)
        return carry

    for r in range(2):
        for h in range(2):
            row = l32_row(r, 15)
            l32[h, row : row + 128, :] = jnp.zeros((128, 128), F32)
    lax.fori_loop(0, 4, forward_z, 0)

    def left_of(block, count):
        parts = [
            l32[h, l32_row(r, block) : l32_row(r, block + count), :] for r in range(2) for h in range(2)
        ]
        return jnp.concatenate(parts, axis=1).astype(BF16)

    for pp in range(8):
        first = (8 - pp) * SLOT
        out = dot(left_of(pp * 2, 2), ty_ref[first : first + 2 * KY, :], NT)
        if pp < 6:
            more = dot(left_of(16 + pp, 1), tyk_ref[first : first + 2 * KY, :], NT)
            o16[pp, 0:128, :] = (out[0:128] + more).astype(BF16)
            o16[pp, 128:256, :] = out[128:256].astype(BF16)
        else:
            o16[pp] = out.astype(BF16)
    for g in range(FWD):
        for to in range(8):
            for v in range(3):
                pick = lambda q: o16[(q - to) % 8, g * 128 : (g + 1) * 128, v * 128 : (v + 1) * 128]
                back[g, to * 8 : to * 8 + 8, :, v * 128 : (v + 1) * 128] = lane_select(lane, v, pick).reshape(8, 16, 128)
        send_all(back.at[g], mine.at[g], GRADS + 1 + g)

    whole(gsent, ggot, GRADS).wait_recv()
    total = lax.fori_loop(0, NDEV, lambda d, t: t + ggot[d].astype(F32), jnp.zeros((16, 256), F32), unroll=4)
    ordered = dot(total, back_ref[...], precision=lax.Precision.HIGHEST)
    grad_in_ref[...] = ordered[0:8, 0:FEAT]
    grad_out_ref[...] = ordered[8:16, 0:FEAT]
    pick = (lax.broadcasted_iota(jnp.int32, (8, 256), 1) == FEAT).astype(F32)
    grad_bias_ref[...] = dot(pick, total[0:8], NT, precision=lax.Precision.HIGHEST)[0:1]

    for g in range(FWD):
        whole(back.at[g], mine.at[g], GRADS + 1 + g).wait_recv()

        def unpack(d, carry):
            for c in range(3):
                row = pl.multiple_of(((g * 3 + c) * NDEV + d) * PART, 8)
                flat[pl.ds(row, 16), :] = mine[g, d, :, c * 128 : (c + 1) * 128].astype(F32)
            return carry

        lax.fori_loop(0, NDEV, unpack, 0, unroll=4)

        def along_x(mp, carry):
            for c in range(3):
                rows = [
                    flat[pl.ds((g * 3 + c) * NDEV * PART + mp * 4 + xx, NDEV, stride=PART), :] for xx in range(4)
                ]
                left = jnp.concatenate(rows, axis=0).astype(BF16)
                out = dot(left, tx_ref[...], TN)
                for r in range(2):
                    for h in range(2):
                        row = pl.multiple_of((mp * 2 + r) * FWD * ROW + (g * 3 + c) * 128, 8)
                        o32[h, pl.ds(row, 128), :] = out[:, (2 * r + h) * 128 : (2 * r + h + 1) * 128]
            return carry

        lax.fori_loop(0, 4, along_x, 0)

    def finish(mp, carry):
        for mh in range(3):
            m = mh * 4 + mp
            kx, ky, kz, retained, square, damping, weight = waves_of(m, j, l)
            scale = weight * retained
            parts = []
            for f in range(5):
                g, pp = divmod(f * 3 + mh, 8)
                row = pl.multiple_of(mp * 2 * FWD * ROW + g * ROW + ((pp + j) & 7) * SLOT, 8)
                wave = lambda r, s: jnp.concatenate([o32[h, pl.ds(row + r * FWD * ROW + s * WY, WY), :] for h in range(2)], axis=1)
                parts.append((wave(0, 0) - wave(1, 1), wave(0, 1) + wave(1, 0)))
            ax, az, ay, wy, wz = parts
            spec = [
                ax,
                (ay[0] + kx * wz[1], ay[1] - kx * wz[0]),
                (az[0] - kx * wy[1], az[1] + kx * wy[0]),
            ]
            for c in range(3):
                for r in range(2):
                    out_ref[c, r, m] = damping * cot_ref[c, r, m] + scale * spec[c][r]
        return carry

    lax.fori_loop(0, 4, finish, 0)
    for group in range(3):
        whole(sent.at[group], got.at[group], group).wait_send()
    whole(gsent, ggot, GRADS).wait_send()
    for g in range(FWD):
        whole(back.at[g], mine.at[g], GRADS + 1 + g).wait_send()


ANY = pl.BlockSpec(memory_space=pltpu.HBM)
VMEM = pl.BlockSpec(memory_space=pltpu.VMEM)


def shards(state, cotangent, w_in, b_in, w_out):
    t = {k: jnp.asarray(v) for k, v in make_tables().items()}
    sds = jax.ShapeDtypeStruct
    operands = [state.transpose(0, 1, 3, 2, 4), cotangent.transpose(0, 1, 3, 2, 4)]
    operands += [t[k] for k in ("tx", "tz", "tzk", "tzt", "tzkt", "perm", "back")]
    operands += [w_in.T, b_in[None, :], w_out]
    grad, grad_in, grad_out, grad_bias = pl.pallas_call(
        main_kernel,
        out_shape=(sds((3, 2, WZ, WY, NG), F32), sds((8, FEAT), F32), sds((8, FEAT), F32), sds((1, 8), F32)),
        in_specs=[ANY] * 14,
        out_specs=(VMEM,) * 4,
        scratch_shapes=[pltpu.VMEM(o.shape, o.dtype) for o in operands]
        + [
            pltpu.VMEM((ROW, 2 * NG), BF16),
            pltpu.VMEM((4 * 27 * 128, 128), F32),
            pltpu.VMEM((3, NDEV, 16, ROW), BF16),
            pltpu.VMEM((3, NDEV, 16, ROW), BF16),
            pltpu.VMEM((2, 144 * PITCH, 128), F32),
            pltpu.VMEM((2, 96 * PITCH, 128), F32),
            pltpu.VMEM((8, 256, ROW), BF16),
            pltpu.VMEM((FWD, NDEV, 16, ROW), BF16),
            pltpu.VMEM((FWD, NDEV, 16, ROW), BF16),
            pltpu.VMEM((NDEV, 16, 256), BF16),
            pltpu.VMEM((NDEV, 16, 256), BF16),
            pltpu.VMEM((4 * KY, 2 * NG), BF16),
            pltpu.VMEM((4 * KY, 2 * NG), BF16),
            pltpu.VMEM((HID, FEAT), BF16),
            pltpu.VMEM((FEAT, HID), BF16),
            pltpu.VMEM((HID, FEAT), BF16),
            pltpu.VMEM((HID, 128), F32),
            pltpu.VMEM((HID, 256), F32),
            pltpu.VMEM((HID, 256), F32),
            pltpu.SemaphoreType.DMA((16,)),
            pltpu.SemaphoreType.DMA((6,)),
            pltpu.SemaphoreType.DMA((6,)),
        ],
        compiler_params=pltpu.CompilerParams(
            collective_id=0, has_side_effects=True, vmem_limit_bytes=LIMIT
        ),
    )(*[pltpu.with_memory_space_constraint(o, pltpu.HBM) for o in [*operands, t["ty"], t["tyk"]]])
    return grad.transpose(0, 1, 3, 2, 4), grad_in, grad_out.T, grad_bias


def solution(mesh):
    split = P("rep", None, "px", "py", None)
    both = ("px", "py")
    return jax.shard_map(
        shards,
        mesh=mesh,
        in_specs=(split, split, P(), P(), P()),
        out_specs=(split, P(both, "rep"), P("rep", both), P("rep", both)),
        check_vma=False,
    )
```

```python
import numpy as np

import jax
import jax.numpy as jnp
from jax import lax
from jax.experimental import pallas as pl
from jax.experimental.pallas import tpu as pltpu
from jax.sharding import PartitionSpec as P

F32 = jnp.float32
BF16 = jnp.bfloat16
MESH = pl.DeviceIdType.MESH
NN = (((1,), (0,)), ((), ()))
NT = (((1,), (1,)), ((), ()))
TN = (((0,), (0,)), ((), ()))

NG, KY, KZ, HID, FEAT = 256, 192, 96, 512, 192
CUT = NG // 3
NU_DT = 5e-05
TIME_STEP = 0.01
FORCING = 20.0
NDEV = 64
WY, WZ = 24, 12
SLOT = 48
ROW = 8 * SLOT
INV = 8
FWD = 2
SPARE = 208
PITCH = 72


def dot(a, b, dims=NN, **kw):
    return lax.dot_general(a, b, dims, preferred_element_type=F32, **kw)


def make_tables():
    bf = jnp.bfloat16

    def angle(k, x):
        theta = 2 * np.pi * ((np.asarray(k)[:, None] % NG) * np.asarray(x)[None, :] % NG) / NG
        return np.cos(theta) / np.sqrt(NG), np.sin(theta) / np.sqrt(NG)

    order_x = np.arange(NG).reshape(64, 4).T.reshape(-1)
    c, s = angle(order_x, np.arange(NG))
    tx = np.concatenate([c, -s], axis=1)
    order = np.arange(NG).reshape(64, 4).T.reshape(-1)
    ids = np.arange(KY)
    ky = np.where(ids < KY // 2, ids, ids - KY)
    c, s = angle(ky, order)
    top = np.concatenate([c, s], axis=1).reshape(8, 1, WY, 2 * NG)
    low = np.concatenate([-s, c], axis=1).reshape(8, 1, WY, 2 * NG)
    kcol = ky.reshape(8, 1, WY, 1)
    ty = np.concatenate([top, low], axis=1).reshape(2 * KY, 2 * NG)
    tyk = np.concatenate([-kcol * low, kcol * top], axis=1).reshape(2 * KY, 2 * NG)
    kz = (np.arange(8)[None, :, None] * WZ + np.arange(3)[:, None, None] * 4 + np.arange(4)[None, None, :]).reshape(-1)
    c, s = angle(order, kz)
    tz = np.concatenate([c, -s], axis=1)
    kk = np.concatenate([kz, kz])[None, :]
    tzk = np.concatenate([s, c], axis=1) * kk
    perm = np.zeros((FEAT, FEAT), np.float32)
    src = np.arange(FEAT).reshape(3, 4, 4, 4).transpose(2, 0, 1, 3).reshape(-1)
    perm[src, np.arange(FEAT)] = 1.0
    back = np.zeros((256, 256), np.float32)
    back[:FEAT, :FEAT] = perm.T
    back[FEAT, FEAT] = 1.0
    arrays = dict(tx=tx, ty=ty, tyk=tyk, tz=tz, tzk=tzk, tzt=tz.T, tzkt=tzk.T, perm=perm)
    out = {k: np.asarray(v, np.float32).astype(bf) for k, v in arrays.items()}
    out["back"] = back
    return out


def waves_of(m, j, l):
    kz_id = l * WZ + m
    kz = kz_id.astype(F32)
    a = lax.broadcasted_iota(jnp.int32, (WY, NG), 0) + j * WY
    n = lax.broadcasted_iota(jnp.int32, (WY, NG), 1)
    ky = jnp.where(a < KY // 2, a, a - KY).astype(F32)
    kx = jnp.where(n < NG // 2, n, n - NG).astype(F32)
    keep = (jnp.abs(kx) <= CUT) & (jnp.abs(ky) <= CUT) & (kz <= float(CUT))
    retained = keep.astype(F32)
    square = kx * kx + ky * ky + kz * kz
    damping = jnp.exp(-NU_DT * square)
    weight = jnp.where(kz_id == 0, 1.0, 2.0).astype(F32)
    return kx, ky, kz, retained, square, damping, weight


LIMIT = 52 * 1024 * 1024
LINES = FWD * ROW + 128
PART = 24
GRADS = INV * 3 // 8


def lane_select(lane, v, pick):
    slots = [q for q in range(8) if q * SLOT < (v + 1) * 128 and (q + 1) * SLOT > v * 128]
    value = pick(slots[0])
    for q in slots[1:]:
        value = jnp.where(lane >= float(q * SLOT - v * 128), pick(q), value)
    return value


def cross(a, b):
    return [a[1] * b[2] - a[2] * b[1], a[2] * b[0] - a[0] * b[2], a[0] * b[1] - a[1] * b[0]]


def main_kernel(
    state_hbm, cot_hbm, tx_hbm, tz_hbm, tzk_hbm, tzt_hbm, tzkt_hbm, perm_hbm, back_hbm, w_in_hbm, b_hbm, w_out_hbm,
    ty_hbm, tyk_hbm,
    out_ref, grad_in_ref, grad_out_ref, grad_bias_ref,
    state_ref, cot_ref, tx_ref, tz_ref, tzk_ref, tzt_ref, tzkt_ref, perm_ref, back_ref, w_in_t, b_row, w_out,
    s_ref, flat, sent, got, v32, va32, o16, mine, gsent, ggot, ty_ref, tyk_ref,
    win, wint, woutt, bias, gin, gout, hid_all, pre_all, feat_all, adj_all, ky_part, spare, load_sem, send_sem, recv_sem,
):
    j, l = lax.axis_index("px"), lax.axis_index("py")
    me = j * 8 + l
    x, core, z, y = j >> 1, j & 1, l >> 2, l & 3
    l32, o32, kz_part, back = flat, v32, state_ref, sent

    def peer(k):
        k = k + jnp.where(k >= 3, 1, 0)
        dx = (k & 3) + 1
        dy = dx + ((k >> 2) & 3)
        px = (((x + dx) & 3) << 1) + ((core + (k >> 4)) & 1)
        py = (((z + (k >> 5)) & 1) << 2) + ((y + dy) & 3)
        return (px << 3) + py, {"px": px, "py": py}

    barrier = pltpu.get_barrier_semaphore()

    def greet(k, carry):
        pl.semaphore_signal(barrier, inc=1, device_id=peer(k)[1], device_id_type=MESH)
        return carry

    half = 2 * KY
    pairs = [(cot_hbm, cot_ref), (tx_hbm, tx_ref), (state_hbm, state_ref)]
    for src, dst in [(ty_hbm, ty_ref), (tyk_hbm, tyk_ref)]:
        pairs += [(src, dst.at[pl.ds(0, half)]), (src, dst.at[pl.ds(half, half)])]
    pairs += [(tz_hbm, tz_ref), (tzk_hbm, tzk_ref), (tzt_hbm, tzt_ref), (tzkt_hbm, tzkt_ref), (perm_hbm, perm_ref)]
    pairs += [(back_hbm, back_ref), (w_in_hbm, w_in_t), (b_hbm, b_row), (w_out_hbm, w_out)]
    loads = [pltpu.make_async_copy(src, dst, load_sem.at[n]) for n, (src, dst) in enumerate(pairs)]
    for load in loads:
        load.start()
    lax.fori_loop(0, NDEV - 1, greet, 0, unroll=3)

    def copy(src, dst, number, where):
        return pltpu.make_async_remote_copy(
            src_ref=src,
            dst_ref=dst,
            send_sem=send_sem.at[number],
            recv_sem=recv_sem.at[number],
            device_id=where,
            device_id_type=MESH,
        )

    def send_all(src, dst, number):
        def send(k, carry):
            t, where = peer(k)
            copy(src.at[t], dst.at[me], number, where).start()
            return carry

        dst[pl.ds(me, 1)] = src[pl.ds(me, 1)]
        lax.fori_loop(0, NDEV - 1, send, 0, unroll=3)

    def whole(src, dst, number):
        rest = pl.ds(0, NDEV - 1)
        return copy(src.at[rest], dst.at[rest], number, peer(0)[1])

    for group in range(3):
        for load in [loads[0:2], loads[2:3], []][group]:
            load.wait()

        def one(mp, carry):
            for mh in range(3):
                fields = [f for f in range(INV) if (f * 3 + mh) // 8 == group]
                m = mh * 4 + mp
                kx, ky, kz, retained, square, damping, weight = waves_of(m, j, l)
                value = {}
                if any(f >= 3 for f in fields):
                    scale = weight * retained
                    v = [[scale * state_ref[(c * 2 + r) * WZ + m] for r in range(2)] for c in range(3)]
                    value.update({3 + c: v[c] for c in range(3)})
                    value[6] = [-(kz * v[0][1] - kx * v[2][1]), kz * v[0][0] - kx * v[2][0]]
                    value[7] = [-(kx * v[1][1] - ky * v[0][1]), kx * v[1][0] - ky * v[0][0]]
                if any(f < 3 for f in fields):
                    inverse = 1.0 / jnp.maximum(square, 1.0)
                    scale = TIME_STEP * retained
                    force = [[], [], []]
                    for r in range(2):
                        w = [damping * cot_ref[c, r, m] for c in range(3)]
                        along = (kx * w[0] + ky * w[1] + kz * w[2]) * inverse
                        for c, k in enumerate((kx, ky, kz)):
                            force[c].append(scale * (w[c] - k * along))
                    value.update({c: force[c] for c in range(3)})
                for f in fields:
                    re, im = value[f]
                    top = jnp.concatenate([re, im], axis=1)
                    low = jnp.concatenate([im, -re], axis=1)
                    row = pl.multiple_of((((f * 3 + mh) % 8 + j) & 7) * SLOT, 16)
                    s_ref[pl.ds(row, SLOT), :] = jnp.concatenate([top, low], axis=0).astype(BF16)
            for first in range(0, ROW, 256):
                width = min(256, ROW - first)
                out = dot(tx_ref[...], s_ref[first : first + width, :], NT)
                for c in range(width // 128):
                    for xx in range(4):
                        base = (first // 128 + c) * NDEV * PART
                        flat[pl.ds(base + mp * 4 + xx, NDEV, stride=PART), :] = out[
                            xx * 64 : (xx + 1) * 64, c * 128 : (c + 1) * 128
                        ]
            return carry

        lax.fori_loop(0, 4, one, 0)

        def pack(d, carry):
            for c in range(3):
                row = pl.multiple_of(c * NDEV * PART + d * PART, 8)
                sent[group, d, :, c * 128 : (c + 1) * 128] = flat[pl.ds(row, 16), :].astype(BF16)
            return carry

        lax.fori_loop(0, NDEV, pack, 0, unroll=4)
        if group == 0:
            pl.semaphore_wait(barrier, NDEV - 1)
        send_all(sent.at[group], got.at[group], group)

    lane = lax.broadcasted_iota(jnp.int32, (1, 128), 1).astype(BF16)
    lane = jnp.broadcast_to(lane, (128, 128))

    for load in loads[3:]:
        load.wait()
    perm = perm_ref[...]
    win[...] = dot(w_in_t[...], perm, TN).astype(BF16)
    wint[...] = dot(perm, w_in_t[...], TN).astype(BF16)
    woutt[...] = dot(w_out[...], perm, TN).astype(BF16)
    gin[...] = jnp.zeros_like(gin)
    gout[...] = jnp.zeros_like(gout)
    feat_all[FEAT:256, :] = jnp.ones((256 - FEAT, 4096), BF16)
    bias[...] = jnp.broadcast_to(b_row[...], (128, HID)).T

    BLOCKS = 27

    def along_y(group):
        for pp in range(8):
            first = (8 - pp) * SLOT
            parts = []
            for v in range(3):
                pick = lambda q: got[group, (q - pp) % 8 * 8 : (q - pp) % 8 * 8 + 8, :, v * 128 : (v + 1) * 128].reshape(128, 128)
                parts.append(lane_select(lane, v, pick))
            left = jnp.concatenate(parts, axis=1)
            todo = [(pp * 3 + group, dot(left, ty_ref[first : first + 2 * KY, :]))]
            f, mh = divmod(group * 8 + pp, 3)
            if f == 5:
                todo.append((24 + mh, -dot(left, tyk_ref[first : first + 2 * KY, :])))
            for block, out in todo:
                for c in range(4):
                    row = (c * BLOCKS + block) * 128
                    flat[row : row + 128, :] = out[:, c * 128 : (c + 1) * 128]

    def columns(f, xx):
        parts = []
        for t in range(2):
            for mh in range(3):
                g, pp = divmod(f * 3 + mh, 8)
                block = 24 + mh if f == INV else pp * 3 + g
                lanes = [
                    flat[pl.ds(((2 * t + h) * BLOCKS + block) * 128 + xx, 32, stride=4), :] for h in range(2)
                ]
                parts.append(jnp.concatenate(lanes, axis=1))
        return jnp.concatenate(parts, axis=0).astype(BF16)

    def along_z(fields):
        def one(xx, carry):
            for slot, f in fields:
                out = dot(tz_ref[...], columns(f, xx))
                if f == INV:
                    out = out + dot(tzk_ref[...], columns(4, xx))
                out = out.astype(BF16).astype(F32)
                for dz in range(4):
                    row = pl.multiple_of((slot * 16 + xx * 4 + dz) * PITCH, 8)
                    for h in range(2):
                        v32[h, pl.ds(row, 64), :] = out[dz * 64 : (dz + 1) * 64, h * 128 : (h + 1) * 128]
            return carry

        lax.fori_loop(0, 4, one, 0)

    def boxes(fields):
        def one(group, carry):
            cols = pl.ds(pl.multiple_of(group * 256, 256), 256)
            for slot, ref, c in fields:
                rows = [pl.ds(slot * 16 * PITCH + group * 4 + b, 16, stride=PITCH) for b in range(4)]
                planes = [[v32[h, r, :] for h in range(2)] for r in rows]
                for dy in range(4):
                    h, at = dy // 2, dy % 2 * 64
                    value = jnp.concatenate([q[h][:, at : at + 64] for q in planes], axis=1)
                    ref[dy * 48 + c * 16 : dy * 48 + (c + 1) * 16, cols] = value.astype(BF16)
            return carry

        lax.fori_loop(0, 16, one, 0, unroll=4 if len(fields) == 1 else 1)

    for group, fields in enumerate([[(6, 0), (7, 1)], [(8, 2), (0, 3), (1, 4)], [(2, 5)]]):
        whole(sent.at[group], got.at[group], group).wait_recv()
        along_y(group)
        along_z(fields)
        if group == 1:
            boxes([(6, adj_all, 0), (7, adj_all, 1), (8, adj_all, 2), (0, feat_all, 0), (1, feat_all, 1)])
    for group in range(3):
        whole(sent.at[group], got.at[group], group).wait_send()

    def put(first, value, xx):
        for r in range(2):
            for mh in range(3):
                for h in range(2):
                    part = value[r * 96 + mh * 32 : r * 96 + (mh + 1) * 32, h * 128 : (h + 1) * 128]
                    if first < 12:
                        va32[h, pl.ds((r * 12 + first + mh) * 128 + xx, 32, stride=4), :] = part
                    else:
                        l32[pl.ds(((2 * r + h) * 9 + first + mh - 12) * 128 + xx, 32, stride=4), :] = part

    def plane(ref, c, xx, dz):
        row = pl.multiple_of((c * 16 + xx * 4 + dz) * PITCH, 8)
        return jnp.concatenate([ref[0, pl.ds(row, 64), :], ref[1, pl.ds(row, 64), :]], axis=1)

    def vort_z(xx, carry):
        parts = [[], [], []]
        for dz in range(4):
            vel = [plane(v32, c, xx, dz) for c in range(3)]
            frc = [plane(v32, 6 + c, xx, dz) for c in range(3)]
            for c, value in enumerate(cross(frc, vel)):
                parts[c].append(value.astype(BF16))
        wx, wy, wz = [jnp.concatenate(q, axis=0) for q in parts]
        tzt = tzt_ref[...]
        tzkt = tzkt_ref[...]
        kz_part[pl.ds(xx * 16, 8)] = dot(tzkt, wy).reshape(8, WY, NG)
        kz_part[pl.ds(xx * 16 + 8, 8)] = dot(tzkt, wx).reshape(8, WY, NG)
        put(0, dot(tzt, wy), xx)
        value = dot(tzt, wz)
        put(3, value, xx)
        put(6, value, xx)
        put(9, -dot(tzt, wx), xx)
        return carry

    def back_y(block, pp, table):
        first = (8 - pp) * SLOT
        parts = []
        for r in range(2):
            for h in range(2):
                if block < 12:
                    parts.append(va32[h, (r * 12 + block) * 128 : (r * 12 + block + 1) * 128, :])
                else:
                    row = ((2 * r + h) * 9 + block - 12) * 128
                    parts.append(l32[row : row + 128, :])
        return dot(jnp.concatenate(parts, axis=1).astype(BF16), table[first : first + 2 * KY, :], NT)

    def leave(g, used):
        for to in range(8):
            for v in range(3):
                pick = lambda q: o16[(q - to) % 8 % used, :, v * 128 : (v + 1) * 128]
                back[g, to * 8 : to * 8 + 8, :, v * 128 : (v + 1) * 128] = lane_select(lane, v, pick).reshape(8, 16, 128)
        send_all(back.at[g], mine.at[g], GRADS + 1 + g)

    lax.fori_loop(0, 4, vort_z, 0)
    for pp in range(6):
        o16[pp] = back_y(pp, pp, ty_ref).astype(BF16)
    leave(0, 6)
    for pp in range(6):
        ky_part[pp] = back_y(6 + pp, pp, tyk_ref)
    boxes([(2, feat_all, 2)])
    along_z([(3, INV), (4, 6), (5, 7)])

    def rows_of(field, bz):
        rows = pl.ds(field * 16 * PITCH + bz, 48, stride=PITCH)
        return [v32[h, rows, :] for h in range(2)]

    def closure(group, carry):
        bzs = [group * 4 + b for b in range(4)]
        cols = pl.ds(pl.multiple_of(group * 256, 256), 256)
        features = feat_all[0:FEAT, cols]
        adjoints = adj_all[:, cols]
        shift = bias[...]
        pre = dot(win[...], features) + jnp.concatenate([shift, shift], axis=1)
        sigmoid = 0.5 + 0.5 * jnp.tanh(0.5 * pre)
        hid_all[:, cols] = (pre * sigmoid).astype(BF16)
        hidden_adj = FORCING * dot(woutt[...], adjoints)
        pre_adj = (hidden_adj * sigmoid * (1.0 + pre * (1.0 - sigmoid))).astype(BF16)
        pre_all[:, cols] = pre_adj
        feat_adj = dot(wint[...], pre_adj)
        for b, bz in enumerate(bzs):
            spin, force = rows_of(3, bz), rows_of(6, bz)
            for h in range(2):
                lanes = [feat_adj[dy * 48 : (dy + 1) * 48, b * 64 : (b + 1) * 64] for dy in (2 * h, 2 * h + 1)]
                pick = lambda a: [a[c * 16 : (c + 1) * 16, :] for c in range(3)]
                first = jnp.concatenate(cross(pick(spin[h]), pick(force[h])), axis=0)
                va32[h, pl.ds(bz, 48, stride=PITCH), :] = first + jnp.concatenate(lanes, axis=1)
        return carry

    lax.fori_loop(0, 16, closure, 0, unroll=2)

    def vel_z(xx, carry):
        tzt = tzt_ref[...]
        field = lambda c: jnp.concatenate([plane(va32, c, xx, dz).astype(BF16) for dz in range(4)], axis=0)
        put(12, dot(tzt, field(0)) - kz_part[pl.ds(xx * 16, 8)].reshape(KY, NG), xx)
        put(15, dot(tzt, field(2)), xx)
        put(18, dot(tzt, field(1)) + kz_part[pl.ds(xx * 16 + 8, 8)].reshape(KY, NG), xx)
        return carry

    lax.fori_loop(0, 4, vel_z, 0)
    for pp in range(8):
        out = back_y(12 + pp, pp, ty_ref)
        o16[pp] = (out + ky_part[pp] if pp < 6 else out).astype(BF16)
    leave(1, 8)
    ninth = back_y(20, 0, ty_ref)
    for to in range(8):
        piece = ninth[:, to * SLOT : (to + 1) * SLOT]
        spare[to] = jnp.concatenate([jnp.zeros((128, SPARE - 128), F32), piece], axis=1)

    def products(k, carry):
        cols = pl.ds(pl.multiple_of(k * 1024, 1024), 1024)
        gin[...] += dot(pre_all[:, cols], feat_all[:, cols], NT)
        gout[:, 0:FEAT] += dot(hid_all[:, cols], adj_all[:, cols], NT)
        return carry

    lax.fori_loop(0, 4, products, 0)
    own_lane = lax.broadcasted_iota(jnp.int32, (16, 128), 1) < SPARE - 128

    def slices(d, carry):
        rows = pl.ds(pl.multiple_of(d * 8, 8), 8)
        extra = spare[d >> 3, pl.ds(pl.multiple_of((d & 7) * 16, 16), 16), :]
        lo = jnp.concatenate([gin[rows, 0:128], FORCING * gout[rows, 0:128]], axis=0)
        hi = jnp.concatenate([gin[rows, 128:256], FORCING * gout[rows, 128:256]], axis=0)
        gsent[d, :, 0:128] = lo.astype(BF16)
        gsent[d, :, 128:256] = jnp.where(own_lane, hi, extra).astype(BF16)
        return carry

    lax.fori_loop(0, NDEV, slices, 0, unroll=4)
    send_all(gsent, ggot, GRADS)

    def arrive(ref, chunk, lanes):
        def unpack(d, carry):
            row = pl.multiple_of((chunk * NDEV + d) * PART, 8)
            flat[pl.ds(row, 16), :] = ref[d, :, lanes : lanes + 128].astype(F32)
            return carry

        lax.fori_loop(0, NDEV, unpack, 0, unroll=8)

    def along_x(chunks):
        def one(mp, carry):
            for c in chunks:
                rows = [flat[pl.ds(c * NDEV * PART + mp * 4 + xx, NDEV, stride=PART), :] for xx in range(4)]
                out = dot(jnp.concatenate(rows, axis=0).astype(BF16), tx_ref[...], TN)
                for r in range(2):
                    for h in range(2):
                        row = pl.multiple_of((mp * 2 + r) * LINES + c * 128, 8)
                        o32[h, pl.ds(row, 128), :] = out[:, (2 * r + h) * 128 : (2 * r + h + 1) * 128]
            return carry

        lax.fori_loop(0, 4, one, 0)

    for g in range(FWD):
        whole(back.at[g], mine.at[g], GRADS + 1 + g).wait_recv()
        for c in range(3):
            arrive(mine.at[g], g * 3 + c, c * 128)
        along_x(range(g * 3, g * 3 + 3))
    whole(gsent, ggot, GRADS).wait_recv()
    arrive(ggot, 6, 128)
    along_x([6])

    total = lax.fori_loop(0, NDEV, lambda d, t: t + ggot[d].astype(F32), jnp.zeros((16, 256), F32), unroll=4)
    ordered = dot(total, back_ref[...], precision=lax.Precision.HIGHEST)
    grad_in_ref[...] = ordered[0:8, 0:FEAT]
    grad_out_ref[...] = ordered[8:16, 0:FEAT]
    pick = (lax.broadcasted_iota(jnp.int32, (8, 256), 1) == FEAT).astype(F32)
    grad_bias_ref[...] = dot(pick, total[0:8], NT, precision=lax.Precision.HIGHEST)[0:1]

    def finish(mp, carry):
        for mh in range(3):
            m = mh * 4 + mp
            kx, ky, kz, retained, square, damping, weight = waves_of(m, j, l)
            scale = weight * retained
            parts = []
            for g, piece in [(0, mh), (0, 3 + mh), (1, mh), (1, 3 + mh), (1, 6 + mh)]:
                place = g * ROW + ((piece + j) & 7) * SLOT if piece < 8 else FWD * ROW + SPARE - 128
                row = pl.multiple_of(mp * 2 * LINES + place, 8)
                wave = lambda r, s: jnp.concatenate([o32[h, pl.ds(row + r * LINES + s * WY, WY), :] for h in range(2)], axis=1)
                parts.append((wave(0, 0) - wave(1, 1), wave(0, 1) + wave(1, 0)))
            wy, wz, ax, az, ay = parts
            spec = [
                ax,
                (ay[0] + kx * wz[1], ay[1] - kx * wz[0]),
                (az[0] - kx * wy[1], az[1] + kx * wy[0]),
            ]
            for c in range(3):
                for r in range(2):
                    out_ref[c, r, m] = damping * cot_ref[c, r, m] + scale * spec[c][r]
        return carry

    lax.fori_loop(0, 4, finish, 0)
    whole(gsent, ggot, GRADS).wait_send()
    for g in range(FWD):
        whole(back.at[g], mine.at[g], GRADS + 1 + g).wait_send()


ANY = pl.BlockSpec(memory_space=pltpu.HBM)
VMEM = pl.BlockSpec(memory_space=pltpu.VMEM)


def shards(state, cotangent, w_in, b_in, w_out):
    t = {k: jnp.asarray(v) for k, v in make_tables().items()}
    sds = jax.ShapeDtypeStruct
    operands = [state.transpose(0, 1, 3, 2, 4).reshape(6 * WZ, WY, NG), cotangent.transpose(0, 1, 3, 2, 4)]
    operands += [t[k] for k in ("tx", "tz", "tzk", "tzt", "tzkt", "perm", "back")]
    operands += [w_in.T, b_in[None, :], w_out]
    grad, grad_in, grad_out, grad_bias = pl.pallas_call(
        main_kernel,
        out_shape=(sds((3, 2, WZ, WY, NG), F32), sds((8, FEAT), F32), sds((8, FEAT), F32), sds((1, 8), F32)),
        in_specs=[ANY] * 14,
        out_specs=(VMEM,) * 4,
        scratch_shapes=[pltpu.VMEM(o.shape, o.dtype) for o in operands]
        + [
            pltpu.VMEM((ROW, 2 * NG), BF16),
            pltpu.VMEM((4 * 27 * 128, 128), F32),
            pltpu.VMEM((3, NDEV, 16, ROW), BF16),
            pltpu.VMEM((3, NDEV, 16, ROW), BF16),
            pltpu.VMEM((2, 144 * PITCH, 128), F32),
            pltpu.VMEM((2, 48 * PITCH, 128), F32),
            pltpu.VMEM((8, 128, ROW), BF16),
            pltpu.VMEM((FWD, NDEV, 16, ROW), BF16),
            pltpu.VMEM((NDEV, 16, 256), BF16),
            pltpu.VMEM((NDEV, 16, 256), BF16),
            pltpu.VMEM((4 * KY, 2 * NG), BF16),
            pltpu.VMEM((4 * KY, 2 * NG), BF16),
            pltpu.VMEM((HID, FEAT), BF16),
            pltpu.VMEM((FEAT, HID), BF16),
            pltpu.VMEM((HID, FEAT), BF16),
            pltpu.VMEM((HID, 128), F32),
            pltpu.VMEM((HID, 256), F32),
            pltpu.VMEM((HID, 256), F32),
            pltpu.VMEM((HID, 4096), BF16),
            pltpu.VMEM((HID, 4096), BF16),
            pltpu.VMEM((256, 4096), BF16),
            pltpu.VMEM((FEAT, 4096), BF16),
            pltpu.VMEM((6, 128, ROW), F32),
            pltpu.VMEM((8, 128, 128), F32),
            pltpu.SemaphoreType.DMA((16,)),
            pltpu.SemaphoreType.DMA((6,)),
            pltpu.SemaphoreType.DMA((6,)),
        ],
        compiler_params=pltpu.CompilerParams(
            collective_id=0, has_side_effects=True, vmem_limit_bytes=LIMIT
        ),
    )(*[pltpu.with_memory_space_constraint(o, pltpu.HBM) for o in [*operands, t["ty"], t["tyk"]]])
    return grad.transpose(0, 1, 3, 2, 4), grad_in, grad_out.T, grad_bias


def solution(mesh):
    split = P("rep", None, "px", "py", None)
    both = ("px", "py")
    return jax.shard_map(
        shards,
        mesh=mesh,
        in_specs=(split, split, P(), P(), P()),
        out_specs=(split, P(both, "rep"), P("rep", both), P("rep", both)),
        check_vma=False,
    )
```

```python
import numpy as np

import jax
import jax.numpy as jnp
from jax import lax
from jax.experimental import pallas as pl
from jax.experimental.pallas import tpu as pltpu
from jax.sharding import PartitionSpec as P

F32 = jnp.float32
BF16 = jnp.bfloat16
MESH = pl.DeviceIdType.MESH
NN = (((1,), (0,)), ((), ()))
NT = (((1,), (1,)), ((), ()))
TN = (((0,), (0,)), ((), ()))

NG, KY, KZ, HID, FEAT = 256, 192, 96, 512, 192
CUT = NG // 3
NU_DT = 5e-05
TIME_STEP = 0.01
FORCING = 20.0
NDEV = 64
WY, WZ = 24, 12
SLOT = 48
ROW = 8 * SLOT
INV = 8
FEW, LAST = 3, 2
ORDER = (0, 1, FEW, LAST)
FWD = 2
SPARE = 208
PITCH = 72


def dot(a, b, dims=NN, **kw):
    return lax.dot_general(a, b, dims, preferred_element_type=F32, **kw)


def make_tables():
    bf = jnp.bfloat16

    def angle(k, x):
        theta = 2 * np.pi * ((np.asarray(k)[:, None] % NG) * np.asarray(x)[None, :] % NG) / NG
        return np.cos(theta) / np.sqrt(NG), np.sin(theta) / np.sqrt(NG)

    order_x = np.arange(NG).reshape(64, 4).T.reshape(-1)
    c, s = angle(order_x, np.arange(NG))
    tx = np.concatenate([c, -s], axis=1)
    order = np.arange(NG).reshape(64, 4).T.reshape(-1)
    ids = np.arange(KY)
    ky = np.where(ids < KY // 2, ids, ids - KY)
    c, s = angle(ky, order)
    top = np.concatenate([c, s], axis=1).reshape(8, 1, WY, 2 * NG)
    low = np.concatenate([-s, c], axis=1).reshape(8, 1, WY, 2 * NG)
    kcol = ky.reshape(8, 1, WY, 1)
    ty = np.concatenate([top, low], axis=1).reshape(2 * KY, 2 * NG)
    tyk = np.concatenate([-kcol * low, kcol * top], axis=1).reshape(2 * KY, 2 * NG)
    kz = (np.arange(8)[None, :, None] * WZ + np.arange(3)[:, None, None] * 4 + np.arange(4)[None, None, :]).reshape(-1)
    c, s = angle(order, kz)
    tz = np.concatenate([c, -s], axis=1)
    kk = np.concatenate([kz, kz])[None, :]
    tzk = np.concatenate([s, c], axis=1) * kk
    perm = np.zeros((FEAT, FEAT), np.float32)
    src = np.arange(FEAT).reshape(3, 4, 4, 4).transpose(2, 0, 1, 3).reshape(-1)
    perm[src, np.arange(FEAT)] = 1.0
    back = np.zeros((256, 256), np.float32)
    back[:FEAT, :FEAT] = perm.T
    back[FEAT, FEAT] = 1.0
    arrays = dict(tx=tx, ty=ty, tyk=tyk, tz=tz, tzk=tzk, tzt=tz.T, tzkt=tzk.T, perm=perm)
    out = {k: np.asarray(v, np.float32).astype(bf) for k, v in arrays.items()}
    out["back"] = back
    return out


def waves_of(m, j, l):
    kz_id = l * WZ + m
    kz = kz_id.astype(F32)
    a = lax.broadcasted_iota(jnp.int32, (WY, NG), 0) + j * WY
    n = lax.broadcasted_iota(jnp.int32, (WY, NG), 1)
    ky = jnp.where(a < KY // 2, a, a - KY).astype(F32)
    kx = jnp.where(n < NG // 2, n, n - NG).astype(F32)
    keep = (jnp.abs(kx) <= CUT) & (jnp.abs(ky) <= CUT) & (kz <= float(CUT))
    retained = keep.astype(F32)
    square = kx * kx + ky * ky + kz * kz
    damping = jnp.exp(-NU_DT * square)
    weight = jnp.where(kz_id == 0, 1.0, 2.0).astype(F32)
    return kx, ky, kz, retained, square, damping, weight


LIMIT = 52 * 1024 * 1024
LINES = FWD * ROW + 128
PART = 24
GRADS = 4


def place(f, mh):
    if f >= 6:
        return LAST, f * 3 + mh - 18
    g, pp = divmod(f * 3 + mh, 8)
    return (FEW if g == 2 else g), pp


def lane_select(lane, v, pick):
    slots = [q for q in range(8) if q * SLOT < (v + 1) * 128 and (q + 1) * SLOT > v * 128]
    value = pick(slots[0])
    for q in slots[1:]:
        value = jnp.where(lane >= float(q * SLOT - v * 128), pick(q), value)
    return value


def cross(a, b):
    return [a[1] * b[2] - a[2] * b[1], a[2] * b[0] - a[0] * b[2], a[0] * b[1] - a[1] * b[0]]


def main_kernel(
    state_hbm, cot_hbm, tx_hbm, tz_hbm, tzk_hbm, tzt_hbm, tzkt_hbm, perm_hbm, back_hbm, w_in_hbm, b_hbm, w_out_hbm,
    ty_hbm, tyk_hbm,
    out_ref, grad_in_ref, grad_out_ref, grad_bias_ref,
    state_ref, cot_ref, tx_ref, tz_ref, tzk_ref, tzt_ref, tzkt_ref, perm_ref, back_ref, w_in_t, b_row, w_out,
    s_ref, flat, sent, got, sent_few, got_few, v32, va32, o16, mine, gsent, ggot, ty_ref, tyk_ref,
    win, wint, woutt, bias, gin, gout, hid_all, pre_all, feat_all, adj_all, ky_part, spare, load_sem, send_sem, recv_sem,
):
    j, l = lax.axis_index("px"), lax.axis_index("py")
    me = j * 8 + l
    x, core, z, y = j >> 1, j & 1, l >> 2, l & 3
    l32, o32, kz_part, back = flat, v32, state_ref, sent

    def peer(k):
        k = k + jnp.where(k >= 3, 1, 0)
        dx = (k & 3) + 1
        dy = dx + ((k >> 2) & 3)
        px = (((x + dx) & 3) << 1) + ((core + (k >> 4)) & 1)
        py = (((z + (k >> 5)) & 1) << 2) + ((y + dy) & 3)
        return (px << 3) + py, {"px": px, "py": py}

    barrier = pltpu.get_barrier_semaphore()

    def greet(k, carry):
        pl.semaphore_signal(barrier, inc=1, device_id=peer(k)[1], device_id_type=MESH)
        return carry

    half = 2 * KY
    pairs = [(cot_hbm, cot_ref), (tx_hbm, tx_ref), (state_hbm, state_ref)]
    for src, dst in [(ty_hbm, ty_ref), (tyk_hbm, tyk_ref)]:
        pairs += [(src, dst.at[pl.ds(0, half)]), (src, dst.at[pl.ds(half, half)])]
    pairs += [(tz_hbm, tz_ref), (tzk_hbm, tzk_ref), (tzt_hbm, tzt_ref), (tzkt_hbm, tzkt_ref), (perm_hbm, perm_ref)]
    pairs += [(back_hbm, back_ref), (w_in_hbm, w_in_t), (b_hbm, b_row), (w_out_hbm, w_out)]
    loads = [pltpu.make_async_copy(src, dst, load_sem.at[n]) for n, (src, dst) in enumerate(pairs)]
    for load in loads:
        load.start()
    lax.fori_loop(0, NDEV - 1, greet, 0, unroll=3)

    def copy(src, dst, number, where):
        return pltpu.make_async_remote_copy(
            src_ref=src,
            dst_ref=dst,
            send_sem=send_sem.at[number],
            recv_sem=recv_sem.at[number],
            device_id=where,
            device_id_type=MESH,
        )

    def send_all(src, dst, number):
        def send(k, carry):
            t, where = peer(k)
            copy(src.at[t], dst.at[me], number, where).start()
            return carry

        dst[pl.ds(me, 1)] = src[pl.ds(me, 1)]
        lax.fori_loop(0, NDEV - 1, send, 0, unroll=3)

    def whole(src, dst, number):
        rest = pl.ds(0, NDEV - 1)
        return copy(src.at[rest], dst.at[rest], number, peer(0)[1])

    ways = [(sent.at[g], got.at[g]) for g in range(3)] + [(sent_few, got_few)]
    for group in ORDER:
        for load in [loads[0:2], loads[2:3], [], []][group]:
            load.wait()
        lanes = 128 if group == FEW else ROW

        def one(mp, carry):
            for mh in range(3):
                fields = [f for f in range(INV) if place(f, mh)[0] == group]
                if not fields:
                    continue
                m = mh * 4 + mp
                kx, ky, kz, retained, square, damping, weight = waves_of(m, j, l)
                value = {}
                if any(f >= 3 for f in fields):
                    scale = weight * retained
                    v = [[scale * state_ref[(c * 2 + r) * WZ + m] for r in range(2)] for c in range(3)]
                    value.update({3 + c: v[c] for c in range(3)})
                    value[6] = [-(kz * v[0][1] - kx * v[2][1]), kz * v[0][0] - kx * v[2][0]]
                    value[7] = [-(kx * v[1][1] - ky * v[0][1]), kx * v[1][0] - ky * v[0][0]]
                if any(f < 3 for f in fields):
                    inverse = 1.0 / jnp.maximum(square, 1.0)
                    scale = TIME_STEP * retained
                    force = [[], [], []]
                    for r in range(2):
                        w = [damping * cot_ref[c, r, m] for c in range(3)]
                        along = (kx * w[0] + ky * w[1] + kz * w[2]) * inverse
                        for c, k in enumerate((kx, ky, kz)):
                            force[c].append(scale * (w[c] - k * along))
                    value.update({c: force[c] for c in range(3)})
                for f in fields:
                    re, im = value[f]
                    top = jnp.concatenate([re, im], axis=1)
                    low = jnp.concatenate([im, -re], axis=1)
                    pp = place(f, mh)[1]
                    row = pp * SLOT if group == FEW else pl.multiple_of(((pp + j) & 7) * SLOT, 16)
                    s_ref[pl.ds(row, SLOT), :] = jnp.concatenate([top, low], axis=0).astype(BF16)
            for first in range(0, lanes, 256):
                width = min(256, lanes - first)
                out = dot(tx_ref[...], s_ref[first : first + width, :], NT)
                for c in range(width // 128):
                    for xx in range(4):
                        base = (first // 128 + c) * NDEV * PART
                        flat[pl.ds(base + mp * 4 + xx, NDEV, stride=PART), :] = out[
                            xx * 64 : (xx + 1) * 64, c * 128 : (c + 1) * 128
                        ]
            return carry

        lax.fori_loop(0, 4, one, 0)

        def pack(d, carry):
            for c in range(lanes // 128):
                row = pl.multiple_of(c * NDEV * PART + d * PART, 8)
                ways[group][0][d, :, c * 128 : (c + 1) * 128] = flat[pl.ds(row, 16), :].astype(BF16)
            return carry

        lax.fori_loop(0, NDEV, pack, 0, unroll=4)
        if group == 0:
            pl.semaphore_wait(barrier, NDEV - 1)
        send_all(*ways[group], group)

    lane = lax.broadcasted_iota(jnp.int32, (1, 128), 1).astype(BF16)
    lane = jnp.broadcast_to(lane, (128, 128))

    for load in loads[3:]:
        load.wait()
    perm = perm_ref[...]
    win[...] = dot(w_in_t[...], perm, TN).astype(BF16)
    wint[...] = dot(perm, w_in_t[...], TN).astype(BF16)
    woutt[...] = dot(w_out[...], perm, TN).astype(BF16)
    gin[...] = jnp.zeros_like(gin)
    gout[...] = jnp.zeros_like(gout)
    feat_all[FEAT:256, :] = jnp.ones((256 - FEAT, 4096), BF16)
    bias[...] = jnp.broadcast_to(b_row[...], (128, HID)).T

    BLOCKS = 27

    def block_of(f, mh):
        g, pp = place(f, mh)
        return 24 + mh if f == INV else {0: 0, 1: 8, FEW: 16, LAST: 18}[g] + pp

    def along_y(group):
        for f in range(INV):
            for mh in range(3):
                g, pp = place(f, mh)
                if g != group:
                    continue
                first = (8 - pp) * SLOT
                parts = []
                if group == FEW:
                    first = 0
                    for n in range(8):
                        rows = got_few[n * 8 : n * 8 + 8].reshape(128, 128).astype(F32)
                        parts.append(rows[:, pp * SLOT : (pp + 1) * SLOT])
                else:
                    for v in range(3):
                        pick = lambda q: got[
                            group, (q - pp) % 8 * 8 : (q - pp) % 8 * 8 + 8, :, v * 128 : (v + 1) * 128
                        ].reshape(128, 128)
                        parts.append(lane_select(lane, v, pick))
                left = jnp.concatenate(parts, axis=1).astype(BF16)
                todo = [(block_of(f, mh), dot(left, ty_ref[first : first + 2 * KY, :]))]
                if f == 5:
                    todo.append((24 + mh, -dot(left, tyk_ref[first : first + 2 * KY, :])))
                for block, out in todo:
                    for c in range(4):
                        row = (c * BLOCKS + block) * 128
                        flat[row : row + 128, :] = out[:, c * 128 : (c + 1) * 128]

    def columns(f, xx):
        parts = []
        for t in range(2):
            for mh in range(3):
                lanes = [
                    flat[pl.ds(((2 * t + h) * BLOCKS + block_of(f, mh)) * 128 + xx, 32, stride=4), :] for h in range(2)
                ]
                parts.append(jnp.concatenate(lanes, axis=1))
        return jnp.concatenate(parts, axis=0).astype(BF16)

    def along_z(fields):
        def one(xx, carry):
            for slot, f in fields:
                out = dot(tz_ref[...], columns(f, xx))
                if f == INV:
                    out = out + dot(tzk_ref[...], columns(4, xx))
                out = out.astype(BF16).astype(F32)
                for dz in range(4):
                    row = pl.multiple_of((slot * 16 + xx * 4 + dz) * PITCH, 8)
                    for h in range(2):
                        v32[h, pl.ds(row, 64), :] = out[dz * 64 : (dz + 1) * 64, h * 128 : (h + 1) * 128]
            return carry

        lax.fori_loop(0, 4, one, 0)

    def boxes(fields):
        def one(group, carry):
            cols = pl.ds(pl.multiple_of(group * 256, 256), 256)
            for slot, ref, c in fields:
                rows = [pl.ds(slot * 16 * PITCH + group * 4 + b, 16, stride=PITCH) for b in range(4)]
                planes = [[v32[h, r, :] for h in range(2)] for r in rows]
                for dy in range(4):
                    h, at = dy // 2, dy % 2 * 64
                    value = jnp.concatenate([q[h][:, at : at + 64] for q in planes], axis=1)
                    ref[dy * 48 + c * 16 : dy * 48 + (c + 1) * 16, cols] = value.astype(BF16)
            return carry

        lax.fori_loop(0, 16, one, 0, unroll=4 if len(fields) == 1 else 1)

    for group, fields in [(0, [(6, 0), (7, 1)]), (1, [(8, 2), (0, 3), (1, 4)]), (FEW, [(2, 5)])]:
        whole(*ways[group], group).wait_recv()
        along_y(group)
        along_z(fields)
        if group == 1:
            boxes([(6, adj_all, 0), (7, adj_all, 1), (8, adj_all, 2), (0, feat_all, 0), (1, feat_all, 1)])
    for group in (0, 1, FEW):
        whole(*ways[group], group).wait_send()

    def put(first, value, xx):
        for r in range(2):
            for mh in range(3):
                for h in range(2):
                    part = value[r * 96 + mh * 32 : r * 96 + (mh + 1) * 32, h * 128 : (h + 1) * 128]
                    if first < 12:
                        va32[h, pl.ds((r * 12 + first + mh) * 128 + xx, 32, stride=4), :] = part
                    else:
                        l32[pl.ds(((2 * r + h) * 9 + first + mh - 12) * 128 + xx, 32, stride=4), :] = part

    def plane(ref, c, xx, dz):
        row = pl.multiple_of((c * 16 + xx * 4 + dz) * PITCH, 8)
        return jnp.concatenate([ref[0, pl.ds(row, 64), :], ref[1, pl.ds(row, 64), :]], axis=1)

    def vort_z(xx, carry):
        parts = [[], [], []]
        for dz in range(4):
            vel = [plane(v32, c, xx, dz) for c in range(3)]
            frc = [plane(v32, 6 + c, xx, dz) for c in range(3)]
            for c, value in enumerate(cross(frc, vel)):
                parts[c].append(value.astype(BF16))
        wx, wy, wz = [jnp.concatenate(q, axis=0) for q in parts]
        tzt = tzt_ref[...]
        tzkt = tzkt_ref[...]
        kz_part[pl.ds(xx * 16, 8)] = dot(tzkt, wy).reshape(8, WY, NG)
        kz_part[pl.ds(xx * 16 + 8, 8)] = dot(tzkt, wx).reshape(8, WY, NG)
        put(0, dot(tzt, wy), xx)
        value = dot(tzt, wz)
        put(3, value, xx)
        put(6, value, xx)
        put(9, -dot(tzt, wx), xx)
        return carry

    def back_y(block, pp, table):
        first = (8 - pp) * SLOT
        parts = []
        for r in range(2):
            for h in range(2):
                if block < 12:
                    parts.append(va32[h, (r * 12 + block) * 128 : (r * 12 + block + 1) * 128, :])
                else:
                    row = ((2 * r + h) * 9 + block - 12) * 128
                    parts.append(l32[row : row + 128, :])
        return dot(jnp.concatenate(parts, axis=1).astype(BF16), table[first : first + 2 * KY, :], NT)

    def leave(g, used):
        for to in range(8):
            for v in range(3):
                pick = lambda q: o16[(q - to) % 8 % used, :, v * 128 : (v + 1) * 128]
                back[g, to * 8 : to * 8 + 8, :, v * 128 : (v + 1) * 128] = lane_select(lane, v, pick).reshape(8, 16, 128)
        send_all(back.at[g], mine.at[g], GRADS + 1 + g)

    lax.fori_loop(0, 4, vort_z, 0)
    for pp in range(6):
        o16[pp] = back_y(pp, pp, ty_ref).astype(BF16)
    leave(0, 6)
    for pp in range(6):
        ky_part[pp] = back_y(6 + pp, pp, tyk_ref)
    boxes([(2, feat_all, 2)])

    def closure(group, carry):
        bzs = [group * 4 + b for b in range(4)]
        cols = pl.ds(pl.multiple_of(group * 256, 256), 256)
        features = feat_all[0:FEAT, cols]
        adjoints = adj_all[:, cols]
        shift = bias[...]
        pre = dot(win[...], features) + jnp.concatenate([shift, shift], axis=1)
        sigmoid = 0.5 + 0.5 * jnp.tanh(0.5 * pre)
        hid_all[:, cols] = (pre * sigmoid).astype(BF16)
        hidden_adj = FORCING * dot(woutt[...], adjoints)
        pre_adj = (hidden_adj * sigmoid * (1.0 + pre * (1.0 - sigmoid))).astype(BF16)
        pre_all[:, cols] = pre_adj
        feat_adj = dot(wint[...], pre_adj)
        for b, bz in enumerate(bzs):
            for h in range(2):
                lanes = [feat_adj[dy * 48 : (dy + 1) * 48, b * 64 : (b + 1) * 64] for dy in (2 * h, 2 * h + 1)]
                va32[h, pl.ds(bz, 48, stride=PITCH), :] = jnp.concatenate(lanes, axis=1)
        return carry

    lax.fori_loop(0, 16, closure, 0, unroll=2)

    whole(*ways[LAST], LAST).wait_recv()
    along_y(LAST)
    along_z([(3, INV), (4, 6), (5, 7)])

    def vel_z(xx, carry):
        tzt = tzt_ref[...]
        parts = [[], [], []]
        for dz in range(4):
            spin = [plane(v32, 3 + c, xx, dz) for c in range(3)]
            frc = [plane(v32, 6 + c, xx, dz) for c in range(3)]
            for c, value in enumerate(cross(spin, frc)):
                parts[c].append((value + plane(va32, c, xx, dz)).astype(BF16))
        field = lambda c: jnp.concatenate(parts[c], axis=0)
        put(12, dot(tzt, field(0)) - kz_part[pl.ds(xx * 16, 8)].reshape(KY, NG), xx)
        put(15, dot(tzt, field(2)), xx)
        put(18, dot(tzt, field(1)) + kz_part[pl.ds(xx * 16 + 8, 8)].reshape(KY, NG), xx)
        return carry

    lax.fori_loop(0, 4, vel_z, 0)
    for pp in range(8):
        out = back_y(12 + pp, pp, ty_ref)
        o16[pp] = (out + ky_part[pp] if pp < 6 else out).astype(BF16)
    leave(1, 8)
    ninth = back_y(20, 0, ty_ref)
    for to in range(8):
        piece = ninth[:, to * SLOT : (to + 1) * SLOT]
        spare[to] = jnp.concatenate([jnp.zeros((128, SPARE - 128), F32), piece], axis=1)

    def products(k, carry):
        cols = pl.ds(pl.multiple_of(k * 1024, 1024), 1024)
        gin[...] += dot(pre_all[:, cols], feat_all[:, cols], NT)
        gout[:, 0:FEAT] += dot(hid_all[:, cols], adj_all[:, cols], NT)
        return carry

    lax.fori_loop(0, 4, products, 0)
    own_lane = lax.broadcasted_iota(jnp.int32, (16, 128), 1) < SPARE - 128

    def slices(d, carry):
        rows = pl.ds(pl.multiple_of(d * 8, 8), 8)
        extra = spare[d >> 3, pl.ds(pl.multiple_of((d & 7) * 16, 16), 16), :]
        lo = jnp.concatenate([gin[rows, 0:128], FORCING * gout[rows, 0:128]], axis=0)
        hi = jnp.concatenate([gin[rows, 128:256], FORCING * gout[rows, 128:256]], axis=0)
        gsent[d, :, 0:128] = lo.astype(BF16)
        gsent[d, :, 128:256] = jnp.where(own_lane, hi, extra).astype(BF16)
        return carry

    lax.fori_loop(0, NDEV, slices, 0, unroll=4)
    send_all(gsent, ggot, GRADS)

    def arrive(ref, chunk, lanes):
        def unpack(d, carry):
            row = pl.multiple_of((chunk * NDEV + d) * PART, 8)
            flat[pl.ds(row, 16), :] = ref[d, :, lanes : lanes + 128].astype(F32)
            return carry

        lax.fori_loop(0, NDEV, unpack, 0, unroll=8)

    def along_x(chunks):
        def one(mp, carry):
            for c in chunks:
                rows = [flat[pl.ds(c * NDEV * PART + mp * 4 + xx, NDEV, stride=PART), :] for xx in range(4)]
                out = dot(jnp.concatenate(rows, axis=0).astype(BF16), tx_ref[...], TN)
                for r in range(2):
                    for h in range(2):
                        row = pl.multiple_of((mp * 2 + r) * LINES + c * 128, 8)
                        o32[h, pl.ds(row, 128), :] = out[:, (2 * r + h) * 128 : (2 * r + h + 1) * 128]
            return carry

        lax.fori_loop(0, 4, one, 0)

    for g in range(FWD):
        whole(back.at[g], mine.at[g], GRADS + 1 + g).wait_recv()
        for c in range(3):
            arrive(mine.at[g], g * 3 + c, c * 128)
        along_x(range(g * 3, g * 3 + 3))
    whole(gsent, ggot, GRADS).wait_recv()
    arrive(ggot, 6, 128)
    along_x([6])

    total = lax.fori_loop(0, NDEV, lambda d, t: t + ggot[d].astype(F32), jnp.zeros((16, 256), F32), unroll=4)
    ordered = dot(total, back_ref[...], precision=lax.Precision.HIGHEST)
    grad_in_ref[...] = ordered[0:8, 0:FEAT]
    grad_out_ref[...] = ordered[8:16, 0:FEAT]
    pick = (lax.broadcasted_iota(jnp.int32, (8, 256), 1) == FEAT).astype(F32)
    grad_bias_ref[...] = dot(pick, total[0:8], NT, precision=lax.Precision.HIGHEST)[0:1]

    def finish(mp, carry):
        for mh in range(3):
            m = mh * 4 + mp
            kx, ky, kz, retained, square, damping, weight = waves_of(m, j, l)
            scale = weight * retained
            parts = []
            for g, piece in [(0, mh), (0, 3 + mh), (1, mh), (1, 3 + mh), (1, 6 + mh)]:
                place = g * ROW + ((piece + j) & 7) * SLOT if piece < 8 else FWD * ROW + SPARE - 128
                row = pl.multiple_of(mp * 2 * LINES + place, 8)
                wave = lambda r, s: jnp.concatenate([o32[h, pl.ds(row + r * LINES + s * WY, WY), :] for h in range(2)], axis=1)
                parts.append((wave(0, 0) - wave(1, 1), wave(0, 1) + wave(1, 0)))
            wy, wz, ax, az, ay = parts
            spec = [
                ax,
                (ay[0] + kx * wz[1], ay[1] - kx * wz[0]),
                (az[0] - kx * wy[1], az[1] + kx * wy[0]),
            ]
            for c in range(3):
                for r in range(2):
                    out_ref[c, r, m] = damping * cot_ref[c, r, m] + scale * spec[c][r]
        return carry

    lax.fori_loop(0, 4, finish, 0)
    whole(*ways[LAST], LAST).wait_send()
    whole(gsent, ggot, GRADS).wait_send()
    for g in range(FWD):
        whole(back.at[g], mine.at[g], GRADS + 1 + g).wait_send()


ANY = pl.BlockSpec(memory_space=pltpu.HBM)
VMEM = pl.BlockSpec(memory_space=pltpu.VMEM)


def shards(state, cotangent, w_in, b_in, w_out):
    t = {k: jnp.asarray(v) for k, v in make_tables().items()}
    sds = jax.ShapeDtypeStruct
    operands = [state.transpose(0, 1, 3, 2, 4).reshape(6 * WZ, WY, NG), cotangent.transpose(0, 1, 3, 2, 4)]
    operands += [t[k] for k in ("tx", "tz", "tzk", "tzt", "tzkt", "perm", "back")]
    operands += [w_in.T, b_in[None, :], w_out]
    grad, grad_in, grad_out, grad_bias = pl.pallas_call(
        main_kernel,
        out_shape=(sds((3, 2, WZ, WY, NG), F32), sds((8, FEAT), F32), sds((8, FEAT), F32), sds((1, 8), F32)),
        in_specs=[ANY] * 14,
        out_specs=(VMEM,) * 4,
        scratch_shapes=[pltpu.VMEM(o.shape, o.dtype) for o in operands]
        + [
            pltpu.VMEM((ROW, 2 * NG), BF16),
            pltpu.VMEM((4 * 27 * 128, 128), F32),
            pltpu.VMEM((3, NDEV, 16, ROW), BF16),
            pltpu.VMEM((3, NDEV, 16, ROW), BF16),
            pltpu.VMEM((NDEV, 16, 128), BF16),
            pltpu.VMEM((NDEV, 16, 128), BF16),
            pltpu.VMEM((2, 144 * PITCH, 128), F32),
            pltpu.VMEM((2, 48 * PITCH, 128), F32),
            pltpu.VMEM((8, 128, ROW), BF16),
            pltpu.VMEM((FWD, NDEV, 16, ROW), BF16),
            pltpu.VMEM((NDEV, 16, 256), BF16),
            pltpu.VMEM((NDEV, 16, 256), BF16),
            pltpu.VMEM((4 * KY, 2 * NG), BF16),
            pltpu.VMEM((4 * KY, 2 * NG), BF16),
            pltpu.VMEM((HID, FEAT), BF16),
            pltpu.VMEM((FEAT, HID), BF16),
            pltpu.VMEM((HID, FEAT), BF16),
            pltpu.VMEM((HID, 128), F32),
            pltpu.VMEM((HID, 256), F32),
            pltpu.VMEM((HID, 256), F32),
            pltpu.VMEM((HID, 4096), BF16),
            pltpu.VMEM((HID, 4096), BF16),
            pltpu.VMEM((256, 4096), BF16),
            pltpu.VMEM((FEAT, 4096), BF16),
            pltpu.VMEM((6, 128, ROW), F32),
            pltpu.VMEM((8, 128, 128), F32),
            pltpu.SemaphoreType.DMA((16,)),
            pltpu.SemaphoreType.DMA((7,)),
            pltpu.SemaphoreType.DMA((7,)),
        ],
        compiler_params=pltpu.CompilerParams(
            collective_id=0, has_side_effects=True, vmem_limit_bytes=LIMIT
        ),
    )(*[pltpu.with_memory_space_constraint(o, pltpu.HBM) for o in [*operands, t["ty"], t["tyk"]]])
    return grad.transpose(0, 1, 3, 2, 4), grad_in, grad_out.T, grad_bias


def solution(mesh):
    split = P("rep", None, "px", "py", None)
    both = ("px", "py")
    return jax.shard_map(
        shards,
        mesh=mesh,
        in_specs=(split, split, P(), P(), P()),
        out_specs=(split, P(both, "rep"), P("rep", both), P("rep", both)),
        check_vma=False,
    )
```

```python
import numpy as np

import jax
import jax.numpy as jnp
from jax import lax
from jax.experimental import pallas as pl
from jax.experimental.pallas import tpu as pltpu
from jax.sharding import PartitionSpec as P

F32 = jnp.float32
BF16 = jnp.bfloat16
MESH = pl.DeviceIdType.MESH
NN = (((1,), (0,)), ((), ()))
NT = (((1,), (1,)), ((), ()))
TN = (((0,), (0,)), ((), ()))

NG, KY, KZ, HID, FEAT = 256, 192, 96, 512, 192
CUT = NG // 3
NU_DT = 5e-05
TIME_STEP = 0.01
FORCING = 20.0
NDEV = 64
WY, WZ = 24, 12
SLOT = 48
ROW = 8 * SLOT
INV = 8
FEW, LAST = 3, 2
ORDER = (0, 1, FEW, LAST)
FWD = 2
SPARE = 208
PITCH = 72


def dot(a, b, dims=NN, **kw):
    return lax.dot_general(a, b, dims, preferred_element_type=F32, **kw)


def make_tables():
    bf = jnp.bfloat16

    def angle(k, x):
        theta = 2 * np.pi * ((np.asarray(k)[:, None] % NG) * np.asarray(x)[None, :] % NG) / NG
        return np.cos(theta) / np.sqrt(NG), np.sin(theta) / np.sqrt(NG)

    order_x = np.arange(NG).reshape(64, 4).T.reshape(-1)
    c, s = angle(order_x, np.arange(NG))
    tx = np.concatenate([c, -s], axis=1)
    order = np.arange(NG).reshape(64, 4).T.reshape(-1)
    ids = np.arange(KY)
    ky = np.where(ids < KY // 2, ids, ids - KY)
    c, s = angle(ky, order)
    top = np.concatenate([c, s], axis=1).reshape(8, 1, WY, 2 * NG)
    low = np.concatenate([-s, c], axis=1).reshape(8, 1, WY, 2 * NG)
    kcol = ky.reshape(8, 1, WY, 1)
    ty = np.concatenate([top, low], axis=1).reshape(2 * KY, 2 * NG)
    tyk = np.concatenate([-kcol * low, kcol * top], axis=1).reshape(2 * KY, 2 * NG)
    kz = (np.arange(8)[None, :, None] * WZ + np.arange(3)[:, None, None] * 4 + np.arange(4)[None, None, :]).reshape(-1)
    c, s = angle(order, kz)
    tz = np.concatenate([c, -s], axis=1)
    kk = np.concatenate([kz, kz])[None, :]
    tzk = np.concatenate([s, c], axis=1) * kk
    perm = np.zeros((FEAT, FEAT), np.float32)
    src = np.arange(FEAT).reshape(3, 4, 4, 4).transpose(2, 0, 1, 3).reshape(-1)
    perm[src, np.arange(FEAT)] = 1.0
    back = np.zeros((256, 256), np.float32)
    back[:FEAT, :FEAT] = perm.T
    back[FEAT, FEAT] = 1.0
    arrays = dict(tx=tx, ty=ty, tyk=tyk, tz=tz, tzk=tzk, tzt=tz.T, tzkt=tzk.T, perm=perm)
    out = {k: np.asarray(v, np.float32).astype(bf) for k, v in arrays.items()}
    out["back"] = back
    return out


def waves_of(m, j, l):
    kz_id = l * WZ + m
    kz = kz_id.astype(F32)
    a = lax.broadcasted_iota(jnp.int32, (WY, NG), 0) + j * WY
    n = lax.broadcasted_iota(jnp.int32, (WY, NG), 1)
    ky = jnp.where(a < KY // 2, a, a - KY).astype(F32)
    kx = jnp.where(n < NG // 2, n, n - NG).astype(F32)
    keep = (jnp.abs(kx) <= CUT) & (jnp.abs(ky) <= CUT) & (kz <= float(CUT))
    retained = keep.astype(F32)
    square = kx * kx + ky * ky + kz * kz
    damping = jnp.exp(-NU_DT * square)
    weight = jnp.where(kz_id == 0, 1.0, 2.0).astype(F32)
    return kx, ky, kz, retained, square, damping, weight


LIMIT = 52 * 1024 * 1024
LINES = FWD * ROW + 128
PART = 24
GRADS = 4


def place(f, mh):
    if f >= 6:
        return LAST, f * 3 + mh - 18
    g, pp = divmod(f * 3 + mh, 8)
    return (FEW if g == 2 else g), pp


def lane_select(lane, v, pick):
    slots = [q for q in range(8) if q * SLOT < (v + 1) * 128 and (q + 1) * SLOT > v * 128]
    value = pick(slots[0])
    for q in slots[1:]:
        value = jnp.where(lane >= float(q * SLOT - v * 128), pick(q), value)
    return value


def cross(a, b):
    return [a[1] * b[2] - a[2] * b[1], a[2] * b[0] - a[0] * b[2], a[0] * b[1] - a[1] * b[0]]


def main_kernel(
    state_hbm, cot_hbm, tx_hbm, tz_hbm, tzk_hbm, tzt_hbm, tzkt_hbm, perm_hbm, back_hbm, w_in_hbm, b_hbm, w_out_hbm,
    ty_hbm, tyk_hbm,
    out_ref, grad_in_ref, grad_out_ref, grad_bias_ref,
    state_ref, cot_ref, tx_ref, tz_ref, tzk_ref, tzt_ref, tzkt_ref, perm_ref, back_ref, w_in_t, b_row, w_out,
    s_ref, flat, sent, got, sent_few, got_few, v32, va32, o16, mine, gsent, ggot, ty_ref, tyk_ref,
    win, wint, woutt, bias, gin, gout, hid_all, pre_all, feat_all, adj_all, ky_part, spare, load_sem, send_sem, recv_sem,
):
    j, l = lax.axis_index("px"), lax.axis_index("py")
    me = j * 8 + l
    x, core, z, y = j >> 1, j & 1, l >> 2, l & 3
    l32, o32, kz_part, back = flat, v32, state_ref, sent

    def peer(k):
        k = k + jnp.where(k >= 3, 1, 0)
        dx = (k & 3) + 1
        dy = dx + ((k >> 2) & 3)
        px = (((x + dx) & 3) << 1) + ((core + (k >> 4)) & 1)
        py = (((z + (k >> 5)) & 1) << 2) + ((y + dy) & 3)
        return (px << 3) + py, {"px": px, "py": py}

    barrier = pltpu.get_barrier_semaphore()

    def greet(k, carry):
        pl.semaphore_signal(barrier, inc=1, device_id=peer(k)[1], device_id_type=MESH)
        return carry

    half = 2 * KY
    pairs = [(cot_hbm, cot_ref), (tx_hbm, tx_ref), (state_hbm, state_ref)]
    for src, dst in [(ty_hbm, ty_ref), (tyk_hbm, tyk_ref)]:
        pairs += [(src, dst.at[pl.ds(0, half)]), (src, dst.at[pl.ds(half, half)])]
    pairs += [(tz_hbm, tz_ref), (tzk_hbm, tzk_ref), (tzt_hbm, tzt_ref), (tzkt_hbm, tzkt_ref), (perm_hbm, perm_ref)]
    pairs += [(back_hbm, back_ref), (w_in_hbm, w_in_t), (b_hbm, b_row), (w_out_hbm, w_out)]
    loads = [pltpu.make_async_copy(src, dst, load_sem.at[n]) for n, (src, dst) in enumerate(pairs)]
    for load in loads:
        load.start()
    lax.fori_loop(0, NDEV - 1, greet, 0, unroll=3)

    def copy(src, dst, number, where):
        return pltpu.make_async_remote_copy(
            src_ref=src,
            dst_ref=dst,
            send_sem=send_sem.at[number],
            recv_sem=recv_sem.at[number],
            device_id=where,
            device_id_type=MESH,
        )

    def send_all(src, dst, number):
        def send(k, carry):
            t, where = peer(k)
            copy(src.at[t], dst.at[me], number, where).start()
            return carry

        dst[pl.ds(me, 1)] = src[pl.ds(me, 1)]
        lax.fori_loop(0, NDEV - 1, send, 0, unroll=3)

    def whole(src, dst, number):
        rest = pl.ds(0, NDEV - 1)
        return copy(src.at[rest], dst.at[rest], number, peer(0)[1])

    ways = [(sent.at[g], got.at[g]) for g in range(3)] + [(sent_few, got_few)]
    for group in ORDER:
        for load in [loads[0:2], loads[2:3], [], []][group]:
            load.wait()
        lanes = 128 if group == FEW else ROW

        def one(mp, carry):
            for mh in range(3):
                fields = [f for f in range(INV) if place(f, mh)[0] == group]
                if not fields:
                    continue
                m = mh * 4 + mp
                kx, ky, kz, retained, square, damping, weight = waves_of(m, j, l)
                value = {}
                if any(f >= 3 for f in fields):
                    scale = weight * retained
                    v = [[scale * state_ref[(c * 2 + r) * WZ + m] for r in range(2)] for c in range(3)]
                    value.update({3 + c: v[c] for c in range(3)})
                    value[6] = [-(kz * v[0][1] - kx * v[2][1]), kz * v[0][0] - kx * v[2][0]]
                    value[7] = [-(kx * v[1][1] - ky * v[0][1]), kx * v[1][0] - ky * v[0][0]]
                if any(f < 3 for f in fields):
                    inverse = 1.0 / jnp.maximum(square, 1.0)
                    scale = TIME_STEP * retained
                    force = [[], [], []]
                    for r in range(2):
                        w = [damping * cot_ref[c, r, m] for c in range(3)]
                        along = (kx * w[0] + ky * w[1] + kz * w[2]) * inverse
                        for c, k in enumerate((kx, ky, kz)):
                            force[c].append(scale * (w[c] - k * along))
                    value.update({c: force[c] for c in range(3)})
                for f in fields:
                    re, im = value[f]
                    top = jnp.concatenate([re, im], axis=1)
                    low = jnp.concatenate([im, -re], axis=1)
                    pp = place(f, mh)[1]
                    row = pp * SLOT if group == FEW else pl.multiple_of(((pp + j) & 7) * SLOT, 16)
                    s_ref[pl.ds(row, SLOT), :] = jnp.concatenate([top, low], axis=0).astype(BF16)
            for first in range(0, lanes, 256):
                width = min(256, lanes - first)
                out = dot(tx_ref[...], s_ref[first : first + width, :], NT)
                for c in range(width // 128):
                    for xx in range(4):
                        base = (first // 128 + c) * NDEV * PART
                        flat[pl.ds(base + mp * 4 + xx, NDEV, stride=PART), :] = out[
                            xx * 64 : (xx + 1) * 64, c * 128 : (c + 1) * 128
                        ]
            return carry

        lax.fori_loop(0, 4, one, 0)

        def pack(d, carry):
            for c in range(lanes // 128):
                row = pl.multiple_of(c * NDEV * PART + d * PART, 8)
                ways[group][0][d, :, c * 128 : (c + 1) * 128] = flat[pl.ds(row, 16), :].astype(BF16)
            return carry

        lax.fori_loop(0, NDEV, pack, 0, unroll=4)
        if group == 0:
            pl.semaphore_wait(barrier, NDEV - 1)
        send_all(*ways[group], group)

    lane = lax.broadcasted_iota(jnp.int32, (1, 128), 1).astype(BF16)
    lane = jnp.broadcast_to(lane, (128, 128))

    for load in loads[3:]:
        load.wait()
    perm = perm_ref[...]
    win[...] = dot(w_in_t[...], perm, TN).astype(BF16)
    wint[...] = dot(perm, w_in_t[...], TN).astype(BF16)
    woutt[...] = dot(w_out[...], perm, TN).astype(BF16)
    gin[...] = jnp.zeros_like(gin)
    gout[...] = jnp.zeros_like(gout)
    feat_all[FEAT:256, :] = jnp.ones((256 - FEAT, 4096), BF16)
    bias[...] = jnp.broadcast_to(b_row[...], (128, HID)).T

    BLOCKS = 27

    def block_of(f, mh):
        g, pp = place(f, mh)
        return 24 + mh if f == INV else {0: 0, 1: 8, FEW: 16, LAST: 18}[g] + pp

    def along_y(group):
        for f in range(INV):
            for mh in range(3):
                g, pp = place(f, mh)
                if g != group:
                    continue
                first = (8 - pp) * SLOT
                parts = []
                if group == FEW:
                    first = 0
                    for n in range(8):
                        rows = got_few[n * 8 : n * 8 + 8].reshape(128, 128).astype(F32)
                        parts.append(rows[:, pp * SLOT : (pp + 1) * SLOT])
                else:
                    for v in range(3):
                        pick = lambda q: got[
                            group, (q - pp) % 8 * 8 : (q - pp) % 8 * 8 + 8, :, v * 128 : (v + 1) * 128
                        ].reshape(128, 128)
                        parts.append(lane_select(lane, v, pick))
                left = jnp.concatenate(parts, axis=1).astype(BF16)
                todo = [(block_of(f, mh), dot(left, ty_ref[first : first + 2 * KY, :]))]
                if f == 5:
                    todo.append((24 + mh, -dot(left, tyk_ref[first : first + 2 * KY, :])))
                for block, out in todo:
                    for c in range(4):
                        row = (c * BLOCKS + block) * 128
                        flat[row : row + 128, :] = out[:, c * 128 : (c + 1) * 128]

    def columns(f, xx):
        parts = []
        for t in range(2):
            for mh in range(3):
                lanes = [
                    flat[pl.ds(((2 * t + h) * BLOCKS + block_of(f, mh)) * 128 + xx, 32, stride=4), :] for h in range(2)
                ]
                parts.append(jnp.concatenate(lanes, axis=1))
        return jnp.concatenate(parts, axis=0).astype(BF16)

    def along_z(fields):
        def one(xx, carry):
            for slot, f in fields:
                out = dot(tz_ref[...], columns(f, xx))
                if f == INV:
                    out = out + dot(tzk_ref[...], columns(4, xx))
                out = out.astype(BF16).astype(F32)
                for dz in range(4):
                    row = pl.multiple_of((slot * 16 + xx * 4 + dz) * PITCH, 8)
                    for h in range(2):
                        v32[h, pl.ds(row, 64), :] = out[dz * 64 : (dz + 1) * 64, h * 128 : (h + 1) * 128]
            return carry

        lax.fori_loop(0, 4, one, 0, unroll=4 if len(fields) == 1 else 2)

    def boxes(fields):
        def one(group, carry):
            cols = pl.ds(pl.multiple_of(group * 256, 256), 256)
            for slot, ref, c in fields:
                rows = [pl.ds(slot * 16 * PITCH + group * 4 + b, 16, stride=PITCH) for b in range(4)]
                planes = [[v32[h, r, :] for h in range(2)] for r in rows]
                for dy in range(4):
                    h, at = dy // 2, dy % 2 * 64
                    value = jnp.concatenate([q[h][:, at : at + 64] for q in planes], axis=1)
                    ref[dy * 48 + c * 16 : dy * 48 + (c + 1) * 16, cols] = value.astype(BF16)
            return carry

        lax.fori_loop(0, 16, one, 0, unroll=4 if len(fields) == 1 else 2)

    for group, fields in [(0, [(6, 0), (7, 1)]), (1, [(8, 2), (0, 3), (1, 4)]), (FEW, [(2, 5)])]:
        whole(*ways[group], group).wait_recv()
        along_y(group)
        along_z(fields)
        if group == 0:
            boxes([(6, adj_all, 0), (7, adj_all, 1)])
        if group == 1:
            boxes([(8, adj_all, 2), (0, feat_all, 0), (1, feat_all, 1)])
    for group in (0, 1, FEW):
        whole(*ways[group], group).wait_send()

    def put(first, value, xx):
        for r in range(2):
            for mh in range(3):
                for h in range(2):
                    part = value[r * 96 + mh * 32 : r * 96 + (mh + 1) * 32, h * 128 : (h + 1) * 128]
                    if first < 12:
                        va32[h, pl.ds((r * 12 + first + mh) * 128 + xx, 32, stride=4), :] = part
                    else:
                        l32[pl.ds(((2 * r + h) * 9 + first + mh - 12) * 128 + xx, 32, stride=4), :] = part

    def plane(ref, c, xx, dz):
        row = pl.multiple_of((c * 16 + xx * 4 + dz) * PITCH, 8)
        return jnp.concatenate([ref[0, pl.ds(row, 64), :], ref[1, pl.ds(row, 64), :]], axis=1)

    def vort_z(xx, carry):
        parts = [[], [], []]
        for dz in range(4):
            vel = [plane(v32, c, xx, dz) for c in range(3)]
            frc = [plane(v32, 6 + c, xx, dz) for c in range(3)]
            for c, value in enumerate(cross(frc, vel)):
                parts[c].append(value.astype(BF16))
        wx, wy, wz = [jnp.concatenate(q, axis=0) for q in parts]
        tzt = tzt_ref[...]
        tzkt = tzkt_ref[...]
        kz_part[pl.ds(xx * 16, 8)] = dot(tzkt, wy).reshape(8, WY, NG)
        kz_part[pl.ds(xx * 16 + 8, 8)] = dot(tzkt, wx).reshape(8, WY, NG)
        put(0, dot(tzt, wy), xx)
        value = dot(tzt, wz)
        put(3, value, xx)
        put(6, value, xx)
        put(9, -dot(tzt, wx), xx)
        return carry

    def back_y(block, pp, table):
        first = (8 - pp) * SLOT
        parts = []
        for r in range(2):
            for h in range(2):
                if block < 12:
                    parts.append(va32[h, (r * 12 + block) * 128 : (r * 12 + block + 1) * 128, :])
                else:
                    row = ((2 * r + h) * 9 + block - 12) * 128
                    parts.append(l32[row : row + 128, :])
        return dot(jnp.concatenate(parts, axis=1).astype(BF16), table[first : first + 2 * KY, :], NT)

    def leave(g, used):
        for to in range(8):
            for v in range(3):
                pick = lambda q: o16[(q - to) % 8 % used, :, v * 128 : (v + 1) * 128]
                back[g, to * 8 : to * 8 + 8, :, v * 128 : (v + 1) * 128] = lane_select(lane, v, pick).reshape(8, 16, 128)
        send_all(back.at[g], mine.at[g], GRADS + 1 + g)

    lax.fori_loop(0, 4, vort_z, 0, unroll=2)
    for pp in range(6):
        o16[pp] = back_y(pp, pp, ty_ref).astype(BF16)
    leave(0, 6)
    for pp in range(6):
        ky_part[pp] = back_y(6 + pp, pp, tyk_ref)
    boxes([(2, feat_all, 2)])

    def closure(group, carry):
        bzs = [group * 4 + b for b in range(4)]
        cols = pl.ds(pl.multiple_of(group * 256, 256), 256)
        features = feat_all[0:FEAT, cols]
        adjoints = adj_all[:, cols]
        shift = bias[...]
        pre = dot(win[...], features) + jnp.concatenate([shift, shift], axis=1)
        sigmoid = 0.5 + 0.5 * jnp.tanh(0.5 * pre)
        hid_all[:, cols] = (pre * sigmoid).astype(BF16)
        hidden_adj = FORCING * dot(woutt[...], adjoints)
        pre_adj = (hidden_adj * sigmoid * (1.0 + pre * (1.0 - sigmoid))).astype(BF16)
        pre_all[:, cols] = pre_adj
        feat_adj = dot(wint[...], pre_adj)
        for b, bz in enumerate(bzs):
            for h in range(2):
                lanes = [feat_adj[dy * 48 : (dy + 1) * 48, b * 64 : (b + 1) * 64] for dy in (2 * h, 2 * h + 1)]
                va32[h, pl.ds(bz, 48, stride=PITCH), :] = jnp.concatenate(lanes, axis=1)
        return carry

    lax.fori_loop(0, 16, closure, 0, unroll=2)

    whole(*ways[LAST], LAST).wait_recv()
    along_y(LAST)
    along_z([(3, INV), (4, 6), (5, 7)])

    def vel_z(xx, carry):
        tzt = tzt_ref[...]
        parts = [[], [], []]
        for dz in range(4):
            spin = [plane(v32, 3 + c, xx, dz) for c in range(3)]
            frc = [plane(v32, 6 + c, xx, dz) for c in range(3)]
            for c, value in enumerate(cross(spin, frc)):
                parts[c].append((value + plane(va32, c, xx, dz)).astype(BF16))
        field = lambda c: jnp.concatenate(parts[c], axis=0)
        put(12, dot(tzt, field(0)) - kz_part[pl.ds(xx * 16, 8)].reshape(KY, NG), xx)
        put(15, dot(tzt, field(2)), xx)
        put(18, dot(tzt, field(1)) + kz_part[pl.ds(xx * 16 + 8, 8)].reshape(KY, NG), xx)
        return carry

    lax.fori_loop(0, 4, vel_z, 0, unroll=2)
    for pp in range(8):
        out = back_y(12 + pp, pp, ty_ref)
        o16[pp] = (out + ky_part[pp] if pp < 6 else out).astype(BF16)
    leave(1, 8)
    ninth = back_y(20, 0, ty_ref)
    for to in range(8):
        piece = ninth[:, to * SLOT : (to + 1) * SLOT]
        spare[to] = jnp.concatenate([jnp.zeros((128, SPARE - 128), F32), piece], axis=1)

    def products(k, carry):
        cols = pl.ds(pl.multiple_of(k * 1024, 1024), 1024)
        gin[...] += dot(pre_all[:, cols], feat_all[:, cols], NT)
        gout[:, 0:FEAT] += dot(hid_all[:, cols], adj_all[:, cols], NT)
        return carry

    lax.fori_loop(0, 4, products, 0)
    own_lane = lax.broadcasted_iota(jnp.int32, (16, 128), 1) < SPARE - 128

    def slices(d, carry):
        rows = pl.ds(pl.multiple_of(d * 8, 8), 8)
        extra = spare[d >> 3, pl.ds(pl.multiple_of((d & 7) * 16, 16), 16), :]
        lo = jnp.concatenate([gin[rows, 0:128], FORCING * gout[rows, 0:128]], axis=0)
        hi = jnp.concatenate([gin[rows, 128:256], FORCING * gout[rows, 128:256]], axis=0)
        gsent[d, :, 0:128] = lo.astype(BF16)
        gsent[d, :, 128:256] = jnp.where(own_lane, hi, extra).astype(BF16)
        return carry

    lax.fori_loop(0, NDEV, slices, 0, unroll=4)
    send_all(gsent, ggot, GRADS)

    def arrive(ref, chunk, lanes):
        def unpack(d, carry):
            row = pl.multiple_of((chunk * NDEV + d) * PART, 8)
            flat[pl.ds(row, 16), :] = ref[d, :, lanes : lanes + 128].astype(F32)
            return carry

        lax.fori_loop(0, NDEV, unpack, 0, unroll=8)

    def along_x(chunks):
        def one(mp, carry):
            for c in chunks:
                rows = [flat[pl.ds(c * NDEV * PART + mp * 4 + xx, NDEV, stride=PART), :] for xx in range(4)]
                out = dot(jnp.concatenate(rows, axis=0).astype(BF16), tx_ref[...], TN)
                for r in range(2):
                    for h in range(2):
                        row = pl.multiple_of((mp * 2 + r) * LINES + c * 128, 8)
                        o32[h, pl.ds(row, 128), :] = out[:, (2 * r + h) * 128 : (2 * r + h + 1) * 128]
            return carry

        lax.fori_loop(0, 4, one, 0)

    def finish(late):
        def one(mp, carry):
            for mh in range(2 if late else 0, 3):
                m = mh * 4 + mp
                kx, ky, kz, retained, square, damping, weight = waves_of(m, j, l)
                scale = weight * retained

                def part(g, piece):
                    at = g * ROW + ((piece + j) & 7) * SLOT if piece < 8 else FWD * ROW + SPARE - 128
                    row = pl.multiple_of(mp * 2 * LINES + at, 8)
                    wave = lambda r, s: jnp.concatenate(
                        [o32[h, pl.ds(row + r * LINES + s * WY, WY), :] for h in range(2)], axis=1
                    )
                    return wave(0, 0) - wave(1, 1), wave(0, 1) + wave(1, 0)

                spec = {}
                if not late:
                    az, wy = part(1, 3 + mh), part(0, mh)
                    spec[0] = part(1, mh)
                    spec[2] = (az[0] - kx * wy[1], az[1] + kx * wy[0])
                if late or mh < 2:
                    ay, wz = part(1, 6 + mh), part(0, 3 + mh)
                    spec[1] = (ay[0] + kx * wz[1], ay[1] - kx * wz[0])
                for c, value in spec.items():
                    for r in range(2):
                        out_ref[c, r, m] = damping * cot_ref[c, r, m] + scale * value[r]
            return carry

        lax.fori_loop(0, 4, one, 0)

    for g in range(FWD):
        whole(back.at[g], mine.at[g], GRADS + 1 + g).wait_recv()
        for c in range(3):
            arrive(mine.at[g], g * 3 + c, c * 128)
        along_x(range(g * 3, g * 3 + 3))
    finish(False)
    whole(gsent, ggot, GRADS).wait_recv()
    arrive(ggot, 6, 128)
    along_x([6])
    finish(True)

    total = lax.fori_loop(0, NDEV, lambda d, t: t + ggot[d].astype(F32), jnp.zeros((16, 256), F32), unroll=4)
    ordered = dot(total, back_ref[...], precision=lax.Precision.HIGHEST)
    grad_in_ref[...] = ordered[0:8, 0:FEAT]
    grad_out_ref[...] = ordered[8:16, 0:FEAT]
    pick = (lax.broadcasted_iota(jnp.int32, (8, 256), 1) == FEAT).astype(F32)
    grad_bias_ref[...] = dot(pick, total[0:8], NT, precision=lax.Precision.HIGHEST)[0:1]

    whole(*ways[LAST], LAST).wait_send()
    whole(gsent, ggot, GRADS).wait_send()
    for g in range(FWD):
        whole(back.at[g], mine.at[g], GRADS + 1 + g).wait_send()


def copy_out(*refs):
    sources, results, sem = refs[:4], refs[4:8], refs[8]
    copies = [pltpu.make_async_copy(a, b, sem.at[n]) for n, (a, b) in enumerate(zip(sources, results))]
    for copy in copies:
        copy.start()
    for copy in copies:
        copy.wait()


ANY = pl.BlockSpec(memory_space=pltpu.HBM)
VMEM = pl.BlockSpec(memory_space=pltpu.VMEM)


def shards(state, cotangent, w_in, b_in, w_out):
    t = {k: jnp.asarray(v) for k, v in make_tables().items()}
    sds = jax.ShapeDtypeStruct
    operands = [state.transpose(0, 1, 3, 2, 4).reshape(6 * WZ, WY, NG), cotangent.transpose(0, 1, 3, 2, 4)]
    operands += [t[k] for k in ("tx", "tz", "tzk", "tzt", "tzkt", "perm", "back")]
    operands += [w_in.T, b_in[None, :], w_out]
    results = pl.pallas_call(
        main_kernel,
        out_shape=(sds((3, 2, WZ, WY, NG), F32), sds((8, FEAT), F32), sds((8, FEAT), F32), sds((1, 8), F32)),
        in_specs=[ANY] * 14,
        out_specs=(VMEM,) * 4,
        scratch_shapes=[pltpu.VMEM(o.shape, o.dtype) for o in operands]
        + [
            pltpu.VMEM((ROW, 2 * NG), BF16),
            pltpu.VMEM((4 * 27 * 128, 128), F32),
            pltpu.VMEM((3, NDEV, 16, ROW), BF16),
            pltpu.VMEM((3, NDEV, 16, ROW), BF16),
            pltpu.VMEM((NDEV, 16, 128), BF16),
            pltpu.VMEM((NDEV, 16, 128), BF16),
            pltpu.VMEM((2, 144 * PITCH, 128), F32),
            pltpu.VMEM((2, 48 * PITCH, 128), F32),
            pltpu.VMEM((8, 128, ROW), BF16),
            pltpu.VMEM((FWD, NDEV, 16, ROW), BF16),
            pltpu.VMEM((NDEV, 16, 256), BF16),
            pltpu.VMEM((NDEV, 16, 256), BF16),
            pltpu.VMEM((4 * KY, 2 * NG), BF16),
            pltpu.VMEM((4 * KY, 2 * NG), BF16),
            pltpu.VMEM((HID, FEAT), BF16),
            pltpu.VMEM((FEAT, HID), BF16),
            pltpu.VMEM((HID, FEAT), BF16),
            pltpu.VMEM((HID, 128), F32),
            pltpu.VMEM((HID, 256), F32),
            pltpu.VMEM((HID, 256), F32),
            pltpu.VMEM((HID, 4096), BF16),
            pltpu.VMEM((HID, 4096), BF16),
            pltpu.VMEM((256, 4096), BF16),
            pltpu.VMEM((FEAT, 4096), BF16),
            pltpu.VMEM((6, 128, ROW), F32),
            pltpu.VMEM((8, 128, 128), F32),
            pltpu.SemaphoreType.DMA((16,)),
            pltpu.SemaphoreType.DMA((7,)),
            pltpu.SemaphoreType.DMA((7,)),
        ],
        compiler_params=pltpu.CompilerParams(
            collective_id=0, has_side_effects=True, vmem_limit_bytes=LIMIT
        ),
    )(*[pltpu.with_memory_space_constraint(o, pltpu.HBM) for o in [*operands, t["ty"], t["tyk"]]])
    free = pl.BlockSpec(memory_space=pl.ANY)
    grad, grad_in, grad_out, grad_bias = pl.pallas_call(
        copy_out,
        out_shape=[sds(r.shape, r.dtype) for r in results],
        in_specs=[free] * 4,
        out_specs=[ANY] * 4,
        scratch_shapes=[pltpu.SemaphoreType.DMA((4,))],
        compiler_params=pltpu.CompilerParams(vmem_limit_bytes=8 * 1024 * 1024),
    )(*results)
    return grad.transpose(0, 1, 3, 2, 4), grad_in, grad_out.T, grad_bias


def solution(mesh):
    split = P("rep", None, "px", "py", None)
    both = ("px", "py")
    return jax.shard_map(
        shards,
        mesh=mesh,
        in_specs=(split, split, P(), P(), P()),
        out_specs=(split, P(both, "rep"), P("rep", both), P("rep", both)),
        check_vma=False,
    )
```

```python
import numpy as np

import jax
import jax.numpy as jnp
from jax import lax
from jax.experimental import pallas as pl
from jax.experimental.pallas import tpu as pltpu
from jax.sharding import PartitionSpec as P

F32 = jnp.float32
BF16 = jnp.bfloat16
MESH = pl.DeviceIdType.MESH
NN = (((1,), (0,)), ((), ()))
NT = (((1,), (1,)), ((), ()))
TN = (((0,), (0,)), ((), ()))

NG, KY, KZ, HID, FEAT = 256, 192, 96, 512, 192
CUT = NG // 3
NU_DT = 5e-05
TIME_STEP = 0.01
FORCING = 20.0
NDEV = 64
WY, WZ = 24, 12
SLOT = 48
ROW = 8 * SLOT
INV = 8
FEW, LAST = 3, 2
ORDER = (0, 1, FEW, LAST)
FWD = 2
SPARE = 208
PITCH = 72


def dot(a, b, dims=NN, **kw):
    return lax.dot_general(a, b, dims, preferred_element_type=F32, **kw)


def make_tables():
    bf = jnp.bfloat16

    def angle(k, x):
        theta = 2 * np.pi * ((np.asarray(k)[:, None] % NG) * np.asarray(x)[None, :] % NG) / NG
        return np.cos(theta) / np.sqrt(NG), np.sin(theta) / np.sqrt(NG)

    order_x = np.arange(NG).reshape(64, 4).T.reshape(-1)
    c, s = angle(order_x, np.arange(NG))
    tx = np.concatenate([c, -s], axis=1)
    order = np.arange(NG).reshape(64, 4).T.reshape(-1)
    ids = np.arange(KY)
    ky = np.where(ids < KY // 2, ids, ids - KY)
    c, s = angle(ky, order)
    top = np.concatenate([c, s], axis=1).reshape(8, 1, WY, 2 * NG)
    low = np.concatenate([-s, c], axis=1).reshape(8, 1, WY, 2 * NG)
    kcol = ky.reshape(8, 1, WY, 1)
    ty = np.concatenate([top, low], axis=1).reshape(2 * KY, 2 * NG)
    tyk = np.concatenate([-kcol * low, kcol * top], axis=1).reshape(2 * KY, 2 * NG)
    kz = (np.arange(8)[None, :, None] * WZ + np.arange(3)[:, None, None] * 4 + np.arange(4)[None, None, :]).reshape(-1)
    c, s = angle(order, kz)
    tz = np.concatenate([c, -s], axis=1)
    kk = np.concatenate([kz, kz])[None, :]
    tzk = np.concatenate([s, c], axis=1) * kk
    perm = np.zeros((FEAT, FEAT), np.float32)
    src = np.arange(FEAT).reshape(3, 4, 4, 4).transpose(2, 0, 1, 3).reshape(-1)
    perm[src, np.arange(FEAT)] = 1.0
    back = np.zeros((256, 256), np.float32)
    back[:FEAT, :FEAT] = perm.T
    back[FEAT, FEAT] = 1.0
    arrays = dict(tx=tx, ty=ty, tyk=tyk, tz=tz, tzk=tzk, tzt=tz.T, tzkt=tzk.T, perm=perm)
    out = {k: np.asarray(v, np.float32).astype(bf) for k, v in arrays.items()}
    out["back"] = back
    return out


def waves_of(m, j, l):
    kz_id = l * WZ + m
    kz = kz_id.astype(F32)
    a = lax.broadcasted_iota(jnp.int32, (WY, NG), 0) + j * WY
    n = lax.broadcasted_iota(jnp.int32, (WY, NG), 1)
    ky = jnp.where(a < KY // 2, a, a - KY).astype(F32)
    kx = jnp.where(n < NG // 2, n, n - NG).astype(F32)
    keep = (jnp.abs(kx) <= CUT) & (jnp.abs(ky) <= CUT) & (kz <= float(CUT))
    retained = keep.astype(F32)
    square = kx * kx + ky * ky + kz * kz
    damping = jnp.exp(-NU_DT * square)
    weight = jnp.where(kz_id == 0, 1.0, 2.0).astype(F32)
    return kx, ky, kz, retained, square, damping, weight


LIMIT = 52 * 1024 * 1024
LINES = FWD * ROW + 128
PART = 24
GRADS = 4


def place(f, mh):
    if f >= 6:
        return LAST, f * 3 + mh - 18
    g, pp = divmod(f * 3 + mh, 8)
    return (FEW if g == 2 else g), pp


def lane_select(lane, v, pick):
    slots = [q for q in range(8) if q * SLOT < (v + 1) * 128 and (q + 1) * SLOT > v * 128]
    value = pick(slots[0])
    for q in slots[1:]:
        value = jnp.where(lane >= float(q * SLOT - v * 128), pick(q), value)
    return value


def cross(a, b):
    return [a[1] * b[2] - a[2] * b[1], a[2] * b[0] - a[0] * b[2], a[0] * b[1] - a[1] * b[0]]


def main_kernel(
    state_hbm, cot_hbm, tx_hbm, tz_hbm, tzk_hbm, tzt_hbm, tzkt_hbm, perm_hbm, back_hbm, w_in_hbm, b_hbm, w_out_hbm,
    ty_hbm, tyk_hbm,
    out_ref, grad_in_ref, grad_out_ref, grad_bias_ref,
    state_ref, cot_ref, tx_ref, tz_ref, tzk_ref, tzt_ref, tzkt_ref, perm_ref, back_ref, w_in_t, b_row, w_out,
    s_ref, flat, sent, got, sent_few, got_few, v32, va32, o16, mine, gsent, ggot, ty_ref, tyk_ref,
    win, wint, woutt, bias, gin, gout, hid_all, pre_all, feat_all, adj_all, ky_part, load_sem, send_sem, recv_sem,
):
    j, l = lax.axis_index("px"), lax.axis_index("py")
    me = j * 8 + l
    x, core, z, y = j >> 1, j & 1, l >> 2, l & 3
    l32, o32, kz_part, back = flat, v32, state_ref, sent

    def peer(k):
        k = k + jnp.where(k >= 3, 1, 0)
        dx = (k & 3) + 1
        dy = dx + ((k >> 2) & 3)
        px = (((x + dx) & 3) << 1) + ((core + (k >> 4)) & 1)
        py = (((z + (k >> 5)) & 1) << 2) + ((y + dy) & 3)
        return (px << 3) + py, {"px": px, "py": py}

    barrier = pltpu.get_barrier_semaphore()

    def greet(k, carry):
        pl.semaphore_signal(barrier, inc=1, device_id=peer(k)[1], device_id_type=MESH)
        return carry

    half = 2 * KY
    pairs = [(cot_hbm, cot_ref), (tx_hbm, tx_ref), (state_hbm, state_ref)]
    for src, dst in [(ty_hbm, ty_ref), (tyk_hbm, tyk_ref)]:
        pairs += [(src, dst.at[pl.ds(0, half)]), (src, dst.at[pl.ds(half, half)])]
    pairs += [(tz_hbm, tz_ref), (tzk_hbm, tzk_ref), (tzt_hbm, tzt_ref), (tzkt_hbm, tzkt_ref), (perm_hbm, perm_ref)]
    pairs += [(back_hbm, back_ref), (w_in_hbm, w_in_t), (b_hbm, b_row), (w_out_hbm, w_out)]
    loads = [pltpu.make_async_copy(src, dst, load_sem.at[n]) for n, (src, dst) in enumerate(pairs)]
    for load in loads:
        load.start()
    lax.fori_loop(0, NDEV - 1, greet, 0, unroll=3)

    def copy(src, dst, number, where):
        return pltpu.make_async_remote_copy(
            src_ref=src,
            dst_ref=dst,
            send_sem=send_sem.at[number],
            recv_sem=recv_sem.at[number],
            device_id=where,
            device_id_type=MESH,
        )

    def send_all(src, dst, number):
        def send(k, carry):
            t, where = peer(k)
            copy(src.at[t], dst.at[me], number, where).start()
            return carry

        dst[pl.ds(me, 1)] = src[pl.ds(me, 1)]
        lax.fori_loop(0, NDEV - 1, send, 0, unroll=3)

    def whole(src, dst, number):
        rest = pl.ds(0, NDEV - 1)
        return copy(src.at[rest], dst.at[rest], number, peer(0)[1])

    ways = [(sent.at[g], got.at[g]) for g in range(3)] + [(sent_few, got_few)]
    for group in ORDER:
        for load in {0: loads[0:2], 1: loads[2:3]}.get(group, []):
            load.wait()
        lanes = 128 if group == FEW else ROW

        def one(mp, carry):
            for mh in range(3):
                fields = [f for f in range(INV) if place(f, mh)[0] == group]
                if not fields:
                    continue
                m = mh * 4 + mp
                kx, ky, kz, retained, square, damping, weight = waves_of(m, j, l)
                value = {}
                if any(f >= 3 for f in fields):
                    scale = weight * retained
                    need = {c for f in fields for c in {6: (0, 2), 7: (0, 1)}.get(f, (f - 3,)) if f >= 3}
                    v = {c: [scale * state_ref[(c * 2 + r) * WZ + m] for r in range(2)] for c in sorted(need)}
                    value.update({3 + c: v[c] for c in v})
                    if 6 in fields:
                        value[6] = [-(kz * v[0][1] - kx * v[2][1]), kz * v[0][0] - kx * v[2][0]]
                    if 7 in fields:
                        value[7] = [-(kx * v[1][1] - ky * v[0][1]), kx * v[1][0] - ky * v[0][0]]
                if any(f < 3 for f in fields):
                    inverse = 1.0 / jnp.maximum(square, 1.0)
                    scale = TIME_STEP * retained
                    force = [[], [], []]
                    for r in range(2):
                        w = [damping * cot_ref[c, r, m] for c in range(3)]
                        along = (kx * w[0] + ky * w[1] + kz * w[2]) * inverse
                        for c, k in enumerate((kx, ky, kz)):
                            force[c].append(scale * (w[c] - k * along))
                    value.update({c: force[c] for c in range(3)})
                for f in fields:
                    re, im = value[f]
                    top = jnp.concatenate([re, im], axis=1)
                    low = jnp.concatenate([im, -re], axis=1)
                    pp = place(f, mh)[1]
                    row = pp * SLOT if group == FEW else pl.multiple_of(((pp + j) & 7) * SLOT, 16)
                    s_ref[pl.ds(row, SLOT), :] = jnp.concatenate([top, low], axis=0).astype(BF16)
            for first in range(0, lanes, 256):
                width = min(256, lanes - first)
                out = dot(tx_ref[...], s_ref[first : first + width, :], NT)
                for c in range(width // 128):
                    for xx in range(4):
                        base = (first // 128 + c) * NDEV * PART
                        flat[pl.ds(base + mp * 4 + xx, NDEV, stride=PART), :] = out[
                            xx * 64 : (xx + 1) * 64, c * 128 : (c + 1) * 128
                        ]
            return carry

        lax.fori_loop(0, 4, one, 0)

        def pack(d, carry):
            for c in range(lanes // 128):
                row = pl.multiple_of(c * NDEV * PART + d * PART, 8)
                ways[group][0][d, :, c * 128 : (c + 1) * 128] = flat[pl.ds(row, 16), :].astype(BF16)
            return carry

        lax.fori_loop(0, NDEV, pack, 0, unroll=4)
        if group == ORDER[0]:
            pl.semaphore_wait(barrier, NDEV - 1)
        send_all(*ways[group], group)

    lane = lax.broadcasted_iota(jnp.int32, (1, 128), 1).astype(BF16)
    lane = jnp.broadcast_to(lane, (128, 128))

    for load in loads[3:]:
        load.wait()
    perm = perm_ref[...]
    win[...] = dot(w_in_t[...], perm, TN).astype(BF16)
    wint[...] = dot(perm, w_in_t[...], TN).astype(BF16)
    woutt[...] = dot(w_out[...], perm, TN).astype(BF16)
    gin[...] = jnp.zeros_like(gin)
    gout[...] = jnp.zeros_like(gout)
    feat_all[FEAT:256, :] = jnp.ones((256 - FEAT, 4096), BF16)
    bias[...] = jnp.broadcast_to(b_row[...], (128, HID)).T

    BLOCKS = 27

    def block_of(f, mh):
        g, pp = place(f, mh)
        return 24 + mh if f == INV else {0: 0, 1: 8, FEW: 16, LAST: 18}[g] + pp

    def along_y(group):
        for f in range(INV):
            for mh in range(3):
                g, pp = place(f, mh)
                if g != group:
                    continue
                first = (8 - pp) * SLOT
                parts = []
                if group == FEW:
                    first = 0
                    for n in range(8):
                        rows = got_few[n * 8 : n * 8 + 8].reshape(128, 128).astype(F32)
                        parts.append(rows[:, pp * SLOT : (pp + 1) * SLOT])
                else:
                    for v in range(3):
                        pick = lambda q: got[
                            group, (q - pp) % 8 * 8 : (q - pp) % 8 * 8 + 8, :, v * 128 : (v + 1) * 128
                        ].reshape(128, 128)
                        parts.append(lane_select(lane, v, pick))
                left = jnp.concatenate(parts, axis=1).astype(BF16)
                todo = [(block_of(f, mh), dot(left, ty_ref[first : first + 2 * KY, :]))]
                if f == 5:
                    todo.append((24 + mh, -dot(left, tyk_ref[first : first + 2 * KY, :])))
                for block, out in todo:
                    for c in range(4):
                        row = (c * BLOCKS + block) * 128
                        flat[row : row + 128, :] = out[:, c * 128 : (c + 1) * 128]

    def columns(f, xx):
        parts = []
        for t in range(2):
            for mh in range(3):
                lanes = [
                    flat[pl.ds(((2 * t + h) * BLOCKS + block_of(f, mh)) * 128 + xx, 32, stride=4), :] for h in range(2)
                ]
                parts.append(jnp.concatenate(lanes, axis=1))
        return jnp.concatenate(parts, axis=0).astype(BF16)

    def along_z(fields):
        def one(xx, carry):
            for slot, f in fields:
                out = dot(tz_ref[...], columns(f, xx))
                if f == INV:
                    out = out + dot(tzk_ref[...], columns(4, xx))
                out = out.astype(BF16).astype(F32)
                for dz in range(4):
                    row = pl.multiple_of((slot * 16 + xx * 4 + dz) * PITCH, 8)
                    for h in range(2):
                        v32[h, pl.ds(row, 64), :] = out[dz * 64 : (dz + 1) * 64, h * 128 : (h + 1) * 128]
            return carry

        lax.fori_loop(0, 4, one, 0, unroll=4 if len(fields) == 1 else 2)

    def boxes(fields):
        def one(group, carry):
            cols = pl.ds(pl.multiple_of(group * 256, 256), 256)
            for slot, ref, c in fields:
                rows = [pl.ds(slot * 16 * PITCH + group * 4 + b, 16, stride=PITCH) for b in range(4)]
                planes = [[v32[h, r, :] for h in range(2)] for r in rows]
                for dy in range(4):
                    h, at = dy // 2, dy % 2 * 64
                    value = jnp.concatenate([q[h][:, at : at + 64] for q in planes], axis=1)
                    ref[dy * 48 + c * 16 : dy * 48 + (c + 1) * 16, cols] = value.astype(BF16)
            return carry

        lax.fori_loop(0, 16, one, 0, unroll=4 if len(fields) == 1 else 2)

    for group, fields in [(0, [(6, 0), (7, 1)]), (1, [(8, 2), (0, 3), (1, 4)]), (FEW, [(2, 5)])]:
        whole(*ways[group], group).wait_recv()
        along_y(group)
        along_z(fields)
        if group == 0:
            boxes([(6, adj_all, 0), (7, adj_all, 1)])
        if group == 1:
            boxes([(8, adj_all, 2), (0, feat_all, 0), (1, feat_all, 1)])
    for group in (0, 1, FEW):
        whole(*ways[group], group).wait_send()

    def put(first, value, xx):
        for r in range(2):
            for mh in range(3):
                for h in range(2):
                    part = value[r * 96 + mh * 32 : r * 96 + (mh + 1) * 32, h * 128 : (h + 1) * 128]
                    if first < 12:
                        va32[h, pl.ds((r * 12 + first + mh) * 128 + xx, 32, stride=4), :] = part
                    else:
                        l32[pl.ds(((2 * r + h) * 9 + first + mh - 12) * 128 + xx, 32, stride=4), :] = part

    def plane(ref, c, xx, dz):
        row = pl.multiple_of((c * 16 + xx * 4 + dz) * PITCH, 8)
        return jnp.concatenate([ref[0, pl.ds(row, 64), :], ref[1, pl.ds(row, 64), :]], axis=1)

    def vort_z(xx, carry):
        parts = [[], [], []]
        for dz in range(4):
            vel = [plane(v32, c, xx, dz) for c in range(3)]
            frc = [plane(v32, 6 + c, xx, dz) for c in range(3)]
            for c, value in enumerate(cross(frc, vel)):
                parts[c].append(value.astype(BF16))
        wx, wy, wz = [jnp.concatenate(q, axis=0) for q in parts]
        tzt = tzt_ref[...]
        tzkt = tzkt_ref[...]
        kz_part[pl.ds(xx * 16, 8)] = dot(tzkt, wy).reshape(8, WY, NG)
        kz_part[pl.ds(xx * 16 + 8, 8)] = dot(tzkt, wx).reshape(8, WY, NG)
        put(0, dot(tzt, wy), xx)
        value = dot(tzt, wz)
        put(3, value, xx)
        put(6, value, xx)
        put(9, -dot(tzt, wx), xx)
        return carry

    def back_y(block, pp, table):
        first = (8 - pp) * SLOT
        parts = []
        for r in range(2):
            for h in range(2):
                if block < 12:
                    parts.append(va32[h, (r * 12 + block) * 128 : (r * 12 + block + 1) * 128, :])
                else:
                    row = ((2 * r + h) * 9 + block - 12) * 128
                    parts.append(l32[row : row + 128, :])
        return dot(jnp.concatenate(parts, axis=1).astype(BF16), table[first : first + 2 * KY, :], NT)

    def leave(g, used):
        for to in range(8):
            for v in range(3):
                pick = lambda q: o16[(q - to) % 8 % used, :, v * 128 : (v + 1) * 128]
                back[g, to * 8 : to * 8 + 8, :, v * 128 : (v + 1) * 128] = lane_select(lane, v, pick).reshape(8, 16, 128)
        send_all(back.at[g], mine.at[g], GRADS + 1 + g)

    lax.fori_loop(0, 4, vort_z, 0, unroll=2)
    for pp in range(6):
        o16[pp] = back_y(pp, pp, ty_ref).astype(BF16)
    leave(0, 6)
    for pp in range(6):
        ky_part[pp] = back_y(6 + pp, pp, tyk_ref)
    boxes([(2, feat_all, 2)])

    def closure(group, carry):
        bzs = [group * 4 + b for b in range(4)]
        cols = pl.ds(pl.multiple_of(group * 256, 256), 256)
        features = feat_all[0:FEAT, cols]
        adjoints = adj_all[:, cols]
        shift = bias[...]
        pre = dot(win[...], features) + jnp.concatenate([shift, shift], axis=1)
        sigmoid = 0.5 + 0.5 * jnp.tanh(0.5 * pre)
        hid_all[:, cols] = (pre * sigmoid).astype(BF16)
        hidden_adj = FORCING * dot(woutt[...], adjoints)
        pre_adj = (hidden_adj * sigmoid * (1.0 + pre * (1.0 - sigmoid))).astype(BF16)
        pre_all[:, cols] = pre_adj
        feat_adj = dot(wint[...], pre_adj)
        for b, bz in enumerate(bzs):
            for h in range(2):
                lanes = [feat_adj[dy * 48 : (dy + 1) * 48, b * 64 : (b + 1) * 64] for dy in (2 * h, 2 * h + 1)]
                va32[h, pl.ds(bz, 48, stride=PITCH), :] = jnp.concatenate(lanes, axis=1)
        return carry

    lax.fori_loop(0, 16, closure, 0, unroll=4)

    whole(*ways[LAST], LAST).wait_recv()
    along_y(LAST)
    along_z([(3, INV), (4, 6), (5, 7)])

    def vel_z(xx, carry):
        tzt = tzt_ref[...]
        parts = [[], [], []]
        for dz in range(4):
            spin = [plane(v32, 3 + c, xx, dz) for c in range(3)]
            frc = [plane(v32, 6 + c, xx, dz) for c in range(3)]
            for c, value in enumerate(cross(spin, frc)):
                parts[c].append((value + plane(va32, c, xx, dz)).astype(BF16))
        field = lambda c: jnp.concatenate(parts[c], axis=0)
        put(12, dot(tzt, field(0)) - kz_part[pl.ds(xx * 16, 8)].reshape(KY, NG), xx)
        put(15, dot(tzt, field(2)), xx)
        put(18, dot(tzt, field(1)) + kz_part[pl.ds(xx * 16 + 8, 8)].reshape(KY, NG), xx)
        return carry

    lax.fori_loop(0, 4, vel_z, 0, unroll=2)
    for pp in range(8):
        out = back_y(12 + pp, pp, ty_ref)
        o16[pp] = (out + ky_part[pp] if pp < 6 else out).astype(BF16)
    leave(1, 8)
    ninth = back_y(20, 0, ty_ref)
    for to in range(8):
        piece = ninth[:, to * SLOT : (to + 1) * SLOT]
        va32[0, to * 128 : (to + 1) * 128, :] = jnp.concatenate([jnp.zeros((128, SPARE - 128), F32), piece], axis=1)

    def products(k, carry):
        cols = pl.ds(pl.multiple_of(k * 1024, 1024), 1024)
        gin[...] += dot(pre_all[:, cols], feat_all[:, cols], NT)
        gout[:, 0:FEAT] += dot(hid_all[:, cols], adj_all[:, cols], NT)
        return carry

    lax.fori_loop(0, 4, products, 0)
    own_lane = lax.broadcasted_iota(jnp.int32, (16, 128), 1) < SPARE - 128

    def slices(d, carry):
        rows = pl.ds(pl.multiple_of(d * 8, 8), 8)
        extra = va32[0, pl.ds(pl.multiple_of(d * 16, 16), 16), :]
        lo = jnp.concatenate([gin[rows, 0:128], FORCING * gout[rows, 0:128]], axis=0)
        hi = jnp.concatenate([gin[rows, 128:256], FORCING * gout[rows, 128:256]], axis=0)
        gsent[d, :, 0:128] = lo.astype(BF16)
        gsent[d, :, 128:256] = jnp.where(own_lane, hi, extra).astype(BF16)
        return carry

    lax.fori_loop(0, NDEV, slices, 0, unroll=4)
    send_all(gsent, ggot, GRADS)

    def arrive(ref, chunk, lanes):
        def unpack(d, carry):
            row = pl.multiple_of((chunk * NDEV + d) * PART, 8)
            flat[pl.ds(row, 16), :] = ref[d, :, lanes : lanes + 128].astype(F32)
            return carry

        lax.fori_loop(0, NDEV, unpack, 0, unroll=8)

    def along_x(chunks):
        def one(mp, carry):
            for c in chunks:
                rows = [flat[pl.ds(c * NDEV * PART + mp * 4 + xx, NDEV, stride=PART), :] for xx in range(4)]
                out = dot(jnp.concatenate(rows, axis=0).astype(BF16), tx_ref[...], TN)
                for r in range(2):
                    for h in range(2):
                        row = pl.multiple_of((mp * 2 + r) * LINES + c * 128, 8)
                        o32[h, pl.ds(row, 128), :] = out[:, (2 * r + h) * 128 : (2 * r + h + 1) * 128]
            return carry

        lax.fori_loop(0, 4, one, 0, unroll=4 if len(chunks) == 1 else 1)

    def finish(late):
        def one(mp, carry):
            for mh in range(2 if late else 0, 3):
                m = mh * 4 + mp
                kx, ky, kz, retained, square, damping, weight = waves_of(m, j, l)
                scale = weight * retained

                def part(g, piece):
                    at = g * ROW + ((piece + j) & 7) * SLOT if piece < 8 else FWD * ROW + SPARE - 128
                    row = pl.multiple_of(mp * 2 * LINES + at, 8)
                    wave = lambda r, s: jnp.concatenate(
                        [o32[h, pl.ds(row + r * LINES + s * WY, WY), :] for h in range(2)], axis=1
                    )
                    return wave(0, 0) - wave(1, 1), wave(0, 1) + wave(1, 0)

                spec = {}
                if not late:
                    az, wy = part(1, 3 + mh), part(0, mh)
                    spec[0] = part(1, mh)
                    spec[2] = (az[0] - kx * wy[1], az[1] + kx * wy[0])
                if late or mh < 2:
                    ay, wz = part(1, 6 + mh), part(0, 3 + mh)
                    spec[1] = (ay[0] + kx * wz[1], ay[1] - kx * wz[0])
                for c, value in spec.items():
                    for r in range(2):
                        out_ref[c, r, m] = damping * cot_ref[c, r, m] + scale * value[r]
            return carry

        lax.fori_loop(0, 4, one, 0)

    for g in range(FWD):
        whole(back.at[g], mine.at[g], GRADS + 1 + g).wait_recv()
        for c in range(3):
            arrive(mine.at[g], g * 3 + c, c * 128)
        along_x(range(g * 3, g * 3 + 3))
    finish(False)
    whole(gsent, ggot, GRADS).wait_recv()
    arrive(ggot, 6, 128)
    along_x([6])
    finish(True)

    total = lax.fori_loop(0, NDEV, lambda d, t: t + ggot[d].astype(F32), jnp.zeros((16, 256), F32), unroll=4)
    ordered = dot(total, back_ref[...], precision=lax.Precision.HIGHEST)
    grad_in_ref[...] = ordered[0:8, 0:FEAT]
    grad_out_ref[...] = ordered[8:16, 0:FEAT]
    pick = (lax.broadcasted_iota(jnp.int32, (8, 256), 1) == FEAT).astype(F32)
    grad_bias_ref[...] = dot(pick, total[0:8], NT, precision=lax.Precision.HIGHEST)[0:1]

    whole(*ways[LAST], LAST).wait_send()
    whole(gsent, ggot, GRADS).wait_send()
    for g in range(FWD):
        whole(back.at[g], mine.at[g], GRADS + 1 + g).wait_send()


def copy_out(*refs):
    sources, results, sem = refs[:4], refs[4:8], refs[8]
    copies = [pltpu.make_async_copy(a, b, sem.at[n]) for n, (a, b) in enumerate(zip(sources, results))]
    for copy in copies:
        copy.start()
    for copy in copies:
        copy.wait()


ANY = pl.BlockSpec(memory_space=pltpu.HBM)
VMEM = pl.BlockSpec(memory_space=pltpu.VMEM)


def shards(state, cotangent, w_in, b_in, w_out):
    t = {k: jnp.asarray(v) for k, v in make_tables().items()}
    sds = jax.ShapeDtypeStruct
    operands = [state.transpose(0, 1, 3, 2, 4).reshape(6 * WZ, WY, NG), cotangent.transpose(0, 1, 3, 2, 4)]
    operands += [t[k] for k in ("tx", "tz", "tzk", "tzt", "tzkt", "perm", "back")]
    operands += [w_in.T, b_in[None, :], w_out]
    results = pl.pallas_call(
        main_kernel,
        out_shape=(sds((3, 2, WZ, WY, NG), F32), sds((8, FEAT), F32), sds((8, FEAT), F32), sds((1, 8), F32)),
        in_specs=[ANY] * 14,
        out_specs=(VMEM,) * 4,
        scratch_shapes=[pltpu.VMEM(o.shape, o.dtype) for o in operands]
        + [
            pltpu.VMEM((ROW, 2 * NG), BF16),
            pltpu.VMEM((4 * 27 * 128, 128), F32),
            pltpu.VMEM((3, NDEV, 16, ROW), BF16),
            pltpu.VMEM((3, NDEV, 16, ROW), BF16),
            pltpu.VMEM((NDEV, 16, 128), BF16),
            pltpu.VMEM((NDEV, 16, 128), BF16),
            pltpu.VMEM((2, 144 * PITCH, 128), F32),
            pltpu.VMEM((2, 48 * PITCH, 128), F32),
            pltpu.VMEM((8, 128, ROW), BF16),
            pltpu.VMEM((FWD, NDEV, 16, ROW), BF16),
            pltpu.VMEM((NDEV, 16, 256), BF16),
            pltpu.VMEM((NDEV, 16, 256), BF16),
            pltpu.VMEM((4 * KY, 2 * NG), BF16),
            pltpu.VMEM((4 * KY, 2 * NG), BF16),
            pltpu.VMEM((HID, FEAT), BF16),
            pltpu.VMEM((FEAT, HID), BF16),
            pltpu.VMEM((HID, FEAT), BF16),
            pltpu.VMEM((HID, 128), F32),
            pltpu.VMEM((HID, 256), F32),
            pltpu.VMEM((HID, 256), F32),
            pltpu.VMEM((HID, 4096), BF16),
            pltpu.VMEM((HID, 4096), BF16),
            pltpu.VMEM((256, 4096), BF16),
            pltpu.VMEM((FEAT, 4096), BF16),
            pltpu.VMEM((6, 128, ROW), F32),
            pltpu.SemaphoreType.DMA((16,)),
            pltpu.SemaphoreType.DMA((7,)),
            pltpu.SemaphoreType.DMA((7,)),
        ],
        compiler_params=pltpu.CompilerParams(
            collective_id=0, has_side_effects=True, vmem_limit_bytes=LIMIT
        ),
    )(*[pltpu.with_memory_space_constraint(o, pltpu.HBM) for o in [*operands, t["ty"], t["tyk"]]])
    free = pl.BlockSpec(memory_space=pl.ANY)
    grad, grad_in, grad_out, grad_bias = pl.pallas_call(
        copy_out,
        out_shape=[sds(r.shape, r.dtype) for r in results],
        in_specs=[free] * 4,
        out_specs=[ANY] * 4,
        scratch_shapes=[pltpu.SemaphoreType.DMA((4,))],
        compiler_params=pltpu.CompilerParams(vmem_limit_bytes=8 * 1024 * 1024),
    )(*results)
    return grad.transpose(0, 1, 3, 2, 4), grad_in, grad_out.T, grad_bias


def solution(mesh):
    split = P("rep", None, "px", "py", None)
    both = ("px", "py")
    return jax.shard_map(
        shards,
        mesh=mesh,
        in_specs=(split, split, P(), P(), P()),
        out_specs=(split, P(both, "rep"), P("rep", both), P("rep", both)),
        check_vma=False,
    )
```

```python
import numpy as np

import jax
import jax.numpy as jnp
from jax import lax
from jax.experimental import pallas as pl
from jax.experimental.pallas import tpu as pltpu
from jax.sharding import PartitionSpec as P

F32 = jnp.float32
BF16 = jnp.bfloat16
MESH = pl.DeviceIdType.MESH
NN = (((1,), (0,)), ((), ()))
NT = (((1,), (1,)), ((), ()))
TN = (((0,), (0,)), ((), ()))

NG, KY, KZ, HID, FEAT = 256, 192, 96, 512, 192
CUT = NG // 3
NU_DT = 5e-05
TIME_STEP = 0.01
FORCING = 20.0
NDEV = 64
WY, WZ = 24, 12
SLOT = 48
ROW = 8 * SLOT
INV = 8
FEW, LAST = 3, 2
ORDER = (0, 1, FEW, LAST)
FWD = 2
SPARE = 208
PITCH = 72


def dot(a, b, dims=NN, **kw):
    return lax.dot_general(a, b, dims, preferred_element_type=F32, **kw)


def make_tables():
    bf = jnp.bfloat16

    def angle(k, x):
        theta = 2 * np.pi * ((np.asarray(k)[:, None] % NG) * np.asarray(x)[None, :] % NG) / NG
        return np.cos(theta) / np.sqrt(NG), np.sin(theta) / np.sqrt(NG)

    order_x = np.arange(NG).reshape(64, 4).T.reshape(-1)
    c, s = angle(order_x, np.arange(NG))
    tx = np.concatenate([c, -s], axis=1)
    order = np.arange(NG).reshape(64, 4).T.reshape(-1)
    ids = np.arange(KY)
    ky = np.where(ids < KY // 2, ids, ids - KY)
    c, s = angle(ky, order)
    top = np.concatenate([c, s], axis=1).reshape(8, 1, WY, 2 * NG)
    low = np.concatenate([-s, c], axis=1).reshape(8, 1, WY, 2 * NG)
    kcol = ky.reshape(8, 1, WY, 1)
    ty = np.concatenate([top, low], axis=1).reshape(2 * KY, 2 * NG)
    tyk = np.concatenate([-kcol * low, kcol * top], axis=1).reshape(2 * KY, 2 * NG)
    kz = (np.arange(8)[None, :, None] * WZ + np.arange(3)[:, None, None] * 4 + np.arange(4)[None, None, :]).reshape(-1)
    c, s = angle(order, kz)
    tz = np.concatenate([c, -s], axis=1)
    kk = np.concatenate([kz, kz])[None, :]
    tzk = np.concatenate([s, c], axis=1) * kk
    perm = np.zeros((FEAT, FEAT), np.float32)
    src = np.arange(FEAT).reshape(3, 4, 4, 4).transpose(2, 0, 1, 3).reshape(-1)
    perm[src, np.arange(FEAT)] = 1.0
    back = np.zeros((256, 256), np.float32)
    back[:FEAT, :FEAT] = perm.T
    back[FEAT, FEAT] = 1.0
    arrays = dict(tx=tx, ty=ty, tyk=tyk, tz=tz, tzk=tzk, tzt=tz.T, tzkt=tzk.T, perm=perm)
    out = {k: np.asarray(v, np.float32).astype(bf) for k, v in arrays.items()}
    out["back"] = back
    return out


def waves_of(m, j, l):
    kz_id = l * WZ + m
    kz = kz_id.astype(F32)
    a = lax.broadcasted_iota(jnp.int32, (WY, NG), 0) + j * WY
    n = lax.broadcasted_iota(jnp.int32, (WY, NG), 1)
    ky = jnp.where(a < KY // 2, a, a - KY).astype(F32)
    kx = jnp.where(n < NG // 2, n, n - NG).astype(F32)
    keep = (jnp.abs(kx) <= CUT) & (jnp.abs(ky) <= CUT) & (kz <= float(CUT))
    retained = keep.astype(F32)
    square = kx * kx + ky * ky + kz * kz
    damping = jnp.exp(-NU_DT * square)
    weight = jnp.where(kz_id == 0, 1.0, 2.0).astype(F32)
    return kx, ky, kz, retained, square, damping, weight


LIMIT = 52 * 1024 * 1024
LINES = FWD * ROW + 128
PART = 24
GRADS = 4


def place(f, mh):
    if f >= 6:
        return LAST, f * 3 + mh - 18
    g, pp = divmod(f * 3 + mh, 8)
    return (FEW if g == 2 else g), pp


def lane_select(lane, v, pick):
    slots = [q for q in range(8) if q * SLOT < (v + 1) * 128 and (q + 1) * SLOT > v * 128]
    value = pick(slots[0])
    for q in slots[1:]:
        value = jnp.where(lane >= float(q * SLOT - v * 128), pick(q), value)
    return value


def cross(a, b):
    return [a[1] * b[2] - a[2] * b[1], a[2] * b[0] - a[0] * b[2], a[0] * b[1] - a[1] * b[0]]


def main_kernel(
    state_hbm, cot_hbm, tx_hbm, tz_hbm, tzk_hbm, tzt_hbm, tzkt_hbm, perm_hbm, back_hbm, w_in_hbm, b_hbm, w_out_hbm,
    ty_hbm, tyk_hbm,
    out_ref, grad_in_ref, grad_out_ref, grad_bias_ref,
    state_ref, cot_ref, tx_ref, tz_ref, tzk_ref, tzt_ref, tzkt_ref, perm_ref, back_ref, w_in_t, b_row, w_out,
    s_ref, flat, sent, got, sent_few, got_few, v32, va32, o16, mine, gsent, ggot, ty_ref, tyk_ref,
    win, wint, woutt, bias, gin, gout, hid_all, pre_all, feat_all, adj_all, ky_part, load_sem, send_sem, recv_sem,
):
    j, l = lax.axis_index("px"), lax.axis_index("py")
    me = j * 8 + l
    x, core, z, y = j >> 1, j & 1, l >> 2, l & 3
    l32, o32, kz_part, back = flat, v32, state_ref, sent

    def peer(k):
        k = k + jnp.where(k >= 6, 1, 0)
        dx = ((k >> 1) & 3) + 1
        dy = dx + ((k >> 3) & 3)
        px = (((x + dx) & 3) << 1) + ((core + (k >> 5)) & 1)
        py = (((z + k) & 1) << 2) + ((y + dy) & 3)
        return (px << 3) + py, {"px": px, "py": py}

    barrier = pltpu.get_barrier_semaphore()

    def greet(k, carry):
        pl.semaphore_signal(barrier, inc=1, device_id=peer(k)[1], device_id_type=MESH)
        return carry

    half = 2 * KY
    pairs = [(cot_hbm, cot_ref), (tx_hbm, tx_ref), (state_hbm, state_ref)]
    for src, dst in [(ty_hbm, ty_ref), (tyk_hbm, tyk_ref)]:
        pairs += [(src, dst.at[pl.ds(0, half)]), (src, dst.at[pl.ds(half, half)])]
    pairs += [(tz_hbm, tz_ref), (tzk_hbm, tzk_ref), (tzt_hbm, tzt_ref), (tzkt_hbm, tzkt_ref), (perm_hbm, perm_ref)]
    pairs += [(back_hbm, back_ref), (w_in_hbm, w_in_t), (b_hbm, b_row), (w_out_hbm, w_out)]
    loads = [pltpu.make_async_copy(src, dst, load_sem.at[n]) for n, (src, dst) in enumerate(pairs)]
    for load in loads:
        load.start()
    lax.fori_loop(0, NDEV - 1, greet, 0, unroll=3)

    def copy(src, dst, number, where):
        return pltpu.make_async_remote_copy(
            src_ref=src,
            dst_ref=dst,
            send_sem=send_sem.at[number],
            recv_sem=recv_sem.at[number],
            device_id=where,
            device_id_type=MESH,
        )

    def send_all(src, dst, number):
        def send(k, carry):
            t, where = peer(k)
            copy(src.at[t], dst.at[me], number, where).start()
            return carry

        dst[pl.ds(me, 1)] = src[pl.ds(me, 1)]
        lax.fori_loop(0, NDEV - 1, send, 0, unroll=3)

    def whole(src, dst, number):
        rest = pl.ds(0, NDEV - 1)
        return copy(src.at[rest], dst.at[rest], number, peer(0)[1])

    ways = [(sent.at[g], got.at[g]) for g in range(3)] + [(sent_few, got_few)]
    for group in ORDER:
        for load in {0: loads[0:2], 1: loads[2:3]}.get(group, []):
            load.wait()
        lanes = 128 if group == FEW else ROW

        def one(mp, carry):
            for mh in range(3):
                fields = [f for f in range(INV) if place(f, mh)[0] == group]
                if not fields:
                    continue
                m = mh * 4 + mp
                kx, ky, kz, retained, square, damping, weight = waves_of(m, j, l)
                value = {}
                if any(f >= 3 for f in fields):
                    scale = weight * retained
                    need = {c for f in fields for c in {6: (0, 2), 7: (0, 1)}.get(f, (f - 3,)) if f >= 3}
                    v = {c: [scale * state_ref[(c * 2 + r) * WZ + m] for r in range(2)] for c in sorted(need)}
                    value.update({3 + c: v[c] for c in v})
                    if 6 in fields:
                        value[6] = [-(kz * v[0][1] - kx * v[2][1]), kz * v[0][0] - kx * v[2][0]]
                    if 7 in fields:
                        value[7] = [-(kx * v[1][1] - ky * v[0][1]), kx * v[1][0] - ky * v[0][0]]
                if any(f < 3 for f in fields):
                    inverse = 1.0 / jnp.maximum(square, 1.0)
                    scale = TIME_STEP * retained
                    force = [[], [], []]
                    for r in range(2):
                        w = [damping * cot_ref[c, r, m] for c in range(3)]
                        along = (kx * w[0] + ky * w[1] + kz * w[2]) * inverse
                        for c, k in enumerate((kx, ky, kz)):
                            force[c].append(scale * (w[c] - k * along))
                    value.update({c: force[c] for c in range(3)})
                for f in fields:
                    re, im = value[f]
                    top = jnp.concatenate([re, im], axis=1)
                    low = jnp.concatenate([im, -re], axis=1)
                    pp = place(f, mh)[1]
                    row = pp * SLOT if group == FEW else pl.multiple_of(((pp + j) & 7) * SLOT, 16)
                    s_ref[pl.ds(row, SLOT), :] = jnp.concatenate([top, low], axis=0).astype(BF16)
            for first in range(0, lanes, 256):
                width = min(256, lanes - first)
                out = dot(tx_ref[...], s_ref[first : first + width, :], NT)
                for c in range(width // 128):
                    for xx in range(4):
                        base = (first // 128 + c) * NDEV * PART
                        flat[pl.ds(base + mp * 4 + xx, NDEV, stride=PART), :] = out[
                            xx * 64 : (xx + 1) * 64, c * 128 : (c + 1) * 128
                        ]
            return carry

        lax.fori_loop(0, 4, one, 0)

        def pack(d, carry):
            for c in range(lanes // 128):
                row = pl.multiple_of(c * NDEV * PART + d * PART, 8)
                ways[group][0][d, :, c * 128 : (c + 1) * 128] = flat[pl.ds(row, 16), :].astype(BF16)
            return carry

        lax.fori_loop(0, NDEV, pack, 0, unroll=4)
        if group == ORDER[0]:
            pl.semaphore_wait(barrier, NDEV - 1)
        send_all(*ways[group], group)

    lane = lax.broadcasted_iota(jnp.int32, (1, 128), 1).astype(BF16)
    lane = jnp.broadcast_to(lane, (128, 128))

    for load in loads[3:]:
        load.wait()
    perm = perm_ref[...]
    win[...] = dot(w_in_t[...], perm, TN).astype(BF16)
    wint[...] = dot(perm, w_in_t[...], TN).astype(BF16)
    woutt[...] = dot(w_out[...], perm, TN).astype(BF16)
    gin[...] = jnp.zeros_like(gin)
    gout[...] = jnp.zeros_like(gout)
    feat_all[FEAT:256, :] = jnp.ones((256 - FEAT, 4096), BF16)
    bias[...] = jnp.broadcast_to(b_row[...], (128, HID)).T

    BLOCKS = 27

    def block_of(f, mh):
        g, pp = place(f, mh)
        return 24 + mh if f == INV else {0: 0, 1: 8, FEW: 16, LAST: 18}[g] + pp

    def along_y(group):
        for f in range(INV):
            for mh in range(3):
                g, pp = place(f, mh)
                if g != group:
                    continue
                first = (8 - pp) * SLOT
                parts = []
                if group == FEW:
                    first = 0
                    for n in range(8):
                        rows = got_few[n * 8 : n * 8 + 8].reshape(128, 128).astype(F32)
                        parts.append(rows[:, pp * SLOT : (pp + 1) * SLOT])
                else:
                    for v in range(3):
                        pick = lambda q: got[
                            group, (q - pp) % 8 * 8 : (q - pp) % 8 * 8 + 8, :, v * 128 : (v + 1) * 128
                        ].reshape(128, 128)
                        parts.append(lane_select(lane, v, pick))
                left = jnp.concatenate(parts, axis=1).astype(BF16)
                todo = [(block_of(f, mh), dot(left, ty_ref[first : first + 2 * KY, :]))]
                if f == 5:
                    todo.append((24 + mh, -dot(left, tyk_ref[first : first + 2 * KY, :])))
                for block, out in todo:
                    for c in range(4):
                        row = (c * BLOCKS + block) * 128
                        flat[row : row + 128, :] = out[:, c * 128 : (c + 1) * 128]

    def columns(f, xx):
        parts = []
        for t in range(2):
            for mh in range(3):
                lanes = [
                    flat[pl.ds(((2 * t + h) * BLOCKS + block_of(f, mh)) * 128 + xx, 32, stride=4), :] for h in range(2)
                ]
                parts.append(jnp.concatenate(lanes, axis=1))
        return jnp.concatenate(parts, axis=0).astype(BF16)

    def along_z(fields):
        def one(xx, carry):
            for slot, f in fields:
                out = dot(tz_ref[...], columns(f, xx))
                if f == INV:
                    out = out + dot(tzk_ref[...], columns(4, xx))
                out = out.astype(BF16).astype(F32)
                for dz in range(4):
                    row = pl.multiple_of((slot * 16 + xx * 4 + dz) * PITCH, 8)
                    for h in range(2):
                        v32[h, pl.ds(row, 64), :] = out[dz * 64 : (dz + 1) * 64, h * 128 : (h + 1) * 128]
            return carry

        lax.fori_loop(0, 4, one, 0, unroll=4 if len(fields) == 1 else 2)

    def boxes(fields):
        def one(group, carry):
            cols = pl.ds(pl.multiple_of(group * 256, 256), 256)
            for slot, ref, c in fields:
                rows = [pl.ds(slot * 16 * PITCH + group * 4 + b, 16, stride=PITCH) for b in range(4)]
                planes = [[v32[h, r, :] for h in range(2)] for r in rows]
                for dy in range(4):
                    h, at = dy // 2, dy % 2 * 64
                    value = jnp.concatenate([q[h][:, at : at + 64] for q in planes], axis=1)
                    ref[dy * 48 + c * 16 : dy * 48 + (c + 1) * 16, cols] = value.astype(BF16)
            return carry

        lax.fori_loop(0, 16, one, 0, unroll=4 if len(fields) == 1 else 2)

    for group, fields in [(0, [(6, 0), (7, 1)]), (1, [(8, 2), (0, 3), (1, 4)]), (FEW, [(2, 5)])]:
        whole(*ways[group], group).wait_recv()
        along_y(group)
        along_z(fields)
        if group == 0:
            boxes([(6, adj_all, 0), (7, adj_all, 1)])
        if group == 1:
            boxes([(8, adj_all, 2), (0, feat_all, 0), (1, feat_all, 1)])
    for group in (0, 1, FEW):
        whole(*ways[group], group).wait_send()

    def put(first, value, xx):
        for r in range(2):
            for mh in range(3):
                for h in range(2):
                    part = value[r * 96 + mh * 32 : r * 96 + (mh + 1) * 32, h * 128 : (h + 1) * 128]
                    if first < 12:
                        va32[h, pl.ds((r * 12 + first + mh) * 128 + xx, 32, stride=4), :] = part
                    else:
                        l32[pl.ds(((2 * r + h) * 9 + first + mh - 12) * 128 + xx, 32, stride=4), :] = part

    def plane(ref, c, xx, dz):
        row = pl.multiple_of((c * 16 + xx * 4 + dz) * PITCH, 8)
        return jnp.concatenate([ref[0, pl.ds(row, 64), :], ref[1, pl.ds(row, 64), :]], axis=1)

    def vort_z(xx, carry):
        parts = [[], [], []]
        for dz in range(4):
            vel = [plane(v32, c, xx, dz) for c in range(3)]
            frc = [plane(v32, 6 + c, xx, dz) for c in range(3)]
            for c, value in enumerate(cross(frc, vel)):
                parts[c].append(value.astype(BF16))
        wx, wy, wz = [jnp.concatenate(q, axis=0) for q in parts]
        tzt = tzt_ref[...]
        tzkt = tzkt_ref[...]
        kz_part[pl.ds(xx * 16, 8)] = dot(tzkt, wy).reshape(8, WY, NG)
        kz_part[pl.ds(xx * 16 + 8, 8)] = dot(tzkt, wx).reshape(8, WY, NG)
        put(0, dot(tzt, wy), xx)
        value = dot(tzt, wz)
        put(3, value, xx)
        put(6, value, xx)
        put(9, -dot(tzt, wx), xx)
        return carry

    def back_y(block, pp, table):
        first = (8 - pp) * SLOT
        parts = []
        for r in range(2):
            for h in range(2):
                if block < 12:
                    parts.append(va32[h, (r * 12 + block) * 128 : (r * 12 + block + 1) * 128, :])
                else:
                    row = ((2 * r + h) * 9 + block - 12) * 128
                    parts.append(l32[row : row + 128, :])
        return dot(jnp.concatenate(parts, axis=1).astype(BF16), table[first : first + 2 * KY, :], NT)

    def leave(g, used):
        for to in range(8):
            for v in range(3):
                pick = lambda q: o16[(q - to) % 8 % used, :, v * 128 : (v + 1) * 128]
                back[g, to * 8 : to * 8 + 8, :, v * 128 : (v + 1) * 128] = lane_select(lane, v, pick).reshape(8, 16, 128)
        send_all(back.at[g], mine.at[g], GRADS + 1 + g)

    lax.fori_loop(0, 4, vort_z, 0, unroll=2)
    for pp in range(6):
        o16[pp] = back_y(pp, pp, ty_ref).astype(BF16)
    leave(0, 6)
    for pp in range(6):
        ky_part[pp] = back_y(6 + pp, pp, tyk_ref)
    boxes([(2, feat_all, 2)])

    def closure(group, carry):
        bzs = [group * 4 + b for b in range(4)]
        cols = pl.ds(pl.multiple_of(group * 256, 256), 256)
        features = feat_all[0:FEAT, cols]
        adjoints = adj_all[:, cols]
        shift = bias[...]
        pre = dot(win[...], features) + jnp.concatenate([shift, shift], axis=1)
        sigmoid = 0.5 + 0.5 * jnp.tanh(0.5 * pre)
        hid_all[:, cols] = (pre * sigmoid).astype(BF16)
        hidden_adj = FORCING * dot(woutt[...], adjoints)
        pre_adj = (hidden_adj * sigmoid * (1.0 + pre * (1.0 - sigmoid))).astype(BF16)
        pre_all[:, cols] = pre_adj
        feat_adj = dot(wint[...], pre_adj)
        for b, bz in enumerate(bzs):
            for h in range(2):
                lanes = [feat_adj[dy * 48 : (dy + 1) * 48, b * 64 : (b + 1) * 64] for dy in (2 * h, 2 * h + 1)]
                va32[h, pl.ds(bz, 48, stride=PITCH), :] = jnp.concatenate(lanes, axis=1)
        return carry

    lax.fori_loop(0, 16, closure, 0, unroll=4)

    whole(*ways[LAST], LAST).wait_recv()
    along_y(LAST)
    along_z([(3, INV), (4, 6), (5, 7)])

    def vel_z(xx, carry):
        tzt = tzt_ref[...]
        parts = [[], [], []]
        for dz in range(4):
            spin = [plane(v32, 3 + c, xx, dz) for c in range(3)]
            frc = [plane(v32, 6 + c, xx, dz) for c in range(3)]
            for c, value in enumerate(cross(spin, frc)):
                parts[c].append((value + plane(va32, c, xx, dz)).astype(BF16))
        field = lambda c: jnp.concatenate(parts[c], axis=0)
        put(12, dot(tzt, field(0)) - kz_part[pl.ds(xx * 16, 8)].reshape(KY, NG), xx)
        put(15, dot(tzt, field(2)), xx)
        put(18, dot(tzt, field(1)) + kz_part[pl.ds(xx * 16 + 8, 8)].reshape(KY, NG), xx)
        return carry

    lax.fori_loop(0, 4, vel_z, 0, unroll=2)
    for pp in range(8):
        out = back_y(12 + pp, pp, ty_ref)
        o16[pp] = (out + ky_part[pp] if pp < 6 else out).astype(BF16)
    leave(1, 8)
    ninth = back_y(20, 0, ty_ref)
    for to in range(8):
        piece = ninth[:, to * SLOT : (to + 1) * SLOT]
        va32[0, to * 128 : (to + 1) * 128, :] = jnp.concatenate([jnp.zeros((128, SPARE - 128), F32), piece], axis=1)

    def products(k, carry):
        cols = pl.ds(pl.multiple_of(k * 1024, 1024), 1024)
        gin[...] += dot(pre_all[:, cols], feat_all[:, cols], NT)
        gout[:, 0:FEAT] += dot(hid_all[:, cols], adj_all[:, cols], NT)
        return carry

    lax.fori_loop(0, 4, products, 0)
    own_lane = lax.broadcasted_iota(jnp.int32, (16, 128), 1) < SPARE - 128

    def slices(d, carry):
        rows = pl.ds(pl.multiple_of(d * 8, 8), 8)
        extra = va32[0, pl.ds(pl.multiple_of(d * 16, 16), 16), :]
        lo = jnp.concatenate([gin[rows, 0:128], FORCING * gout[rows, 0:128]], axis=0)
        hi = jnp.concatenate([gin[rows, 128:256], FORCING * gout[rows, 128:256]], axis=0)
        gsent[d, :, 0:128] = lo.astype(BF16)
        gsent[d, :, 128:256] = jnp.where(own_lane, hi, extra).astype(BF16)
        return carry

    lax.fori_loop(0, NDEV, slices, 0, unroll=4)
    send_all(gsent, ggot, GRADS)

    def arrive(ref, chunk, lanes):
        def unpack(d, carry):
            row = pl.multiple_of((chunk * NDEV + d) * PART, 8)
            flat[pl.ds(row, 16), :] = ref[d, :, lanes : lanes + 128].astype(F32)
            return carry

        lax.fori_loop(0, NDEV, unpack, 0, unroll=8)

    def along_x(chunks):
        def one(mp, carry):
            for c in chunks:
                rows = [flat[pl.ds(c * NDEV * PART + mp * 4 + xx, NDEV, stride=PART), :] for xx in range(4)]
                out = dot(jnp.concatenate(rows, axis=0).astype(BF16), tx_ref[...], TN)
                for r in range(2):
                    for h in range(2):
                        row = pl.multiple_of((mp * 2 + r) * LINES + c * 128, 8)
                        o32[h, pl.ds(row, 128), :] = out[:, (2 * r + h) * 128 : (2 * r + h + 1) * 128]
            return carry

        lax.fori_loop(0, 4, one, 0, unroll=4 if len(chunks) == 1 else 1)

    def finish(late):
        def one(mp, carry):
            for mh in range(2 if late else 0, 3):
                m = mh * 4 + mp
                kx, ky, kz, retained, square, damping, weight = waves_of(m, j, l)
                scale = weight * retained

                def part(g, piece):
                    at = g * ROW + ((piece + j) & 7) * SLOT if piece < 8 else FWD * ROW + SPARE - 128
                    row = pl.multiple_of(mp * 2 * LINES + at, 8)
                    wave = lambda r, s: jnp.concatenate(
                        [o32[h, pl.ds(row + r * LINES + s * WY, WY), :] for h in range(2)], axis=1
                    )
                    return wave(0, 0) - wave(1, 1), wave(0, 1) + wave(1, 0)

                spec = {}
                if not late:
                    az, wy = part(1, 3 + mh), part(0, mh)
                    spec[0] = part(1, mh)
                    spec[2] = (az[0] - kx * wy[1], az[1] + kx * wy[0])
                if late or mh < 2:
                    ay, wz = part(1, 6 + mh), part(0, 3 + mh)
                    spec[1] = (ay[0] + kx * wz[1], ay[1] - kx * wz[0])
                for c, value in spec.items():
                    for r in range(2):
                        out_ref[c, r, m] = damping * cot_ref[c, r, m] + scale * value[r]
            return carry

        lax.fori_loop(0, 4, one, 0)

    for g in range(FWD):
        whole(back.at[g], mine.at[g], GRADS + 1 + g).wait_recv()
        for c in range(3):
            arrive(mine.at[g], g * 3 + c, c * 128)
        along_x(range(g * 3, g * 3 + 3))
    finish(False)
    whole(gsent, ggot, GRADS).wait_recv()
    arrive(ggot, 6, 128)
    along_x([6])
    finish(True)

    total = lax.fori_loop(0, NDEV, lambda d, t: t + ggot[d].astype(F32), jnp.zeros((16, 256), F32), unroll=4)
    ordered = dot(total, back_ref[...], precision=lax.Precision.HIGHEST)
    grad_in_ref[...] = ordered[0:8, 0:FEAT]
    grad_out_ref[...] = ordered[8:16, 0:FEAT]
    pick = (lax.broadcasted_iota(jnp.int32, (8, 256), 1) == FEAT).astype(F32)
    grad_bias_ref[...] = dot(pick, total[0:8], NT, precision=lax.Precision.HIGHEST)[0:1]

    whole(*ways[LAST], LAST).wait_send()
    whole(gsent, ggot, GRADS).wait_send()
    for g in range(FWD):
        whole(back.at[g], mine.at[g], GRADS + 1 + g).wait_send()


def copy_out(*refs):
    sources, results, sem = refs[:4], refs[4:8], refs[8]
    copies = [pltpu.make_async_copy(a, b, sem.at[n]) for n, (a, b) in enumerate(zip(sources, results))]
    for copy in copies:
        copy.start()
    for copy in copies:
        copy.wait()


ANY = pl.BlockSpec(memory_space=pltpu.HBM)
VMEM = pl.BlockSpec(memory_space=pltpu.VMEM)


def shards(state, cotangent, w_in, b_in, w_out):
    t = {k: jnp.asarray(v) for k, v in make_tables().items()}
    sds = jax.ShapeDtypeStruct
    operands = [state.transpose(0, 1, 3, 2, 4).reshape(6 * WZ, WY, NG), cotangent.transpose(0, 1, 3, 2, 4)]
    operands += [t[k] for k in ("tx", "tz", "tzk", "tzt", "tzkt", "perm", "back")]
    operands += [w_in.T, b_in[None, :], w_out]
    results = pl.pallas_call(
        main_kernel,
        out_shape=(sds((3, 2, WZ, WY, NG), F32), sds((8, FEAT), F32), sds((8, FEAT), F32), sds((1, 8), F32)),
        in_specs=[ANY] * 14,
        out_specs=(VMEM,) * 4,
        scratch_shapes=[pltpu.VMEM(o.shape, o.dtype) for o in operands]
        + [
            pltpu.VMEM((ROW, 2 * NG), BF16),
            pltpu.VMEM((4 * 27 * 128, 128), F32),
            pltpu.VMEM((3, NDEV, 16, ROW), BF16),
            pltpu.VMEM((3, NDEV, 16, ROW), BF16),
            pltpu.VMEM((NDEV, 16, 128), BF16),
            pltpu.VMEM((NDEV, 16, 128), BF16),
            pltpu.VMEM((2, 144 * PITCH, 128), F32),
            pltpu.VMEM((2, 48 * PITCH, 128), F32),
            pltpu.VMEM((8, 128, ROW), BF16),
            pltpu.VMEM((FWD, NDEV, 16, ROW), BF16),
            pltpu.VMEM((NDEV, 16, 256), BF16),
            pltpu.VMEM((NDEV, 16, 256), BF16),
            pltpu.VMEM((4 * KY, 2 * NG), BF16),
            pltpu.VMEM((4 * KY, 2 * NG), BF16),
            pltpu.VMEM((HID, FEAT), BF16),
            pltpu.VMEM((FEAT, HID), BF16),
            pltpu.VMEM((HID, FEAT), BF16),
            pltpu.VMEM((HID, 128), F32),
            pltpu.VMEM((HID, 256), F32),
            pltpu.VMEM((HID, 256), F32),
            pltpu.VMEM((HID, 4096), BF16),
            pltpu.VMEM((HID, 4096), BF16),
            pltpu.VMEM((256, 4096), BF16),
            pltpu.VMEM((FEAT, 4096), BF16),
            pltpu.VMEM((6, 128, ROW), F32),
            pltpu.SemaphoreType.DMA((16,)),
            pltpu.SemaphoreType.DMA((7,)),
            pltpu.SemaphoreType.DMA((7,)),
        ],
        compiler_params=pltpu.CompilerParams(
            collective_id=0, has_side_effects=True, vmem_limit_bytes=LIMIT
        ),
    )(*[pltpu.with_memory_space_constraint(o, pltpu.HBM) for o in [*operands, t["ty"], t["tyk"]]])
    free = pl.BlockSpec(memory_space=pl.ANY)
    grad, grad_in, grad_out, grad_bias = pl.pallas_call(
        copy_out,
        out_shape=[sds(r.shape, r.dtype) for r in results],
        in_specs=[free] * 4,
        out_specs=[ANY] * 4,
        scratch_shapes=[pltpu.SemaphoreType.DMA((4,))],
        compiler_params=pltpu.CompilerParams(vmem_limit_bytes=8 * 1024 * 1024),
    )(*results)
    return grad.transpose(0, 1, 3, 2, 4), grad_in, grad_out.T, grad_bias


def solution(mesh):
    split = P("rep", None, "px", "py", None)
    both = ("px", "py")
    return jax.shard_map(
        shards,
        mesh=mesh,
        in_specs=(split, split, P(), P(), P()),
        out_specs=(split, P(both, "rep"), P("rep", both), P("rep", both)),
        check_vma=False,
    )
```
